128 devices in a mesh: blk: 64 (over x, y_hi, z, core), rep: 2 (over y_lo).
Axes of the slice: x: 4, y: 4 (y_hi: 2, y_lo: 2; y = y_hi * 2 + y_lo), z: 4, core: 2. Of those that a mesh axis runs over, the one named last changes fastest.
Arguments:
- captions: bfloat16 [24576, 768], P(('blk', 'rep')), may hold values from -512 to 512
- images: bfloat16 [24576, 768], P(('blk', 'rep')), may hold values from -512 to 512
- positives: int32 [24576], P(('blk', 'rep')), may hold values from 0 to 24575, each once
- valid: int32 [24576], P(('blk', 'rep')), may hold values from 0 to 1, as said below
Outputs:
- caption_loss: float32 [24576], P(('blk', 'rep'))
- image_loss: float32 [24576], P(('blk', 'rep'))
- loss: float32 [], replicated
The draws below stay inside these ranges and needn't reach their ends.
Inputs may be any that keep to these rules, and one draw needn't show every extreme that they name: `positives`: each image row is the positive of exactly one caption; a program may pack several of these indices into one sent element. `valid`: the last image row is always real; a program may pack several of these flags into one sent element.
All inputs are finite; a program needn't handle non-finite values.
Results may differ from the reference program's by a relative error of at most 0.0003.
Values may be sent and summed in bfloat16 or wider, within the bound.
No kernel may reach another device: no remote copies, remote signals or barrier semaphores. Data moves between devices by JAX's collectives and lax.ppermute only.
A program may use at most 128 MiB of HBM per device.

```python
import math
import jax
import jax.numpy as jnp
from jax import lax

E = 768
PAIRS = 24576


def pair_fields(key):
    base_key = jax.random.fold_in(key, 11)
    caption_key, image_key = jax.random.split(base_key, 2)
    caption_rows = jax.random.normal(caption_key, (PAIRS, E), jnp.float32)
    image_rows = jax.random.normal(image_key, (PAIRS, E), jnp.float32) * (3.0 / math.sqrt(E))
    return (caption_rows.astype(jnp.bfloat16), image_rows.astype(jnp.bfloat16))


def draw_captions(key, part):
    return pair_fields(key)[0]


def draw_images(key, part):
    return pair_fields(key)[1]


def draw_valid(key, part):
    position = jax.lax.iota(jnp.int32, PAIRS)
    rolled = jax.random.randint(jax.random.fold_in(key, 23), (PAIRS,), 0, 4 * PAIRS)
    flags = (rolled < PAIRS + 2 * position).astype(jnp.int32)
    return flags.at[PAIRS - 1].set(1)


def setup_inputs(seed: int = 0) -> dict:
    keys = jax.random.split(jax.random.key(seed), 5)
    captions = draw_captions(jax.random.fold_in(keys[4], 71), 0)
    images = draw_images(jax.random.fold_in(keys[4], 71), 0)
    positives = jax.random.permutation(keys[2], PAIRS).astype(jnp.int32)
    valid = draw_valid(jax.random.fold_in(keys[4], 71), 0)
    return {"captions": captions, "images": images, "positives": positives, "valid": valid}


very_low = -1.0e30


def reference(captions, images, positives, valid):
    pair_count = captions.shape[0]
    block_size = math.gcd(pair_count, 1024)
    image_ok = valid.astype(jnp.float32)
    caption_ok = jnp.take(image_ok, positives, axis=0)
    usable = image_ok[None, :] > 0
    columns = lax.iota(jnp.int32, pair_count)

    def one_block(running, block_index):
        column_peak, column_total, column_match = running
        offset = (block_index * block_size).astype(jnp.int32)
        caption_rows = lax.dynamic_slice_in_dim(captions, offset, block_size)
        match_rows = lax.dynamic_slice_in_dim(positives, offset, block_size)
        ok_rows = lax.dynamic_slice_in_dim(caption_ok, offset, block_size)
        scores = jnp.dot(caption_rows, images.T, preferred_element_type=jnp.float32)
        is_positive = match_rows[:, None] == columns[None, :]
        picked = jnp.where(is_positive, scores, 0.0)
        highest = jnp.max(jnp.where(usable, scores, very_low), axis=1)
        row_total = jnp.sum(jnp.where(usable, jnp.exp(scores - highest[:, None]), 0.0), axis=1)
        row_loss = ok_rows * (highest + jnp.log(row_total) - jnp.sum(picked, axis=1))
        caption_live = ok_rows[:, None] > 0
        column_high = jnp.max(jnp.where(caption_live, scores, very_low), axis=0)
        renewed = jnp.maximum(column_peak, column_high)
        powers = jnp.where(caption_live, jnp.exp(scores - renewed[None, :]), 0.0)
        column_total = column_total * jnp.exp(column_peak - renewed) + jnp.sum(powers, axis=0)
        column_match = column_match + jnp.sum(picked, axis=0)
        return (renewed, column_total, column_match), row_loss

    started = (jnp.full((pair_count,), very_low, jnp.float32), jnp.zeros((pair_count,), jnp.float32), jnp.zeros((pair_count,), jnp.float32))
    finished, row_losses = lax.scan(one_block, started, jnp.arange(pair_count // block_size, dtype=jnp.int32))
    caption_loss = row_losses.reshape(pair_count)
    image_loss = image_ok * (finished[0] + jnp.log(finished[1]) - finished[2])
    loss = (jnp.sum(caption_loss) + jnp.sum(image_loss)) / (2.0 * jnp.sum(image_ok))
    return (caption_loss, image_loss, loss)
```

```python
import itertools

import jax
import jax.numpy as jnp
from jax import lax
from jax.experimental import pallas as pl
from jax.experimental.pallas import tpu as pltpu
from jax.sharding import Mesh
from jax.sharding import PartitionSpec as P


SIZES = {"x": 4, "h": 2, "z": 4, "c": 2, "l": 2}
AXES = tuple(SIZES)
LOG2E = 1.4426950408889634
LN2 = 0.6931471805599453
LOW = -1.0e30

B = 192
E = 768
CAPS = 16
IMGS = 8
R = CAPS * B
C = IMGS * B

CAP_OFFSETS = [
    (dx, dc, dl) for dc in (0, 1) for dx, dl in
    ((0, 0), (0, 1), (3, 0), (3, 1), (1, 0), (1, 1), (2, 0), (2, 1))
]
IMG_OFFSETS = [(0, 0), (0, 1), (3, 0), (3, 1), (1, 0), (1, 1), (2, 0), (2, 1)]


def shift(value, **off):
    axes = tuple(a for a in AXES if off.get(a))
    sizes = [SIZES[a] for a in axes]
    pairs = []
    for at in itertools.product(*map(range, sizes)):
        src = dst = 0
        for i, a, s in zip(at, axes, sizes):
            src, dst = src * s + i, dst * s + (i + off[a]) % s
        pairs.append((src, dst))
    return lax.ppermute(value, axes if len(axes) > 1 else axes[0], pairs)


def around(block, near, axis):
    pair = [block, near]
    left = [shift(b, **{axis: 1}) for b in pair]
    right = [shift(b, **{axis: 3}) for b in pair]
    far = [shift(left[0], **{axis: 1}), shift(right[1], **{axis: 3})]
    return pair + left + right + far


def place():
    return {a: lax.axis_index(a) for a in AXES}


def flat(p):
    at = 0
    for a in AXES:
        at = at * SIZES[a] + p[a]
    return at


def moved(p, off):
    q = dict(p)
    for a, d in off.items():
        q[a] = lax.rem(p[a] + d, SIZES[a])
    return q


def cap_place(p, k):
    dx, dc, dl = CAP_OFFSETS[k]
    return moved(p, {"x": dx, "c": dc, "l": dl})


def img_place(p, m):
    dz, dy = IMG_OFFSETS[m]
    return moved(p, {"z": dz, "h": dy, "l": dy})


def rows_of(k, n=B):
    return pl.ds(pl.multiple_of(k * n, n), n)


def scores_kernel(table, *refs):
    caps, imgs = refs[:CAPS], refs[CAPS:CAPS + IMGS]
    row_out, col_out = refs[CAPS + IMGS:CAPS + IMGS + 2]
    (cap_v, img_v, t_v, pos_b, bias_b, pos16, ids, rmax, rmatch, cmax, cmatch,
     sems) = refs[CAPS + IMGS + 2:]
    p = place()
    img_copies = [
        pltpu.make_async_copy(imgs[m], img_v.at[pl.ds(m * B, B)], sems.at[CAPS + m])
        for m in range(IMGS)
    ]
    cap_copies = [
        pltpu.make_async_copy(caps[k], cap_v.at[pl.ds(k * B, B)], sems.at[k])
        for k in range(CAPS)
    ]
    for copy in img_copies + cap_copies:
        copy.start()

    for k in range(CAPS):
        row = table[pl.ds(flat(cap_place(p, k)), 1), :]
        pos16[k:k + 1, :B] = lax.shift_right_arithmetic(row, 1).astype(jnp.float32)
    for m in range(IMGS):
        block = flat(img_place(p, m))
        row = table[pl.ds(block, 1), :]
        ok = (row & 1) > 0
        ids[0:1, m * B:(m + 1) * B] = (
            lax.broadcasted_iota(jnp.int32, (1, B), 1) + block * B
        ).astype(jnp.float32)
        ids[1:2, m * B:(m + 1) * B] = jnp.where(ok, 0.0, LOW)
    ok_all = (table[...] & 1).astype(jnp.float32).astype(jnp.bfloat16)
    columns = jnp.transpose(pos16[...])
    lane = lax.broadcasted_iota(jnp.int32, (B, 128), 1).astype(jnp.float32)
    lane_b = lax.broadcasted_iota(jnp.int32, (B, B), 1).astype(jnp.float32)
    for k in range(CAPS):
        pos = columns[:B, k:k + 1]
        hi = jnp.floor((pos + 0.5) * (1.0 / B))
        lo = pos - hi * B
        pick = jnp.where(hi == lane, 1.0, 0.0).astype(jnp.bfloat16)
        flags = jnp.dot(pick, ok_all, preferred_element_type=jnp.float32)
        ok = jnp.sum(jnp.where(lane_b == lo, flags, 0.0), axis=1, keepdims=True)
        pos_b[k * B:(k + 1) * B, :] = jnp.broadcast_to(pos, (B, 128))
        bias_b[k * B:(k + 1) * B, :] = jnp.broadcast_to(
            jnp.where(ok > 0.5, 0.0, LOW), (B, 128)
        )

    cmax[...] = jnp.full(cmax.shape, 4.0 * LOW, jnp.float32)
    cmatch[...] = jnp.zeros(cmatch.shape, jnp.float32)
    rmax[...] = jnp.full(rmax.shape, 4.0 * LOW, jnp.float32)
    rmatch[...] = jnp.zeros(rmatch.shape, jnp.float32)
    for copy in img_copies:
        copy.wait()

    step = 4 * B

    @pl.loop(0, R // step)
    def _(i):
        for j in range(4):
            pltpu.make_async_copy(
                caps[0], cap_v.at[pl.ds(0, B)], sems.at[i * 4 + j]
            ).wait()
        rows = rows_of(i, step)
        a = cap_v[rows, :]
        for n in range(C // 256):
            s = lax.dot_general(
                a, img_v[n * 256:(n + 1) * 256, :], (((1,), (1,)), ((), ())),
                preferred_element_type=jnp.float32,
            )
            q = s * LOG2E
            for half in range(2):
                at = pl.ds(n * 256 + half * 128, 128)
                qh = q[:, half * 128:(half + 1) * 128]
                t = (qh + bias_b[rows, :]) + ids[1:2, at]
                t_v[rows, at] = t
                w = jnp.where(pos_b[rows, :] == ids[0:1, at], qh, 0.0)
                rmax[rows, :] = jnp.maximum(rmax[rows, :], t)
                rmatch[rows, :] += w
                cmax[:, at] = jnp.maximum(cmax[:, at], jnp.max(t.reshape(-1, 8, 128), axis=0))
                cmatch[:, at] += jnp.sum(w.reshape(-1, 8, 128), axis=0)

    top = jnp.max(cmax[...], axis=0, keepdims=True)
    cmax[...] = jnp.broadcast_to(top, cmax.shape)

    lanes = lax.broadcasted_iota(jnp.int32, (B, 128), 1)
    totals = [jnp.zeros((8, 128), jnp.float32) for _ in range(C // 128)]
    part = 64

    def block(k, totals):
        def piece(r, totals):
            rows = pl.ds(pl.multiple_of(k * B + r * part, part), part)
            peak = jnp.broadcast_to(jnp.max(rmax[rows, :], axis=1, keepdims=True), (part, 128))
            rmax[rows, :] = peak
            acc = jnp.zeros((part, 128), jnp.float32)
            out = []
            for n in range(C // 128):
                t = t_v[rows, n * 128:(n + 1) * 128]
                acc = acc + jnp.exp2(t - peak)
                f = jnp.exp2(t.reshape(-1, 8, 128) - cmax[:, n * 128:(n + 1) * 128][None])
                out.append(totals[n] + jnp.sum(f, axis=0))
            pos_b[rows, :] = acc
            return tuple(out)

        return lax.fori_loop(0, B // part, piece, totals)

    totals = lax.fori_loop(0, CAPS, block, tuple(totals))

    for k in range(CAPS):
        rows = pl.ds(k * B, B)
        total = jnp.sum(pos_b[rows, :], axis=1, keepdims=True)
        match = jnp.sum(rmatch[rows, :], axis=1, keepdims=True)
        packed = jnp.where(
            lanes == 0, rmax[rows, :],
            jnp.where(lanes == 1, total, jnp.where(lanes == 2, match, bias_b[rows, :])),
        )
        q = cap_place(p, k)
        to = (q["x"] * 2 + q["c"]) * 2 + q["l"]
        row_out[to, :, :] = jnp.transpose(packed)[0:4, :]

    empty = lax.broadcasted_iota(jnp.int32, (4, B), 0)
    for k in range(16):
        col_out[k, :, :] = jnp.where(empty == 0, 4.0 * LOW, 0.0)
    total = jnp.concatenate(
        [jnp.sum(v, axis=0, keepdims=True) for v in totals], axis=1
    )
    match = jnp.sum(cmatch[...], axis=0, keepdims=True)
    for m in range(IMGS):
        q = img_place(p, m)
        to = (q["h"] * 4 + q["z"]) * 2 + q["l"]
        at = slice(m * B, (m + 1) * B)
        col_out[to, 0:1, :] = top[:, at]
        col_out[to, 1:2, :] = total[:, at]
        col_out[to, 2:3, :] = match[:, at]


def score_tile(table, caps, imgs):
    any_space = pl.BlockSpec(memory_space=pltpu.HBM)
    vmem = pl.BlockSpec(memory_space=pltpu.VMEM)
    f32 = jnp.float32
    return pl.pallas_call(
        scores_kernel,
        out_shape=[
            jax.ShapeDtypeStruct((16, 4, B), f32),
            jax.ShapeDtypeStruct((16, 4, B), f32),
        ],
        in_specs=[vmem] + [any_space] * (CAPS + IMGS),
        out_specs=[vmem, vmem],
        scratch_shapes=[
            pltpu.VMEM((R, E), jnp.bfloat16),
            pltpu.VMEM((C, E), jnp.bfloat16),
            pltpu.VMEM((R, C), f32),
            pltpu.VMEM((R, 128), f32),
            pltpu.VMEM((R, 128), f32),
            pltpu.VMEM((128, 256), f32),
            pltpu.VMEM((8, C), f32),
            pltpu.VMEM((R, 128), f32),
            pltpu.VMEM((R, 128), f32),
            pltpu.VMEM((8, C), f32),
            pltpu.VMEM((8, C), f32),
            pltpu.SemaphoreType.DMA((CAPS + IMGS,)),
        ],
        compiler_params=pltpu.CompilerParams(vmem_limit_bytes=56 * 1024 * 1024),
        cost_estimate=pl.CostEstimate(
            flops=2 * R * C * E, bytes_accessed=2 * (R + C) * E, transcendentals=2 * R * C
        ),
    )(table, *caps, *imgs)


def joined(parts, count):
    peak = jnp.max(parts[:, 0, :], axis=0, keepdims=True)
    total = jnp.sum(parts[:, 1, :] * jnp.exp2(parts[:, 0, :] - peak), axis=0, keepdims=True)
    match = jnp.sum(parts[:, 2, :], axis=0, keepdims=True)
    return LN2 * (peak - match + jnp.log2(total))


def loss_kernel(rows, cols, valid, caption_loss, image_loss, total):
    row_parts, col_parts = rows[...], cols[...]
    ok = row_parts[0:1, 3, :] > 0.5 * LOW
    caption = jnp.where(ok, joined(row_parts, 16), 0.0)
    image = jnp.where(valid[...] > 0, joined(col_parts, 16), 0.0)
    caption_loss[...] = caption
    image_loss[...] = image
    total[...] = jnp.full((128, 8), jnp.sum(caption) + jnp.sum(image), jnp.float32)


def local(captions, images, positives, valid):
    word = positives * 2 + valid
    table = lax.all_to_all(
        jnp.broadcast_to(word[None], (128, B)), AXES, 0, 0, tiled=True
    )
    near_caption = shift(captions, l=1)
    near_image = shift(images, h=1, l=1)
    caps = around(captions, near_caption, "x")
    imgs = around(images, near_image, "z")
    caps = caps + [shift(b, c=1) for b in caps]
    row_parts, col_parts = score_tile(table, caps, imgs)
    rows = lax.all_to_all(row_parts, ("x", "c", "l"), 0, 0, tiled=True)
    cols = lax.all_to_all(col_parts, ("h", "z", "l"), 0, 0, tiled=True)
    f32 = jnp.float32
    vmem = pl.BlockSpec(memory_space=pltpu.VMEM)
    caption_loss, image_loss, total = pl.pallas_call(
        loss_kernel,
        out_shape=[
            jax.ShapeDtypeStruct((1, B), f32),
            jax.ShapeDtypeStruct((1, B), f32),
            jax.ShapeDtypeStruct((128, 8), f32),
        ],
        in_specs=[vmem] * 3,
        out_specs=[vmem] * 3,
    )(rows, cols, valid[None])
    totals = lax.all_to_all(total, AXES, 0, 0, tiled=True)
    count = jnp.sum(table & 1).astype(f32)
    loss = jnp.sum(totals[:, 0]) / (2.0 * count)
    return caption_loss.reshape(B), image_loss.reshape(B), loss


def solution(mesh):
    torus = Mesh(mesh.devices.reshape(*SIZES.values()), AXES)
    return jax.shard_map(
        local,
        mesh=torus,
        in_specs=(P(AXES, None), P(AXES, None), P(AXES), P(AXES)),
        out_specs=(P(AXES), P(AXES), P()),
        check_vma=False,
    )
```

```python
import itertools

import jax
import jax.numpy as jnp
from jax import lax
from jax.experimental import pallas as pl
from jax.experimental.pallas import tpu as pltpu
from jax.sharding import Mesh
from jax.sharding import PartitionSpec as P


SIZES = {"x": 4, "h": 2, "z": 4, "c": 2, "l": 2}
AXES = tuple(SIZES)
LOG2E = 1.4426950408889634
LN2 = 0.6931471805599453
LOW = -1.0e30

B = 192
E = 768
CAPS = 16
IMGS = 8
R = CAPS * B
C = IMGS * B
RC = 512
NC = 256
PIECE = 64
GRAIN = 16
OK_BIT = 15
RANK_BIT = 16
ABSENT = 9999.0

RING = ((0, 0), (0, 1), (3, 0), (3, 1), (1, 0), (1, 1), (2, 0), (2, 1))
CAP_OFFSETS = [(dz, dc, dl) for dc in (0, 1) for dz, dl in RING]
IMG_OFFSETS = RING

F32 = jnp.float32
BF16 = jnp.bfloat16
VMEM = pl.BlockSpec(memory_space=pltpu.VMEM)
SMEM = pl.BlockSpec(memory_space=pltpu.SMEM)


def shift(value, **off):
    axes = tuple(a for a in AXES if off.get(a))
    sizes = [SIZES[a] for a in axes]
    pairs = []
    for at in itertools.product(*map(range, sizes)):
        src = dst = 0
        for i, a, s in zip(at, axes, sizes):
            src, dst = src * s + i, dst * s + (i + off[a]) % s
        pairs.append((src, dst))
    return lax.ppermute(value, axes if len(axes) > 1 else axes[0], pairs)


def neighbours(block, near, axis):
    pair = [block, near]
    return [shift(b, **{axis: step}) for step in (1, 3) for b in pair]


def opposite(sides, axis):
    return [shift(sides[0], **{axis: 1}), shift(sides[3], **{axis: 3})]


def place():
    return {a: lax.axis_index(a) for a in AXES}


def flat(p):
    at = 0
    for a in AXES:
        at = at * SIZES[a] + p[a]
    return at


def moved(p, off):
    q = dict(p)
    for a, d in off.items():
        q[a] = lax.rem(p[a] + d, SIZES[a])
    return q


def cap_place(p, k):
    dz, dc, dl = CAP_OFFSETS[k]
    return moved(p, {"z": dz, "c": dc, "l": dl})


def img_place(p, m):
    dx, dy = IMG_OFFSETS[m]
    return moved(p, {"x": dx, "h": dy, "l": dy})


def iota(shape, dim):
    return lax.broadcasted_iota(jnp.int32, shape, dim).astype(F32)


def dot(a, b):
    return jnp.dot(a, b, preferred_element_type=F32)


def earlier():
    return jnp.where(iota((B, B), 0) < iota((B, B), 1), 1.0, 0.0).astype(BF16)


def grains(n):
    return lax.shift_left(lax.shift_right_logical(n + (GRAIN - 1), 4), 4)


def pack_kernel(images, positives, valid, packed, words, ranks):
    ok = valid[...]
    marks = jnp.broadcast_to(ok, (16, B)).astype(F32).astype(BF16)
    rank = dot(marks, earlier())[0:1, :]
    found = jnp.where(ok > 0, rank, ABSENT)
    pick = jnp.where(iota((B, B), 0) == found, 1.0, 0.0).astype(BF16)
    packed[...] = dot(pick, images[...]).astype(BF16)
    word = positives[...] + ok * (1 << OK_BIT) + rank.astype(jnp.int32) * (1 << RANK_BIT)
    words[...] = jnp.broadcast_to(word, (128, B))
    ranks[...] = found


def lookup_kernel(table, ranks, targets, counts, pos):
    p = place()
    words = table[...]
    ok = (lax.shift_right_logical(words, OK_BIT) & 1).astype(F32)
    rank = lax.shift_right_logical(words, RANK_BIT).astype(F32)
    known = jnp.transpose(jnp.where(ok > 0, rank + 1.0, 0.0)).astype(BF16)
    for k in range(CAPS):
        row = table[pl.ds(flat(cap_place(p, k)), 1), :]
        pos[k:k + 1, :] = (row & ((1 << OK_BIT) - 1)).astype(F32)
    at = pos[...]
    hi = jnp.floor((at + 0.5) * (1.0 / B))
    lo = at - hi * B
    block = iota((128, B), 0)
    inner = iota((B, B), 0)
    for k in range(CAPS):
        pick = jnp.where(block == hi[k:k + 1, :], 1.0, 0.0).astype(BF16)
        column = dot(known, pick)
        pos[k:k + 1, :] = jnp.sum(
            jnp.where(inner == lo[k:k + 1, :], column, 0.0), axis=0, keepdims=True
        )
    value = pos[...]
    live = value > 0.0
    marks = jnp.where(live, 1.0, 0.0)
    order = dot(marks.astype(BF16), earlier())
    ranks[...] = jnp.where(live, order, ABSENT)
    start = jnp.zeros((1, 1), F32)
    base = jnp.full((CAPS, B), -ABSENT, F32)
    counts[0:CAPS, :] = jnp.broadcast_to(
        jnp.sum(marks, axis=1, keepdims=True).astype(jnp.int32), (CAPS, 128)
    )
    for m in range(IMGS):
        number = flat(img_place(p, m))
        row = lax.shift_right_logical(table[pl.ds(number, 1), :], OK_BIT) & 1
        count = jnp.sum(row.astype(F32), axis=1, keepdims=True)
        base = jnp.where(hi == number.astype(F32), start, base)
        start = start + jnp.floor((count + (GRAIN - 1.0)) * (1.0 / GRAIN)) * GRAIN
        counts[CAPS + m:CAPS + m + 1, :] = jnp.broadcast_to(count.astype(jnp.int32), (1, 128))
    targets[...] = jnp.where(live, base + value - 1.0, -ABSENT)


def score_kernel(counts, ranks, targets, *refs):
    caps, imgs = refs[:CAPS], refs[CAPS:CAPS + IMGS]
    row_out, col_out = refs[CAPS + IMGS:CAPS + IMGS + 2]
    (cap_v, img_v, t_v, pos_b, bias_b, rmax, rmatch, rsum, col_bias, cmax,
     cmatch, csum) = refs[CAPS + IMGS + 2:]
    p = place()

    starts, at = [], jnp.int32(0)
    column = iota((8, C), 1)
    bias = jnp.full((8, C), LOW, F32)
    for m in range(IMGS):
        at = pl.multiple_of(at, GRAIN)
        img_v[pl.ds(at, B), :] = imgs[m][...]
        count = counts[CAPS + m, 0]
        first = at.astype(F32)
        inside = (column >= first) & (column < first + count.astype(F32))
        bias = jnp.where(inside, 0.0, bias)
        starts.append(at)
        at = at + grains(count)
    columns = at
    img_v[pl.ds(pl.multiple_of(at, GRAIN), NC), :] = jnp.zeros((NC, E), BF16)
    col_bias[...] = bias

    cap_starts, at = [], jnp.int32(0)
    slot = iota((B, B), 0)
    slot_b = iota((B, 128), 0)
    for k in range(CAPS):
        at = pl.multiple_of(at, GRAIN)
        hit = slot == ranks[k:k + 1, :]
        pick = jnp.where(hit, 1.0, 0.0).astype(BF16)
        cap_v[pl.ds(at, B), :] = dot(pick, caps[k][...]).astype(BF16)
        target = jnp.sum(jnp.where(hit, targets[k:k + 1, :], 0.0), axis=1, keepdims=True)
        pos_b[pl.ds(at, B), :] = jnp.broadcast_to(target, (B, 128))
        count = counts[k, 0]
        bias_b[pl.ds(at, B), :] = jnp.where(slot_b < count.astype(F32), 0.0, LOW)
        cap_starts.append(at)
        at = at + grains(count)
    rows_used = at
    tail = pl.ds(pl.multiple_of(at, GRAIN), RC)
    cap_v[tail, :] = jnp.zeros((RC, E), BF16)
    bias_b[tail, :] = jnp.full((RC, 128), LOW, F32)
    pos_b[tail, :] = jnp.full((RC, 128), -ABSENT, F32)

    cmax[...] = jnp.full(cmax.shape, 4.0 * LOW, F32)
    cmatch[...] = jnp.zeros(cmatch.shape, F32)
    csum[...] = jnp.zeros(csum.shape, F32)
    rmax[...] = jnp.full(rmax.shape, 4.0 * LOW, F32)

    def tiles(count):
        @pl.loop(0, lax.div(rows_used + (RC - 1), RC))
        def _(i):
            rows = pl.ds(pl.multiple_of(i * RC, RC), RC)
            a = cap_v[rows, :]
            for n in range(count):
                s = lax.dot_general(
                    a, img_v[n * NC:(n + 1) * NC, :], (((1,), (1,)), ((), ())),
                    preferred_element_type=F32,
                )
                q = s * LOG2E
                highest, found = None, None
                for half in range(2):
                    span = pl.ds(n * NC + half * 128, 128)
                    qh = q[:, half * 128:(half + 1) * 128]
                    t = (qh + bias_b[rows, :]) + col_bias[0:1, span]
                    t_v[rows, span] = t
                    number = iota((1, 128), 1) + float(n * NC + half * 128)
                    w = jnp.where(pos_b[rows, :] == number, qh, 0.0)
                    highest = t if half == 0 else jnp.maximum(highest, t)
                    found = w if half == 0 else found + w
                    cmax[:, span] = jnp.maximum(
                        cmax[:, span], jnp.max(t.reshape(-1, 8, 128), axis=0)
                    )
                    cmatch[:, span] += jnp.sum(w.reshape(-1, 8, 128), axis=0)
                if n == 0:
                    rmax[rows, :] = highest
                    rmatch[rows, :] = found
                else:
                    rmax[rows, :] = jnp.maximum(rmax[rows, :], highest)
                    rmatch[rows, :] += found
            rmax[rows, :] = jnp.broadcast_to(
                jnp.max(rmax[rows, :], axis=1, keepdims=True), (RC, 128)
            )

        top = jnp.max(cmax[...], axis=0, keepdims=True)
        cmax[...] = jnp.broadcast_to(top, cmax.shape)

        def piece(r, totals):
            rows = pl.ds(pl.multiple_of(r * PIECE, PIECE), PIECE)
            peak = rmax[rows, :]
            acc = jnp.zeros((PIECE, 128), F32)
            out = []
            for n in range(2 * count):
                t = t_v[rows, n * 128:(n + 1) * 128]
                acc = acc + jnp.exp2(t - peak)
                f = jnp.exp2(t.reshape(-1, 8, 128) - cmax[:, n * 128:(n + 1) * 128][None])
                out.append(totals[n] + jnp.sum(f, axis=0))
            rsum[rows, :] = acc
            return tuple(out)

        totals = lax.fori_loop(
            0, lax.div(rows_used + (PIECE - 1), PIECE), piece,
            tuple(jnp.zeros((8, 128), F32) for _ in range(2 * count)),
        )
        for n in range(2 * count):
            csum[:, n * 128:(n + 1) * 128] = totals[n]

    used = jnp.maximum(lax.div(columns + (NC - 1), NC), 1)
    for count in range(1, C // NC + 1):
        pl.when(used == count)(lambda count=count: tiles(count))

    lanes = lax.broadcasted_iota(jnp.int32, (B, 128), 1)
    for k in range(CAPS):
        rows = pl.ds(pl.multiple_of(cap_starts[k], GRAIN), B)
        total = jnp.sum(rsum[rows, :], axis=1, keepdims=True)
        match = jnp.sum(rmatch[rows, :], axis=1, keepdims=True)
        lines = jnp.where(lanes == 0, rmax[rows, :], jnp.where(lanes == 1, total, match))
        q = cap_place(p, k)
        row_out[(q["z"] * 2 + q["c"]) * 2 + q["l"], :, :] = jnp.transpose(lines)[0:4, :]

    empty = lax.broadcasted_iota(jnp.int32, (4, B), 0)
    for k in range(16):
        col_out[k, :, :] = jnp.where(empty == 0, 4.0 * LOW, 0.0)
    line = lax.broadcasted_iota(jnp.int32, (8, C + NC), 0)
    wide = lambda v: jnp.concatenate([v, jnp.zeros((1, NC), F32)], axis=1)
    stats = jnp.where(
        line == 0, wide(cmax[0:1, :]),
        jnp.where(
            line == 1, wide(jnp.sum(csum[...], axis=0, keepdims=True)),
            wide(jnp.sum(cmatch[...], axis=0, keepdims=True)),
        ),
    )
    for m in range(IMGS):
        q = img_place(p, m)
        mine = pltpu.roll(stats, lax.rem((C + NC) - starts[m], C + NC), 1)
        col_out[(q["x"] * 2 + q["h"]) * 2 + q["l"], :, :] = mine[0:4, :B]


def joined(parts, ranks):
    peak = jnp.max(parts[:, 0, :], axis=0, keepdims=True)
    total = jnp.sum(parts[:, 1, :] * jnp.exp2(parts[:, 0, :] - peak), axis=0, keepdims=True)
    match = jnp.sum(parts[:, 2, :], axis=0, keepdims=True)
    packed = jnp.broadcast_to(LN2 * (peak - match + jnp.log2(total)), (8, B))
    packed = jnp.concatenate([packed, jnp.zeros((8, 256 - B), F32)], axis=1)
    column = jnp.transpose(packed)[:B, 0:1]
    return jnp.sum(jnp.where(iota((B, B), 0) == ranks, column, 0.0), axis=0, keepdims=True)


def loss_kernel(rows, cols, row_ranks, col_ranks, caption_loss, image_loss, total):
    caption = joined(rows[...], row_ranks[0:1, :])
    image = joined(cols[...], col_ranks[...])
    caption_loss[...] = caption
    image_loss[...] = image
    total[...] = jnp.full((128, 8), jnp.sum(caption) + jnp.sum(image), F32)


def score_tile(counts, ranks, targets, caps, imgs):
    return pl.pallas_call(
        score_kernel,
        out_shape=[jax.ShapeDtypeStruct((16, 4, B), F32)] * 2,
        in_specs=[SMEM] + [VMEM] * (2 + CAPS + IMGS),
        out_specs=[VMEM, VMEM],
        scratch_shapes=[
            pltpu.VMEM((R + RC, E), BF16),
            pltpu.VMEM((C + NC, E), BF16),
            pltpu.VMEM((R, C), F32),
            pltpu.VMEM((R + RC, 128), F32),
            pltpu.VMEM((R + RC, 128), F32),
            pltpu.VMEM((R + RC, 128), F32),
            pltpu.VMEM((R + RC, 128), F32),
            pltpu.VMEM((R + RC, 128), F32),
            pltpu.VMEM((8, C), F32),
            pltpu.VMEM((8, C), F32),
            pltpu.VMEM((8, C), F32),
            pltpu.VMEM((8, C), F32),
        ],
        compiler_params=pltpu.CompilerParams(vmem_limit_bytes=48 * 1024 * 1024),
        cost_estimate=pl.CostEstimate(
            flops=R * C * E, bytes_accessed=2 * (R + C) * E, transcendentals=R * C
        ),
    )(counts, ranks, targets, *caps, *imgs)


def local(captions, images, positives, valid):
    shape = jax.ShapeDtypeStruct
    packed, words, image_ranks = pl.pallas_call(
        pack_kernel,
        out_shape=[shape((B, E), BF16), shape((128, B), jnp.int32), shape((1, B), F32)],
        in_specs=[VMEM] * 3,
        out_specs=[VMEM] * 3,
        cost_estimate=pl.CostEstimate(flops=2 * B * B * E, bytes_accessed=4 * B * E, transcendentals=0),
    )(images, positives[None], valid[None])
    near_caption = shift(captions, l=1)
    near_image = shift(packed, h=1, l=1)
    words, near_caption, near_image = lax.optimization_barrier((words, near_caption, near_image))
    table = lax.all_to_all(words, AXES, 0, 0, tiled=True)
    cap_sides = neighbours(captions, near_caption, "z")
    img_sides = neighbours(packed, near_image, "x")
    (cap_sides[0], cap_sides[3], img_sides[0], img_sides[3], table) = lax.optimization_barrier(
        (cap_sides[0], cap_sides[3], img_sides[0], img_sides[3], table)
    )
    ranks, targets, counts = pl.pallas_call(
        lookup_kernel,
        out_shape=[shape((CAPS, B), F32), shape((CAPS, B), F32), shape((24, 128), jnp.int32)],
        in_specs=[VMEM],
        out_specs=[VMEM] * 3,
        scratch_shapes=[pltpu.VMEM((CAPS, B), F32)],
        cost_estimate=pl.CostEstimate(flops=10**9, bytes_accessed=10**6, transcendentals=0),
    )(table)
    caps = [captions, near_caption, *cap_sides, *opposite(cap_sides, "z")]
    imgs = [packed, near_image, *img_sides, *opposite(img_sides, "x")]
    caps = caps + [shift(b, c=1) for b in caps]
    row_parts, col_parts = score_tile(counts, ranks, targets, caps, imgs)
    rows = lax.all_to_all(row_parts, ("z", "c", "l"), 0, 0, tiled=True)
    cols = lax.all_to_all(col_parts, ("x", "h", "l"), 0, 0, tiled=True)
    caption_loss, image_loss, total = pl.pallas_call(
        loss_kernel,
        out_shape=[shape((1, B), F32), shape((1, B), F32), shape((128, 8), F32)],
        in_specs=[VMEM] * 4,
        out_specs=[VMEM] * 3,
    )(rows, cols, ranks, image_ranks)
    totals = lax.all_to_all(total, AXES, 0, 0, tiled=True)
    count = jnp.sum(lax.shift_right_logical(table, OK_BIT) & 1).astype(F32)
    loss = jnp.sum(totals[:, 0]) / (2.0 * count)
    return caption_loss.reshape(B), image_loss.reshape(B), loss


def solution(mesh):
    torus = Mesh(mesh.devices.reshape(*SIZES.values()), AXES)
    return jax.shard_map(
        local,
        mesh=torus,
        in_specs=(P(AXES, None), P(AXES, None), P(AXES), P(AXES)),
        out_specs=(P(AXES), P(AXES), P()),
        check_vma=False,
    )
```

```python
import itertools

import jax
import jax.numpy as jnp
from jax import lax
from jax.experimental import pallas as pl
from jax.experimental.pallas import tpu as pltpu
from jax.sharding import Mesh
from jax.sharding import PartitionSpec as P


SIZES = {"x": 4, "h": 2, "z": 4, "c": 2, "l": 2}
AXES = tuple(SIZES)
LOG2E = 1.4426950408889634
LN2 = 0.6931471805599453
LOW = -1.0e30

B = 192
E = 768
MET = ((0, 0), (0, 1), (3, 0), (1, 0), (3, 1), (1, 1), (2, 0), (2, 1))
EARLY = 6
CAPS = len(MET)
IMGS = 2 * len(MET)
C = IMGS * B
RC = 448
R = -(-CAPS * B // RC) * RC
NC = 256
COUNTS = (2, 4, 5, 6, 7, 8, 10, 12)
PIECE = 64
GRAIN = 16
OK_BIT = 15
ABSENT = 9999.0

F32 = jnp.float32
BF16 = jnp.bfloat16
VMEM = pl.BlockSpec(memory_space=pltpu.VMEM)
SMEM = pl.BlockSpec(memory_space=pltpu.SMEM)


def send(value, to):
    pairs = []
    for at in itertools.product(*map(range, SIZES.values())):
        p = dict(zip(AXES, at))
        pairs.append((flat(p), flat({**p, **to(p)})))
    return lax.ppermute(value, AXES, pairs)


def other_core(p):
    return {"c": 1 - p["c"]}


def partner(p):
    return {"l": 1 - p["l"], "h": p["h"] ^ p["c"]}


def along(step):
    def to(p):
        axis = "x" if p["c"] else "z"
        return {axis: (p[axis] + step) % 4}

    return to


def place():
    return {a: lax.axis_index(a) for a in AXES}


def flat(p):
    at = 0
    for a in AXES:
        at = at * SIZES[a] + p[a]
    return at


def moved(p, off):
    q = dict(p)
    for a, d in off.items():
        q[a] = lax.rem(p[a] + d, SIZES[a])
    return q


def cap_place(p, k):
    step, y = MET[k]
    return moved(p, {"z": step, "l": y})


def img_place(p, m):
    step, y = MET[m // 2]
    return {**moved(p, {"x": step, "h": y, "l": y}), "c": m % 2}


def iota(shape, dim):
    return lax.broadcasted_iota(jnp.int32, shape, dim).astype(F32)


def dot(a, b):
    return jnp.dot(a, b, preferred_element_type=F32)


def earlier():
    return jnp.where(iota((B, B), 0) < iota((B, B), 1), 1.0, 0.0).astype(BF16)


def grains(n):
    return lax.shift_left(lax.shift_right_logical(n + (GRAIN - 1), 4), 4)


def pair_kernel(
    cap, img, positives, valid, cap_other, img_other, valid_other,
    carried, kept, words, ranks,
):
    first = lax.axis_index("c") == 0
    ok = jnp.concatenate([valid[...], valid_other[...]], axis=0)
    order = dot(jnp.broadcast_to(ok[:, None], (2, 8, B)).reshape(16, B).astype(F32).astype(BF16), earlier())
    found = jnp.where(ok > 0, jnp.concatenate([order[0:1], order[8:9]], axis=0), ABSENT)
    ranks[...] = found[0:1, :]
    words[...] = jnp.broadcast_to(
        positives[...] + valid[...] * (1 << OK_BIT), (128, B)
    ).reshape(128, 1, B)
    packed = []
    for i, block in enumerate((img, img_other)):
        pick = jnp.where(iota((B, B), 0) == found[i:i + 1, :], 1.0, 0.0).astype(BF16)
        packed.append(dot(pick, block[...]).astype(BF16))
    carried[0:B, :] = jnp.where(first, cap[...], packed[1])
    carried[B:2 * B, :] = jnp.where(first, cap_other[...], packed[0])
    kept[0:B, :] = jnp.where(first, packed[0], cap_other[...])
    kept[B:2 * B, :] = jnp.where(first, packed[1], cap[...])


def lookup_kernel(table, ranks, columns, counts, real, pos, words_v):
    p = place()
    words = table[...].reshape(128, B)
    words_v[...] = words
    ok = (lax.shift_right_logical(words, OK_BIT) & 1).astype(F32)
    rank = dot(ok.astype(BF16), earlier())
    real[...] = jnp.full((8, 128), jnp.sum(ok), F32)
    known = jnp.transpose(jnp.where(ok > 0, rank + 1.0, 0.0)).astype(BF16)
    for k in range(CAPS):
        row = words_v[pl.ds(flat(cap_place(p, k)), 1), :]
        pos[k:k + 1, :] = (row & ((1 << OK_BIT) - 1)).astype(F32)
    at = pos[...]
    hi = jnp.floor((at + 0.5) * (1.0 / B))
    lo = at - hi * B
    block = iota((128, B), 0)
    inner = iota((B, B), 0)
    for k in range(CAPS):
        pick = jnp.where(block == hi[k:k + 1, :], 1.0, 0.0).astype(BF16)
        column = dot(known, pick)
        pos[k:k + 1, :] = jnp.sum(
            jnp.where(inner == lo[k:k + 1, :], column, 0.0), axis=0, keepdims=True
        )
    value = pos[...]
    live = value > 0.0
    marks = jnp.where(live, 1.0, 0.0)
    order = dot(marks.astype(BF16), earlier())
    ranks[...] = jnp.where(live, order, ABSENT)
    start = jnp.zeros((1, 1), F32)
    base = jnp.full((CAPS, B), -ABSENT, F32)
    counts[0:CAPS, :] = jnp.broadcast_to(
        jnp.sum(marks, axis=1, keepdims=True).astype(jnp.int32), (CAPS, 128)
    )
    for m in range(IMGS):
        number = flat(img_place(p, m))
        row = words_v[pl.ds(number, 1), :]
        row = lax.shift_right_logical(row, OK_BIT) & 1
        count = jnp.sum(row.astype(F32), axis=1, keepdims=True)
        base = jnp.where(hi == number.astype(F32), start, base)
        start = start + jnp.floor((count + (GRAIN - 1.0)) * (1.0 / GRAIN)) * GRAIN
        counts[CAPS + m:CAPS + m + 1, :] = jnp.broadcast_to(count.astype(jnp.int32), (1, 128))
    targets = jnp.where(live, base + value - 1.0, -ABSENT)
    order = ranks[...]
    lane = iota((B, 128), 1)
    result = jnp.zeros((B, 128), F32)
    for k in range(CAPS):
        hit = inner == order[k:k + 1, :]
        target = jnp.sum(jnp.where(hit, targets[k:k + 1, :], 0.0), axis=1, keepdims=True)
        result = jnp.where(lane == float(k), target, result)
    columns[...] = result


def starts_of(counts, first, number):
    found, at = [], jnp.int32(0)
    for k in range(number):
        found.append(pl.multiple_of(at, GRAIN))
        at = at + grains(counts[first + k, 0])
    return found + [pl.multiple_of(at, GRAIN)]


def compact(counts, ranks, carried, kept, cap_out, img_out, first):
    core = lax.axis_index("c")
    slot = iota((B, B), 0)
    at = starts_of(counts, 0, CAPS)
    for k, (a, b) in enumerate(zip(carried, kept), first):
        block = jnp.where(core == 0, a[0:B, :], b[B:2 * B, :])
        pick = jnp.where(slot == ranks[k:k + 1, :], 1.0, 0.0).astype(BF16)
        cap_out[pl.ds(at[k], B), :] = dot(pick, block).astype(BF16)
    at = starts_of(counts, CAPS, IMGS)
    for k, (a, b) in enumerate(zip(carried, kept), first):
        for side in range(2):
            rows = pl.ds(side * B, B)
            img_out[pl.ds(at[2 * k + side], B), :] = jnp.where(core == 0, b[rows, :], a[rows, :])


def early_kernel(counts, ranks, *refs):
    cap_out, img_out = refs[2 * EARLY:]
    cap_out[...] = jnp.zeros(cap_out.shape, BF16)
    img_out[...] = jnp.zeros(img_out.shape, BF16)
    compact(counts, ranks, refs[:EARLY], refs[EARLY:2 * EARLY], cap_out, img_out, 0)


def late_kernel(counts, ranks, cap_in, img_in, *refs):
    del cap_in, img_in
    late = CAPS - EARLY
    cap_out, img_out = refs[2 * late:]
    compact(counts, ranks, refs[:late], refs[late:2 * late], cap_out, img_out, EARLY)


def score_kernel(
    counts, columns, cap_v, img_v, out, own_row,
    t_v, pos_b, bias_b, rmax, rmatch, rsum, col_bias, cmax, cmatch, csum, lines_v,
):
    img_at = starts_of(counts, CAPS, IMGS)
    column = iota((8, C), 1)
    bias = jnp.full((8, C), LOW, F32)
    for m in range(IMGS):
        begin = img_at[m].astype(F32)
        end = begin + counts[CAPS + m, 0].astype(F32)
        bias = jnp.where((column >= begin) & (column < end), 0.0, bias)
    col_bias[...] = bias
    cap_at = starts_of(counts, 0, CAPS)
    slot = iota((B, 128), 0)
    for k in range(CAPS):
        rows = pl.ds(cap_at[k], B)
        pos_b[rows, :] = jnp.broadcast_to(columns[:, k:k + 1], (B, 128))
        bias_b[rows, :] = jnp.where(slot < counts[k, 0].astype(F32), 0.0, LOW)
    rows_used = cap_at[CAPS]
    tail = pl.ds(rows_used, RC)
    bias_b[tail, :] = jnp.full((RC, 128), LOW, F32)
    pos_b[tail, :] = jnp.full((RC, 128), -ABSENT, F32)
    cmax[...] = jnp.full(cmax.shape, 4.0 * LOW, F32)
    cmatch[...] = jnp.zeros(cmatch.shape, F32)
    csum[...] = jnp.zeros(csum.shape, F32)

    def tiles(count):
        @pl.loop(0, lax.div(rows_used + (RC - 1), RC))
        def _(i):
            rows = pl.ds(pl.multiple_of(i * RC, RC), RC)
            a = cap_v[rows, :]
            for n in range(count):
                s = lax.dot_general(
                    a, img_v[n * NC:(n + 1) * NC, :], (((1,), (1,)), ((), ())),
                    preferred_element_type=F32,
                )
                q = s * LOG2E
                highest, found = None, None
                for half in range(2):
                    span = pl.ds(n * NC + half * 128, 128)
                    qh = q[:, half * 128:(half + 1) * 128]
                    t = (qh + bias_b[rows, :]) + col_bias[0:1, span]
                    t_v[rows, span] = t
                    number = iota((1, 128), 1) + float(n * NC + half * 128)
                    w = jnp.where(pos_b[rows, :] == number, qh, 0.0)
                    highest = t if half == 0 else jnp.maximum(highest, t)
                    found = w if half == 0 else found + w
                    cmax[:, span] = jnp.maximum(
                        cmax[:, span], jnp.max(t.reshape(-1, 8, 128), axis=0)
                    )
                    cmatch[:, span] += jnp.sum(w.reshape(-1, 8, 128), axis=0)
                if n == 0:
                    rmax[rows, :] = highest
                    rmatch[rows, :] = found
                else:
                    rmax[rows, :] = jnp.maximum(rmax[rows, :], highest)
                    rmatch[rows, :] += found
            rmax[rows, :] = jnp.broadcast_to(
                jnp.max(rmax[rows, :], axis=1, keepdims=True), (RC, 128)
            )

        top = jnp.max(cmax[...], axis=0, keepdims=True)
        cmax[...] = jnp.broadcast_to(top, cmax.shape)

        def piece(r, totals):
            rows = pl.ds(pl.multiple_of(r * PIECE, PIECE), PIECE)
            peak = rmax[rows, :]
            acc = jnp.zeros((PIECE, 128), F32)
            out = []
            for n in range(2 * count):
                t = t_v[rows, n * 128:(n + 1) * 128]
                acc = acc + jnp.exp2(t - peak)
                f = jnp.exp2(t.reshape(-1, 8, 128) - cmax[:, n * 128:(n + 1) * 128][None])
                out.append(totals[n] + jnp.sum(f, axis=0))
            rsum[rows, :] = acc
            return tuple(out)

        totals = lax.fori_loop(
            0, lax.div(rows_used + (PIECE - 1), PIECE), piece,
            tuple(jnp.zeros((8, 128), F32) for _ in range(2 * count)),
        )
        for n in range(2 * count):
            csum[:, n * 128:(n + 1) * 128] = totals[n]

    used = jnp.maximum(lax.div(img_at[IMGS] + (NC - 1), NC), 1)
    for below, count in zip((0, *COUNTS), COUNTS):
        pl.when((used > below) & (used <= count))(lambda count=count: tiles(count))

    p = place()
    lanes = lax.broadcasted_iota(jnp.int32, (B, 128), 1)
    for k in range(CAPS):
        rows = pl.ds(cap_at[k], B)
        total = jnp.sum(rsum[rows, :], axis=1, keepdims=True)
        match = jnp.sum(rmatch[rows, :], axis=1, keepdims=True)
        packed = jnp.where(lanes == 0, rmax[rows, :] + jnp.log2(total), match)
        lines = jnp.transpose(packed)
        if k:
            put(out, flat(cap_place(p, k)), lines)
        else:
            put(own_row, 0, lines)
    line = lax.broadcasted_iota(jnp.int32, (8, C), 0)
    total = jnp.sum(csum[...], axis=0, keepdims=True)
    match = jnp.sum(cmatch[...], axis=0, keepdims=True)
    lines_v[:, :C] = jnp.where(line == 0, cmax[0:1, :] + jnp.log2(total), match)
    lines_v[:, C:] = jnp.zeros((8, 384), F32)
    for m in range(IMGS):
        whole = lax.shift_left(lax.shift_right_logical(img_at[m], 7), 7)
        slab = lines_v[:, pl.ds(pl.multiple_of(whole, 128), 384)]
        slab = pltpu.roll(slab, lax.rem(384 - (img_at[m] - whole), 384), 1)
        put(out, flat(img_place(p, m)), slab)


def put(out, at, lines):
    for i in range(2):
        out[at, 0:1, i * B:(i + 1) * B] = lines[i:i + 1, :B]


def joined(parts, ranks):
    sums, matches = parts[:, :B], parts[:, B:]
    peak = jnp.max(sums, axis=0, keepdims=True)
    total = jnp.sum(jnp.exp2(sums - peak), axis=0, keepdims=True)
    match = jnp.sum(matches, axis=0, keepdims=True)
    packed = jnp.broadcast_to(LN2 * (peak - match + jnp.log2(total)), (8, B))
    packed = jnp.concatenate([packed, jnp.zeros((8, 256 - B), F32)], axis=1)
    column = jnp.transpose(packed)[:B, 0:1]
    return jnp.sum(jnp.where(iota((B, B), 0) == ranks, column, 0.0), axis=0, keepdims=True)


def loss_kernel(
    parts, own_row, row_ranks, col_ranks, real, caption_loss, image_loss, total, rows, cols
):
    p = place()
    rows[0:1, :] = own_row[0, :, :]
    for k in range(1, CAPS):
        rows[k:k + 1, :] = parts[flat(cap_place(p, k)), :, :]
    for m in range(IMGS):
        cols[m:m + 1, :] = parts[flat(img_place(p, m)), :, :]
    caption = joined(rows[...], row_ranks[0:1, :])
    image = joined(cols[...], col_ranks[...])
    caption_loss[...] = caption
    image_loss[...] = image
    both = jnp.sum(caption, axis=1, keepdims=True) + jnp.sum(image, axis=1, keepdims=True)
    share = both / (2.0 * real[0:1, 0:1])
    total[...] = jnp.broadcast_to(share, (128, 8)).reshape(128, 1, 8)


def small(mib, flops):
    return dict(
        compiler_params=pltpu.CompilerParams(vmem_limit_bytes=mib * 1024 * 1024),
        cost_estimate=pl.CostEstimate(flops=flops, bytes_accessed=10**6, transcendentals=0),
    )


def step(captions, images, positives, valid):
    shape = jax.ShapeDtypeStruct
    pair = shape((2 * B, E), BF16)
    others = [send(value, other_core) for value in (captions, images, valid[None])]
    carried, kept, words, image_ranks = pl.pallas_call(
        pair_kernel,
        out_shape=[pair, pair, shape((128, 1, B), jnp.int32), shape((1, B), F32)],
        in_specs=[VMEM] * 7,
        out_specs=[VMEM] * 4,
        **small(8, 10**8),
    )(captions, images, positives[None], valid[None], *others)
    near = send(carried, partner)
    a1, a3 = (send(carried, along(s)) for s in (1, 3))
    b1, b3 = (send(near, along(s)) for s in (1, 3))
    c1, c3 = send(a1, along(1)), send(b3, along(3))
    met = dict(y=near, a1=a1, a3=a3, b1=b1, b3=b3, c1=c1, c3=c3)
    swapped = [kept] + [send(v, other_core) for v in met.values()]
    carried = [carried, *met.values()]
    table = lax.all_to_all(words, AXES, 0, 0, tiled=True)
    ranks, columns, counts, real = pl.pallas_call(
        lookup_kernel,
        out_shape=[
            shape((CAPS, B), F32), shape((B, 128), F32),
            shape((CAPS + IMGS, 128), jnp.int32), shape((8, 128), F32),
        ],
        in_specs=[VMEM],
        out_specs=[VMEM] * 4,
        scratch_shapes=[pltpu.VMEM((CAPS, B), F32), pltpu.VMEM((128, B), jnp.int32)],
        **small(4, 3 * 10**9),
    )(table)
    packed_shapes = [shape((R, E), BF16), shape((C, E), BF16)]
    cap_v, img_v = pl.pallas_call(
        early_kernel,
        out_shape=packed_shapes,
        in_specs=[SMEM] + [VMEM] * (1 + 2 * EARLY),
        out_specs=[VMEM] * 2,
        **small(12, 2 * 10**9),
    )(counts, ranks, *carried[:EARLY], *swapped[:EARLY])
    cap_v, img_v = pl.pallas_call(
        late_kernel,
        out_shape=packed_shapes,
        in_specs=[SMEM] + [VMEM] * (3 + 2 * (CAPS - EARLY)),
        out_specs=[VMEM] * 2,
        input_output_aliases={2: 0, 3: 1},
        **small(12, 5 * 10**8),
    )(counts, ranks, cap_v, img_v, *carried[EARLY:], *swapped[EARLY:])
    out, own_row = pl.pallas_call(
        score_kernel,
        out_shape=[shape((n, 1, 2 * B), F32) for n in (128, 1)],
        in_specs=[SMEM] + [VMEM] * 3,
        out_specs=[VMEM] * 2,
        scratch_shapes=[
            pltpu.VMEM((R, C), F32),
            *[pltpu.VMEM((R + RC, 128), F32)] * 5,
            *[pltpu.VMEM((8, C), F32)] * 4,
            pltpu.VMEM((8, C + 384), F32),
        ],
        compiler_params=pltpu.CompilerParams(vmem_limit_bytes=36 * 1024 * 1024),
        cost_estimate=pl.CostEstimate(
            flops=R * C * E, bytes_accessed=2 * (R + C) * E, transcendentals=R * C
        ),
    )(counts, columns, cap_v, img_v)
    parts = lax.all_to_all(out, AXES, 0, 0, tiled=True)
    caption_loss, image_loss, total = pl.pallas_call(
        loss_kernel,
        out_shape=[shape((1, B), F32), shape((1, B), F32), shape((128, 1, 8), F32)],
        in_specs=[VMEM] * 5,
        out_specs=[VMEM] * 3,
        scratch_shapes=[pltpu.VMEM((CAPS, 2 * B), F32), pltpu.VMEM((IMGS, 2 * B), F32)],
        **small(4, 10**8),
    )(parts, own_row, ranks, image_ranks, real)
    totals = lax.all_to_all(total, AXES, 0, 0, tiled=True)
    return caption_loss.reshape(B), image_loss.reshape(B), jnp.sum(totals[:, 0, 0])


def solution(mesh):
    torus = Mesh(mesh.devices.reshape(*SIZES.values()), AXES)
    return jax.shard_map(
        step,
        mesh=torus,
        in_specs=(P(AXES, None), P(AXES, None), P(AXES), P(AXES)),
        out_specs=(P(AXES), P(AXES), P()),
        check_vma=False,
    )
```

```python
import functools
import itertools

import jax
import jax.numpy as jnp
from jax import lax
from jax.experimental import pallas as pl
from jax.experimental.pallas import tpu as pltpu
from jax.sharding import Mesh
from jax.sharding import PartitionSpec as P


SIZES = {"x": 4, "h": 2, "z": 4, "c": 2, "l": 2}
AXES = tuple(SIZES)
LOG2E = 1.4426950408889634
LN2 = 0.6931471805599453
LOW = -1.0e30

B = 192
E = 768
MET = ((0, 0), (0, 1), (3, 0), (1, 0), (3, 1), (1, 1), (2, 0), (2, 1))
PARTS = ((0, 4), (4, 6), (6, 8))
CAPS = len(MET)
IMGS = 2 * len(MET)
C = IMGS * B
RC = 448
R = -(-CAPS * B // RC) * RC
CAP_ROWS = CAPS * B + RC
NC = 256
COUNTS = (2, 4, 5, 6, 7, 8, 10, 12)
TAIL = 2 * NC
IMG_ROWS = C + TAIL
PIECE = 64
GRAIN = 16
OK_BIT = 15
ABSENT = 9999.0

F32 = jnp.float32
BF16 = jnp.bfloat16
VMEM = pl.BlockSpec(memory_space=pltpu.VMEM)
SMEM = pl.BlockSpec(memory_space=pltpu.SMEM)


def send(value, to):
    pairs = []
    for at in itertools.product(*map(range, SIZES.values())):
        p = dict(zip(AXES, at))
        pairs.append((flat(p), flat({**p, **to(p)})))
    return lax.ppermute(value, AXES, pairs)


def other_core(p):
    return {"c": 1 - p["c"]}


def partner(p):
    return {"l": 1 - p["l"], "h": p["h"] ^ p["c"]}


def along(step):
    def to(p):
        axis = "x" if p["c"] else "z"
        return {axis: (p[axis] + step) % 4}

    return to


def place():
    return {a: lax.axis_index(a) for a in AXES}


def flat(p):
    at = 0
    for a in AXES:
        at = at * SIZES[a] + p[a]
    return at


def moved(p, off):
    q = dict(p)
    for a, d in off.items():
        q[a] = lax.rem(p[a] + d, SIZES[a])
    return q


def cap_place(p, k):
    step, y = MET[k]
    return moved(p, {"z": step, "l": y})


def img_place(p, m):
    step, y = MET[m // 2]
    return {**moved(p, {"x": step, "h": y, "l": y}), "c": m % 2}


def iota(shape, dim):
    return lax.broadcasted_iota(jnp.int32, shape, dim).astype(F32)


def dot(a, b):
    return jnp.dot(a, b, preferred_element_type=F32)


def earlier():
    return jnp.where(iota((B, B), 0) < iota((B, B), 1), 1.0, 0.0).astype(BF16)


def grains(n):
    return lax.shift_left(lax.shift_right_logical(n + (GRAIN - 1), 4), 4)


def pair_kernel(
    cap, img, word, cap_other, img_other, word_other, carried, kept, words, ranks
):
    first = lax.axis_index("c") == 0
    ok = lax.shift_right_logical(
        jnp.concatenate([word[...], word_other[...]], axis=0), OK_BIT
    )
    order = dot(jnp.broadcast_to(ok[:, None], (2, 8, B)).reshape(16, B).astype(F32).astype(BF16), earlier())
    found = jnp.where(ok > 0, jnp.concatenate([order[0:1], order[8:9]], axis=0), ABSENT)
    ranks[...] = found[0:1, :]
    words[...] = jnp.broadcast_to(word[...], (128, B)).reshape(128, 1, B)
    packed = []
    for i, block in enumerate((img, img_other)):
        pick = jnp.where(iota((B, B), 0) == found[i:i + 1, :], 1.0, 0.0).astype(BF16)
        packed.append(dot(pick, block[...]).astype(BF16))
    carried[0:B, :] = jnp.where(first, cap[...], packed[1])
    carried[B:2 * B, :] = jnp.where(first, cap_other[...], packed[0])
    kept[0:B, :] = jnp.where(first, packed[0], cap_other[...])
    kept[B:2 * B, :] = jnp.where(first, packed[1], cap[...])


def lookup_kernel(table, ranks, columns, counts, real, pos, words_v):
    p = place()
    words = table[...].reshape(128, B)
    words_v[...] = words
    ok = (lax.shift_right_logical(words, OK_BIT) & 1).astype(F32)
    rank = dot(ok.astype(BF16), earlier())
    real[...] = jnp.full((8, 128), jnp.sum(ok), F32)
    known = jnp.transpose(jnp.where(ok > 0, rank + 1.0, 0.0)).astype(BF16)
    for k in range(CAPS):
        row = words_v[pl.ds(flat(cap_place(p, k)), 1), :]
        pos[k:k + 1, :] = (row & ((1 << OK_BIT) - 1)).astype(F32)
    at = pos[...]
    hi = jnp.floor((at + 0.5) * (1.0 / B))
    lo = at - hi * B
    block = iota((128, B), 0)
    inner = iota((B, B), 0)
    for k in range(CAPS):
        pick = jnp.where(block == hi[k:k + 1, :], 1.0, 0.0).astype(BF16)
        column = dot(known, pick)
        pos[k:k + 1, :] = jnp.sum(
            jnp.where(inner == lo[k:k + 1, :], column, 0.0), axis=0, keepdims=True
        )
    value = pos[...]
    live = value > 0.0
    marks = jnp.where(live, 1.0, 0.0)
    order = dot(marks.astype(BF16), earlier())
    ranks[...] = jnp.where(live, order, ABSENT)
    start = jnp.zeros((1, 1), F32)
    base = jnp.full((CAPS, B), -ABSENT, F32)
    counts[0:CAPS, :] = jnp.broadcast_to(
        jnp.sum(marks, axis=1, keepdims=True).astype(jnp.int32), (CAPS, 128)
    )
    for m in range(IMGS):
        number = flat(img_place(p, m))
        row = words_v[pl.ds(number, 1), :]
        row = lax.shift_right_logical(row, OK_BIT) & 1
        count = jnp.sum(row.astype(F32), axis=1, keepdims=True)
        base = jnp.where(hi == number.astype(F32), start, base)
        start = start + jnp.floor((count + (GRAIN - 1.0)) * (1.0 / GRAIN)) * GRAIN
        counts[CAPS + m:CAPS + m + 1, :] = jnp.broadcast_to(count.astype(jnp.int32), (1, 128))
    targets = jnp.where(live, base + value - 1.0, -ABSENT)
    order = ranks[...]
    lane = iota((B, 128), 1)
    result = jnp.zeros((B, 128), F32)
    for k in range(CAPS):
        hit = inner == order[k:k + 1, :]
        target = jnp.sum(jnp.where(hit, targets[k:k + 1, :], 0.0), axis=1, keepdims=True)
        result = jnp.where(lane == float(k), target, result)
    columns[...] = result


def starts_of(counts, first, number):
    found, at = [], jnp.int32(0)
    for k in range(number):
        found.append(pl.multiple_of(at, GRAIN))
        at = at + grains(counts[first + k, 0])
    return found + [pl.multiple_of(at, GRAIN)]


def compact(counts, ranks, carried, kept, cap_out, img_out, first):
    core = lax.axis_index("c")
    slot = iota((B, B), 0)
    at = starts_of(counts, 0, CAPS)
    for k, (a, b) in enumerate(zip(carried, kept), first):
        block = jnp.where(core == 0, a[0:B, :], b[B:2 * B, :])
        pick = jnp.where(slot == ranks[k:k + 1, :], 1.0, 0.0).astype(BF16)
        cap_out[pl.ds(at[k], B), :] = dot(pick, block).astype(BF16)
    at = starts_of(counts, CAPS, IMGS)
    for k, (a, b) in enumerate(zip(carried, kept), first):
        for side in range(2):
            rows = pl.ds(side * B, B)
            img_out[pl.ds(at[2 * k + side], B), :] = jnp.where(core == 0, b[rows, :], a[rows, :])


def compact_kernel(part, counts, ranks, *refs):
    first, last = PARTS[part]
    refs = refs[2 if part else 0:]
    number = last - first
    cap_out, img_out = refs[2 * number:]
    compact(counts, ranks, refs[:number], refs[number:2 * number], cap_out, img_out, first)
    if last == CAPS:
        cap_end = starts_of(counts, 0, CAPS)[-1]
        img_end = starts_of(counts, CAPS, IMGS)[-1]
        cap_out[pl.ds(cap_end, RC), :] = jnp.zeros((RC, E), BF16)
        img_out[pl.ds(img_end, TAIL), :] = jnp.zeros((TAIL, E), BF16)


def score_kernel(
    counts, columns, cap_v, img_v, out, own_row,
    t_v, pos_b, bias_b, rmax, rmatch, rsum, col_bias, cmax, cmatch, csum, lines_v,
):
    img_at = starts_of(counts, CAPS, IMGS)
    column = iota((8, C), 1)
    bias = jnp.full((8, C), LOW, F32)
    for m in range(IMGS):
        begin = img_at[m].astype(F32)
        end = begin + counts[CAPS + m, 0].astype(F32)
        bias = jnp.where((column >= begin) & (column < end), 0.0, bias)
    col_bias[...] = bias
    cap_at = starts_of(counts, 0, CAPS)
    slot = iota((B, 128), 0)
    for k in range(CAPS):
        rows = pl.ds(cap_at[k], B)
        pos_b[rows, :] = jnp.broadcast_to(columns[:, k:k + 1], (B, 128))
        bias_b[rows, :] = jnp.where(slot < counts[k, 0].astype(F32), 0.0, LOW)
    rows_used = cap_at[CAPS]
    tail = pl.ds(rows_used, RC)
    bias_b[tail, :] = jnp.full((RC, 128), LOW, F32)
    pos_b[tail, :] = jnp.full((RC, 128), -ABSENT, F32)
    cmax[...] = jnp.full(cmax.shape, 4.0 * LOW, F32)
    cmatch[...] = jnp.zeros(cmatch.shape, F32)
    csum[...] = jnp.zeros(csum.shape, F32)

    def tiles(count):
        @pl.loop(0, lax.div(rows_used + (RC - 1), RC))
        def _(i):
            rows = pl.ds(pl.multiple_of(i * RC, RC), RC)
            a = cap_v[rows, :]
            for n in range(count):
                s = lax.dot_general(
                    a, img_v[n * NC:(n + 1) * NC, :], (((1,), (1,)), ((), ())),
                    preferred_element_type=F32,
                )
                q = s * LOG2E
                highest, found = None, None
                for half in range(2):
                    span = pl.ds(n * NC + half * 128, 128)
                    qh = q[:, half * 128:(half + 1) * 128]
                    t = (qh + bias_b[rows, :]) + col_bias[0:1, span]
                    t_v[rows, span] = t
                    number = iota((1, 128), 1) + float(n * NC + half * 128)
                    w = jnp.where(pos_b[rows, :] == number, qh, 0.0)
                    highest = t if half == 0 else jnp.maximum(highest, t)
                    found = w if half == 0 else found + w
                    cmax[:, span] = jnp.maximum(
                        cmax[:, span], jnp.max(t.reshape(-1, 8, 128), axis=0)
                    )
                    cmatch[:, span] += jnp.sum(w.reshape(-1, 8, 128), axis=0)
                if n == 0:
                    rmax[rows, :] = highest
                    rmatch[rows, :] = found
                else:
                    rmax[rows, :] = jnp.maximum(rmax[rows, :], highest)
                    rmatch[rows, :] += found
            rmax[rows, :] = jnp.broadcast_to(
                jnp.max(rmax[rows, :], axis=1, keepdims=True), (RC, 128)
            )

        top = jnp.max(cmax[...], axis=0, keepdims=True)
        cmax[...] = jnp.broadcast_to(top, cmax.shape)

        def piece(r, totals):
            rows = pl.ds(pl.multiple_of(r * PIECE, PIECE), PIECE)
            peak = rmax[rows, :]
            acc = jnp.zeros((PIECE, 128), F32)
            out = []
            for n in range(2 * count):
                t = t_v[rows, n * 128:(n + 1) * 128]
                acc = acc + jnp.exp2(t - peak)
                f = jnp.exp2(t.reshape(-1, 8, 128) - cmax[:, n * 128:(n + 1) * 128][None])
                out.append(totals[n] + jnp.sum(f, axis=0))
            rsum[rows, :] = acc
            return tuple(out)

        totals = lax.fori_loop(
            0, lax.div(rows_used + (PIECE - 1), PIECE), piece,
            tuple(jnp.zeros((8, 128), F32) for _ in range(2 * count)),
        )
        for n in range(2 * count):
            csum[:, n * 128:(n + 1) * 128] = totals[n]

    used = jnp.maximum(lax.div(img_at[IMGS] + (NC - 1), NC), 1)
    for below, count in zip((0, *COUNTS), COUNTS):
        pl.when((used > below) & (used <= count))(lambda count=count: tiles(count))

    p = place()
    lanes = lax.broadcasted_iota(jnp.int32, (B, 128), 1)
    for k in range(CAPS):
        rows = pl.ds(cap_at[k], B)
        total = jnp.sum(rsum[rows, :], axis=1, keepdims=True)
        match = jnp.sum(rmatch[rows, :], axis=1, keepdims=True)
        packed = jnp.where(lanes == 0, rmax[rows, :] + jnp.log2(total), match)
        lines = jnp.transpose(packed)
        if k:
            put(out, flat(cap_place(p, k)), lines)
        else:
            put(own_row, 0, lines)
    line = lax.broadcasted_iota(jnp.int32, (8, C), 0)
    total = jnp.sum(csum[...], axis=0, keepdims=True)
    match = jnp.sum(cmatch[...], axis=0, keepdims=True)
    lines_v[:, :C] = jnp.where(line == 0, cmax[0:1, :] + jnp.log2(total), match)
    lines_v[:, C:] = jnp.zeros((8, 384), F32)
    for m in range(IMGS):
        whole = lax.shift_left(lax.shift_right_logical(img_at[m], 7), 7)
        slab = lines_v[:, pl.ds(pl.multiple_of(whole, 128), 384)]
        slab = pltpu.roll(slab, lax.rem(384 - (img_at[m] - whole), 384), 1)
        put(out, flat(img_place(p, m)), slab)


def put(out, at, lines):
    for i in range(2):
        out[at, 0:1, i * B:(i + 1) * B] = lines[i:i + 1, :B]


def joined(parts, ranks):
    sums, matches = parts[:, :B], parts[:, B:]
    peak = jnp.max(sums, axis=0, keepdims=True)
    total = jnp.sum(jnp.exp2(sums - peak), axis=0, keepdims=True)
    match = jnp.sum(matches, axis=0, keepdims=True)
    packed = jnp.broadcast_to(LN2 * (peak - match + jnp.log2(total)), (8, B))
    packed = jnp.concatenate([packed, jnp.zeros((8, 256 - B), F32)], axis=1)
    column = jnp.transpose(packed)[:B, 0:1]
    return jnp.sum(jnp.where(iota((B, B), 0) == ranks, column, 0.0), axis=0, keepdims=True)


def loss_kernel(
    parts, own_row, row_ranks, col_ranks, real, caption_loss, image_loss, total, rows, cols
):
    p = place()
    rows[0:1, :] = own_row[0, :, :]
    for k in range(1, CAPS):
        rows[k:k + 1, :] = parts[flat(cap_place(p, k)), :, :]
    for m in range(IMGS):
        cols[m:m + 1, :] = parts[flat(img_place(p, m)), :, :]
    caption = joined(rows[...], row_ranks[0:1, :])
    image = joined(cols[...], col_ranks[...])
    caption_loss[...] = caption
    image_loss[...] = image
    both = jnp.sum(caption, axis=1, keepdims=True) + jnp.sum(image, axis=1, keepdims=True)
    share = both / (2.0 * real[0:1, 0:1])
    total[...] = jnp.broadcast_to(share, (128, 8)).reshape(128, 1, 8)


def small(mib, flops):
    return dict(
        compiler_params=pltpu.CompilerParams(vmem_limit_bytes=mib * 1024 * 1024),
        cost_estimate=pl.CostEstimate(flops=flops, bytes_accessed=10**6, transcendentals=0),
    )


def step(captions, images, positives, valid):
    shape = jax.ShapeDtypeStruct
    pair = shape((2 * B, E), BF16)
    word = (positives + valid * (1 << OK_BIT))[None]
    others = [send(value, other_core) for value in (captions, images, word)]
    carried, kept, words, image_ranks = pl.pallas_call(
        pair_kernel,
        out_shape=[pair, pair, shape((128, 1, B), jnp.int32), shape((1, B), F32)],
        in_specs=[VMEM] * 6,
        out_specs=[VMEM] * 4,
        **small(8, 10**8),
    )(captions, images, word, *others)
    near = send(carried, partner)
    a1, a3 = (send(carried, along(s)) for s in (1, 3))
    b1, b3 = (send(near, along(s)) for s in (1, 3))
    c1, c3 = send(a1, along(1)), send(b3, along(3))
    met = dict(y=near, a1=a1, a3=a3, b1=b1, b3=b3, c1=c1, c3=c3)
    swapped = [kept] + [send(v, other_core) for v in met.values()]
    carried = [carried, *met.values()]
    table = lax.all_to_all(words, AXES, 0, 0, tiled=True)
    ranks, columns, counts, real = pl.pallas_call(
        lookup_kernel,
        out_shape=[
            shape((CAPS, B), F32), shape((B, 128), F32),
            shape((CAPS + IMGS, 128), jnp.int32), shape((8, 128), F32),
        ],
        in_specs=[VMEM],
        out_specs=[VMEM] * 4,
        scratch_shapes=[pltpu.VMEM((CAPS, B), F32), pltpu.VMEM((128, B), jnp.int32)],
        **small(4, 3 * 10**9),
    )(table)
    buffers = []
    for part, (first, last) in enumerate(PARTS):
        buffers = pl.pallas_call(
            functools.partial(compact_kernel, part),
            out_shape=[shape((CAP_ROWS, E), BF16), shape((IMG_ROWS, E), BF16)],
            in_specs=[SMEM] + [VMEM] * (1 + len(buffers) + 2 * (last - first)),
            out_specs=[VMEM] * 2,
            input_output_aliases={2: 0, 3: 1} if part else {},
            **small(10, 10**9),
        )(counts, ranks, *buffers, *carried[first:last], *swapped[first:last])
    cap_v, img_v = buffers
    out, own_row = pl.pallas_call(
        score_kernel,
        out_shape=[shape((n, 1, 2 * B), F32) for n in (128, 1)],
        in_specs=[SMEM] + [VMEM] * 3,
        out_specs=[VMEM] * 2,
        scratch_shapes=[
            pltpu.VMEM((R, C), F32),
            *[pltpu.VMEM((R + RC, 128), F32)] * 5,
            *[pltpu.VMEM((8, C), F32)] * 4,
            pltpu.VMEM((8, C + 384), F32),
        ],
        compiler_params=pltpu.CompilerParams(vmem_limit_bytes=31 * 1024 * 1024),
        cost_estimate=pl.CostEstimate(
            flops=R * C * E, bytes_accessed=2 * (R + C) * E, transcendentals=R * C
        ),
    )(counts, columns, cap_v, img_v)
    parts = lax.all_to_all(out, AXES, 0, 0, tiled=True)
    caption_loss, image_loss, total = pl.pallas_call(
        loss_kernel,
        out_shape=[shape((1, B), F32), shape((1, B), F32), shape((128, 1, 8), F32)],
        in_specs=[VMEM] * 5,
        out_specs=[VMEM] * 3,
        scratch_shapes=[pltpu.VMEM((CAPS, 2 * B), F32), pltpu.VMEM((IMGS, 2 * B), F32)],
        **small(4, 10**8),
    )(parts, own_row, ranks, image_ranks, real)
    totals = lax.all_to_all(total, AXES, 0, 0, tiled=True)
    return caption_loss.reshape(B), image_loss.reshape(B), jnp.sum(totals[:, 0, 0])


def solution(mesh):
    torus = Mesh(mesh.devices.reshape(*SIZES.values()), AXES)
    return jax.shard_map(
        step,
        mesh=torus,
        in_specs=(P(AXES, None), P(AXES, None), P(AXES), P(AXES)),
        out_specs=(P(AXES), P(AXES), P()),
        check_vma=False,
    )
```

```python
import functools
import itertools

import jax
import jax.numpy as jnp
from jax import lax
from jax.experimental import pallas as pl
from jax.experimental.pallas import tpu as pltpu
from jax.sharding import Mesh
from jax.sharding import PartitionSpec as P


SIZES = {"x": 4, "h": 2, "z": 4, "c": 2, "l": 2}
AXES = tuple(SIZES)
LOG2E = 1.4426950408889634
LN2 = 0.6931471805599453
LOW = -1.0e30

B = 192
E = 768
MET = ((0, 0), (0, 1), (3, 0), (1, 0), (3, 1), (1, 1), (2, 0), (2, 1))
PARTS = ((0, 4), (4, 6), (6, 8))
CAPS = len(MET)
IMGS = 2 * len(MET)
C = IMGS * B
RC = 448
R = -(-CAPS * B // RC) * RC
CAP_ROWS = CAPS * B + RC
NC = 256
GROUP = 7 * NC
IMG_ROWS = -(-C // GROUP) * GROUP
PIECE = 64
GRAIN = 16
OK_BIT = 15
ABSENT = 9999.0

F32 = jnp.float32
BF16 = jnp.bfloat16
VMEM = pl.BlockSpec(memory_space=pltpu.VMEM)
SMEM = pl.BlockSpec(memory_space=pltpu.SMEM)


def send(value, to):
    pairs = []
    for at in itertools.product(*map(range, SIZES.values())):
        p = dict(zip(AXES, at))
        pairs.append((flat(p), flat({**p, **to(p)})))
    return lax.ppermute(value, AXES, pairs)


def other_core(p):
    return {"c": 1 - p["c"]}


def partner(p):
    return {"l": 1 - p["l"], "h": p["h"] ^ p["c"]}


def along(step):
    def to(p):
        axis = "x" if p["c"] else "z"
        return {axis: (p[axis] + step) % 4}

    return to


def place():
    return {a: lax.axis_index(a) for a in AXES}


def flat(p):
    at = 0
    for a in AXES:
        at = at * SIZES[a] + p[a]
    return at


def moved(p, off):
    q = dict(p)
    for a, d in off.items():
        q[a] = lax.rem(p[a] + d, SIZES[a])
    return q


def cap_place(p, k):
    step, y = MET[k]
    return moved(p, {"z": step, "l": y})


def img_place(p, m):
    step, y = MET[m // 2]
    return {**moved(p, {"x": step, "h": y, "l": y}), "c": m % 2}


def iota(shape, dim):
    return lax.broadcasted_iota(jnp.int32, shape, dim).astype(F32)


def dot(a, b):
    return jnp.dot(a, b, preferred_element_type=F32)


def earlier():
    return jnp.where(iota((B, B), 0) < iota((B, B), 1), 1.0, 0.0).astype(BF16)


def grains(n):
    return lax.shift_left(lax.shift_right_logical(n + (GRAIN - 1), 4), 4)


def pair_kernel(
    cap, img, word, cap_other, img_other, word_other, carried, kept, words, ranks
):
    first = lax.axis_index("c") == 0
    ok = lax.shift_right_logical(
        jnp.concatenate([word[...], word_other[...]], axis=0), OK_BIT
    )
    order = dot(jnp.broadcast_to(ok[:, None], (2, 8, B)).reshape(16, B).astype(F32).astype(BF16), earlier())
    found = jnp.where(ok > 0, jnp.concatenate([order[0:1], order[8:9]], axis=0), ABSENT)
    ranks[...] = found[0:1, :]
    words[...] = jnp.broadcast_to(word[...], (128, B)).reshape(128, 1, B)
    packed = []
    for i, block in enumerate((img, img_other)):
        pick = jnp.where(iota((B, B), 0) == found[i:i + 1, :], 1.0, 0.0).astype(BF16)
        packed.append(dot(pick, block[...]).astype(BF16))
    carried[0:B, :] = jnp.where(first, cap[...], packed[1])
    carried[B:2 * B, :] = jnp.where(first, cap_other[...], packed[0])
    kept[0:B, :] = jnp.where(first, packed[0], cap_other[...])
    kept[B:2 * B, :] = jnp.where(first, packed[1], cap[...])


def lookup_kernel(table, ranks, columns, counts, real, pos, words_v):
    p = place()
    words = table[...].reshape(128, B)
    words_v[...] = words
    ok = (lax.shift_right_logical(words, OK_BIT) & 1).astype(F32)
    rank = dot(ok.astype(BF16), earlier())
    real[...] = jnp.full((8, 128), jnp.sum(ok), F32)
    known = jnp.transpose(jnp.where(ok > 0, rank + 1.0, 0.0)).astype(BF16)
    for k in range(CAPS):
        row = words_v[pl.ds(flat(cap_place(p, k)), 1), :]
        pos[k:k + 1, :] = (row & ((1 << OK_BIT) - 1)).astype(F32)
    at = pos[...]
    hi = jnp.floor((at + 0.5) * (1.0 / B))
    lo = at - hi * B
    block = iota((128, B), 0)
    inner = iota((B, B), 0)
    for k in range(CAPS):
        pick = jnp.where(block == hi[k:k + 1, :], 1.0, 0.0).astype(BF16)
        column = dot(known, pick)
        pos[k:k + 1, :] = jnp.sum(
            jnp.where(inner == lo[k:k + 1, :], column, 0.0), axis=0, keepdims=True
        )
    value = pos[...]
    live = value > 0.0
    marks = jnp.where(live, 1.0, 0.0)
    order = dot(marks.astype(BF16), earlier())
    ranks[...] = jnp.where(live, order, ABSENT)
    start = jnp.zeros((1, 1), F32)
    base = jnp.full((CAPS, B), -ABSENT, F32)
    counts[0:CAPS, :] = jnp.broadcast_to(
        jnp.sum(marks, axis=1, keepdims=True).astype(jnp.int32), (CAPS, 128)
    )
    for m in range(IMGS):
        number = flat(img_place(p, m))
        row = words_v[pl.ds(number, 1), :]
        row = lax.shift_right_logical(row, OK_BIT) & 1
        count = jnp.sum(row.astype(F32), axis=1, keepdims=True)
        base = jnp.where(hi == number.astype(F32), start, base)
        start = start + jnp.floor((count + (GRAIN - 1.0)) * (1.0 / GRAIN)) * GRAIN
        counts[CAPS + m:CAPS + m + 1, :] = jnp.broadcast_to(count.astype(jnp.int32), (1, 128))
    targets = jnp.where(live, base + value - 1.0, -ABSENT)
    order = ranks[...]
    lane = iota((B, 128), 1)
    result = jnp.zeros((B, 128), F32)
    for k in range(CAPS):
        hit = inner == order[k:k + 1, :]
        target = jnp.sum(jnp.where(hit, targets[k:k + 1, :], 0.0), axis=1, keepdims=True)
        result = jnp.where(lane == float(k), target, result)
    columns[...] = result


def starts_of(counts, first, number):
    found, at = [], jnp.int32(0)
    for k in range(number):
        found.append(pl.multiple_of(at, GRAIN))
        at = at + grains(counts[first + k, 0])
    return found + [pl.multiple_of(at, GRAIN)]


def groups_of(columns):
    return jnp.maximum(lax.div(columns + (GROUP - 1), GROUP), 1)


def compact(counts, ranks, carried, kept, cap_out, img_out, first):
    core = lax.axis_index("c")
    slot = iota((B, B), 0)
    at = starts_of(counts, 0, CAPS)
    for k, (a, b) in enumerate(zip(carried, kept), first):
        block = jnp.where(core == 0, a[0:B, :], b[B:2 * B, :])
        pick = jnp.where(slot == ranks[k:k + 1, :], 1.0, 0.0).astype(BF16)
        cap_out[pl.ds(at[k], B), :] = dot(pick, block).astype(BF16)
    at = starts_of(counts, CAPS, IMGS)
    for k, (a, b) in enumerate(zip(carried, kept), first):
        for side in range(2):
            rows = pl.ds(side * B, B)
            img_out[pl.ds(at[2 * k + side], B), :] = jnp.where(core == 0, b[rows, :], a[rows, :])


def compact_kernel(part, counts, ranks, *refs):
    first, last = PARTS[part]
    refs = refs[2 if part else 0:]
    number = last - first
    cap_out, img_out = refs[2 * number:]
    compact(counts, ranks, refs[:number], refs[number:2 * number], cap_out, img_out, first)
    if last == CAPS:
        cap_end = starts_of(counts, 0, CAPS)[-1]
        img_end = starts_of(counts, CAPS, IMGS)[-1]
        cap_out[pl.ds(cap_end, RC), :] = jnp.zeros((RC, E), BF16)
        blank = jnp.zeros((64, E), BF16)
        goal = groups_of(img_end) * GROUP

        @pl.loop(0, lax.div(goal - img_end, 64))
        def _(i):
            img_out[pl.ds(pl.multiple_of(img_end + i * 64, GRAIN), 64), :] = blank

        img_out[pl.ds(pl.multiple_of(goal - 64, GRAIN), 64), :] = jnp.where(
            iota((64, E), 0) + (goal - 64).astype(F32) < img_end.astype(F32),
            img_out[pl.ds(pl.multiple_of(goal - 64, GRAIN), 64), :], blank,
        )


def score_kernel(
    counts, columns, cap_v, img_v, out, own_row,
    t_v, pos_b, bias_b, rmax, rmatch, rsum, col_bias, cmax, cmatch, csum, lines_v,
):
    img_at = starts_of(counts, CAPS, IMGS)
    column = iota((8, IMG_ROWS), 1)
    bias = jnp.full((8, IMG_ROWS), LOW, F32)
    for m in range(IMGS):
        begin = img_at[m].astype(F32)
        end = begin + counts[CAPS + m, 0].astype(F32)
        bias = jnp.where((column >= begin) & (column < end), 0.0, bias)
    col_bias[...] = bias
    cap_at = starts_of(counts, 0, CAPS)
    slot = iota((B, 128), 0)
    for k in range(CAPS):
        rows = pl.ds(cap_at[k], B)
        pos_b[rows, :] = jnp.broadcast_to(columns[:, k:k + 1], (B, 128))
        bias_b[rows, :] = jnp.where(slot < counts[k, 0].astype(F32), 0.0, LOW)
    rows_used = cap_at[CAPS]
    tail = pl.ds(rows_used, RC)
    bias_b[tail, :] = jnp.full((RC, 128), LOW, F32)
    pos_b[tail, :] = jnp.full((RC, 128), -ABSENT, F32)
    cmax[...] = jnp.full(cmax.shape, 4.0 * LOW, F32)
    cmatch[...] = jnp.zeros(cmatch.shape, F32)
    csum[...] = jnp.zeros(csum.shape, F32)

    groups = groups_of(img_at[IMGS])
    steps = lax.div(rows_used + (RC - 1), RC)

    @pl.loop(0, steps)
    def _(i):
        rows = pl.ds(pl.multiple_of(i * RC, RC), RC)
        rmax[rows, :] = jnp.full((RC, 128), 4.0 * LOW, F32)
        rmatch[rows, :] = jnp.zeros((RC, 128), F32)
        rsum[rows, :] = jnp.zeros((RC, 128), F32)

    @pl.loop(0, groups * steps)
    def _(at):
        g = lax.div(at, steps)
        first = pl.multiple_of(g * GROUP, GROUP)
        rows = pl.ds(pl.multiple_of((at - g * steps) * RC, RC), RC)
        a = cap_v[rows, :]
        for n in range(GROUP // NC):
            s = lax.dot_general(
                a, img_v[pl.ds(pl.multiple_of(first + n * NC, NC), NC), :],
                (((1,), (1,)), ((), ())), preferred_element_type=F32,
            )
            q = s * LOG2E
            highest, found = None, None
            for half in range(2):
                column = first + (n * NC + half * 128)
                span = pl.ds(pl.multiple_of(column, 128), 128)
                qh = q[:, half * 128:(half + 1) * 128]
                t = (qh + bias_b[rows, :]) + col_bias[0:1, span]
                t_v[rows, span] = t
                number = iota((1, 128), 1) + column.astype(F32)
                w = jnp.where(pos_b[rows, :] == number, qh, 0.0)
                highest = t if half == 0 else jnp.maximum(highest, t)
                found = w if half == 0 else found + w
                cmax[:, span] = jnp.maximum(
                    cmax[:, span], jnp.max(t.reshape(-1, 8, 128), axis=0)
                )
                cmatch[:, span] += jnp.sum(w.reshape(-1, 8, 128), axis=0)
            rmax[rows, :] = jnp.maximum(rmax[rows, :], highest)
            rmatch[rows, :] += found

    @pl.loop(0, steps)
    def _(i):
        rows = pl.ds(pl.multiple_of(i * RC, RC), RC)
        rmax[rows, :] = jnp.broadcast_to(
            jnp.max(rmax[rows, :], axis=1, keepdims=True), (RC, 128)
        )

    top = jnp.max(cmax[...], axis=0, keepdims=True)
    cmax[...] = jnp.broadcast_to(top, cmax.shape)
    width = GROUP // 128

    @pl.loop(0, groups)
    def _(g):
        spans = [
            pl.ds(pl.multiple_of(g * GROUP + n * 128, 128), 128) for n in range(width)
        ]

        def piece(r, totals):
            rows = pl.ds(pl.multiple_of(r * PIECE, PIECE), PIECE)
            peak = rmax[rows, :]
            acc = rsum[rows, :]
            out = []
            for n, span in enumerate(spans):
                t = t_v[rows, span]
                acc = acc + jnp.exp2(t - peak)
                f = jnp.exp2(t.reshape(-1, 8, 128) - cmax[:, span][None])
                out.append(totals[n] + jnp.sum(f, axis=0))
            rsum[rows, :] = acc
            return tuple(out)

        totals = lax.fori_loop(
            0, lax.div(rows_used + (PIECE - 1), PIECE), piece,
            tuple(jnp.zeros((8, 128), F32) for _ in range(width)),
        )
        for n, span in enumerate(spans):
            csum[:, span] = totals[n]

    p = place()
    lanes = lax.broadcasted_iota(jnp.int32, (B, 128), 1)
    for k in range(CAPS):
        rows = pl.ds(cap_at[k], B)
        total = jnp.sum(rsum[rows, :], axis=1, keepdims=True)
        match = jnp.sum(rmatch[rows, :], axis=1, keepdims=True)
        packed = jnp.where(lanes == 0, rmax[rows, :] + jnp.log2(total), match)
        lines = jnp.transpose(packed)
        if k:
            put(out, flat(cap_place(p, k)), lines)
        else:
            put(own_row, 0, lines)
    line = lax.broadcasted_iota(jnp.int32, (8, IMG_ROWS), 0)
    total = jnp.sum(csum[...], axis=0, keepdims=True)
    match = jnp.sum(cmatch[...], axis=0, keepdims=True)
    lines_v[:, :IMG_ROWS] = jnp.where(line == 0, cmax[0:1, :] + jnp.log2(total), match)
    lines_v[:, IMG_ROWS:] = jnp.zeros((8, 384), F32)
    for m in range(IMGS):
        whole = lax.shift_left(lax.shift_right_logical(img_at[m], 7), 7)
        slab = lines_v[:, pl.ds(pl.multiple_of(whole, 128), 384)]
        slab = pltpu.roll(slab, lax.rem(384 - (img_at[m] - whole), 384), 1)
        put(out, flat(img_place(p, m)), slab)


def put(out, at, lines):
    for i in range(2):
        out[at, 0:1, i * B:(i + 1) * B] = lines[i:i + 1, :B]


def joined(parts, ranks):
    sums, matches = parts[:, :B], parts[:, B:]
    peak = jnp.max(sums, axis=0, keepdims=True)
    total = jnp.sum(jnp.exp2(sums - peak), axis=0, keepdims=True)
    match = jnp.sum(matches, axis=0, keepdims=True)
    packed = jnp.broadcast_to(LN2 * (peak - match + jnp.log2(total)), (8, B))
    packed = jnp.concatenate([packed, jnp.zeros((8, 256 - B), F32)], axis=1)
    column = jnp.transpose(packed)[:B, 0:1]
    return jnp.sum(jnp.where(iota((B, B), 0) == ranks, column, 0.0), axis=0, keepdims=True)


def loss_kernel(
    parts, own_row, row_ranks, col_ranks, real, caption_loss, image_loss, total, rows, cols
):
    p = place()
    rows[0:1, :] = own_row[0, :, :]
    for k in range(1, CAPS):
        rows[k:k + 1, :] = parts[flat(cap_place(p, k)), :, :]
    for m in range(IMGS):
        cols[m:m + 1, :] = parts[flat(img_place(p, m)), :, :]
    caption = joined(rows[...], row_ranks[0:1, :])
    image = joined(cols[...], col_ranks[...])
    caption_loss[...] = caption
    image_loss[...] = image
    both = jnp.sum(caption, axis=1, keepdims=True) + jnp.sum(image, axis=1, keepdims=True)
    share = both / (2.0 * real[0:1, 0:1])
    total[...] = jnp.broadcast_to(share, (128, 8)).reshape(128, 1, 8)


def small(mib, flops):
    return dict(
        compiler_params=pltpu.CompilerParams(vmem_limit_bytes=mib * 1024 * 1024),
        cost_estimate=pl.CostEstimate(flops=flops, bytes_accessed=10**6, transcendentals=0),
    )


def step(captions, images, positives, valid):
    shape = jax.ShapeDtypeStruct
    pair = shape((2 * B, E), BF16)
    word = (positives + valid * (1 << OK_BIT))[None]
    others = [send(value, other_core) for value in (captions, images, word)]
    carried, kept, words, image_ranks = pl.pallas_call(
        pair_kernel,
        out_shape=[pair, pair, shape((128, 1, B), jnp.int32), shape((1, B), F32)],
        in_specs=[VMEM] * 6,
        out_specs=[VMEM] * 4,
        **small(8, 10**8),
    )(captions, images, word, *others)
    near = send(carried, partner)
    a1, a3 = (send(carried, along(s)) for s in (1, 3))
    b1, b3 = (send(near, along(s)) for s in (1, 3))
    c1, c3 = send(a1, along(1)), send(b3, along(3))
    met = dict(y=near, a1=a1, a3=a3, b1=b1, b3=b3, c1=c1, c3=c3)
    swapped = [kept] + [send(v, other_core) for v in met.values()]
    carried = [carried, *met.values()]
    table = lax.all_to_all(words, AXES, 0, 0, tiled=True)
    ranks, columns, counts, real = pl.pallas_call(
        lookup_kernel,
        out_shape=[
            shape((CAPS, B), F32), shape((B, 128), F32),
            shape((CAPS + IMGS, 128), jnp.int32), shape((8, 128), F32),
        ],
        in_specs=[VMEM],
        out_specs=[VMEM] * 4,
        scratch_shapes=[pltpu.VMEM((CAPS, B), F32), pltpu.VMEM((128, B), jnp.int32)],
        **small(4, 3 * 10**9),
    )(table)
    buffers = []
    for part, (first, last) in enumerate(PARTS):
        buffers = pl.pallas_call(
            functools.partial(compact_kernel, part),
            out_shape=[shape((CAP_ROWS, E), BF16), shape((IMG_ROWS, E), BF16)],
            in_specs=[SMEM] + [VMEM] * (1 + len(buffers) + 2 * (last - first)),
            out_specs=[VMEM] * 2,
            input_output_aliases={2: 0, 3: 1} if part else {},
            **small(10, 10**9),
        )(counts, ranks, *buffers, *carried[first:last], *swapped[first:last])
    cap_v, img_v = buffers
    out, own_row = pl.pallas_call(
        score_kernel,
        out_shape=[shape((n, 1, 2 * B), F32) for n in (128, 1)],
        in_specs=[SMEM] + [VMEM] * 3,
        out_specs=[VMEM] * 2,
        scratch_shapes=[
            pltpu.VMEM((R, IMG_ROWS), F32),
            *[pltpu.VMEM((R + RC, 128), F32)] * 5,
            *[pltpu.VMEM((8, IMG_ROWS), F32)] * 4,
            pltpu.VMEM((8, IMG_ROWS + 384), F32),
        ],
        compiler_params=pltpu.CompilerParams(vmem_limit_bytes=36 * 1024 * 1024),
        cost_estimate=pl.CostEstimate(
            flops=R * C * E, bytes_accessed=2 * (R + C) * E, transcendentals=R * C
        ),
    )(counts, columns, cap_v, img_v)
    parts = lax.all_to_all(out, AXES, 0, 0, tiled=True)
    caption_loss, image_loss, total = pl.pallas_call(
        loss_kernel,
        out_shape=[shape((1, B), F32), shape((1, B), F32), shape((128, 1, 8), F32)],
        in_specs=[VMEM] * 5,
        out_specs=[VMEM] * 3,
        scratch_shapes=[pltpu.VMEM((CAPS, 2 * B), F32), pltpu.VMEM((IMGS, 2 * B), F32)],
        **small(4, 10**8),
    )(parts, own_row, ranks, image_ranks, real)
    totals = lax.all_to_all(total, AXES, 0, 0, tiled=True)
    return caption_loss.reshape(B), image_loss.reshape(B), jnp.sum(totals[:, 0, 0])


def solution(mesh):
    torus = Mesh(mesh.devices.reshape(*SIZES.values()), AXES)
    return jax.shard_map(
        step,
        mesh=torus,
        in_specs=(P(AXES, None), P(AXES, None), P(AXES), P(AXES)),
        out_specs=(P(AXES), P(AXES), P()),
        check_vma=False,
    )
```

```python
import functools
import itertools

import jax
import jax.numpy as jnp
from jax import lax
from jax.experimental import pallas as pl
from jax.experimental.pallas import tpu as pltpu
from jax.sharding import Mesh
from jax.sharding import PartitionSpec as P


SIZES = {"x": 4, "h": 2, "z": 4, "c": 2, "l": 2}
AXES = tuple(SIZES)
LOG2E = 1.4426950408889634
LN2 = 0.6931471805599453
LOW = -1.0e30

B = 192
E = 768
MET = ((0, 0), (0, 1), (3, 0), (1, 0), (3, 1), (1, 1), (2, 0), (2, 1))
PARTS = ((0, 4), (4, 6), (6, 8))
CAPS = len(MET)
IMGS = 2 * len(MET)
C = IMGS * B
RC = 448
R = -(-CAPS * B // RC) * RC
CAP_ROWS = CAPS * B + RC
NC = 256
COUNTS = (2, 4, 5, 6, 7, 8, 10, 12)
TAIL = 2 * NC
IMG_ROWS = C + TAIL
PIECE = 32
GRAIN = 16
OK_BIT = 15
ABSENT = 9999.0

F32 = jnp.float32
BF16 = jnp.bfloat16
VMEM = pl.BlockSpec(memory_space=pltpu.VMEM)
SMEM = pl.BlockSpec(memory_space=pltpu.SMEM)


def send(value, to):
    pairs = []
    for at in itertools.product(*map(range, SIZES.values())):
        p = dict(zip(AXES, at))
        pairs.append((flat(p), flat({**p, **to(p)})))
    return lax.ppermute(value, AXES, pairs)


def other_core(p):
    return {"c": 1 - p["c"]}


def partner(p):
    return {"l": 1 - p["l"], "h": p["h"] ^ p["c"]}


def along(step):
    def to(p):
        axis = "x" if p["c"] else "z"
        return {axis: (p[axis] + step) % 4}

    return to


def place():
    return {a: lax.axis_index(a) for a in AXES}


def flat(p):
    at = 0
    for a in AXES:
        at = at * SIZES[a] + p[a]
    return at


def moved(p, off):
    q = dict(p)
    for a, d in off.items():
        q[a] = lax.rem(p[a] + d, SIZES[a])
    return q


def cap_place(p, k):
    step, y = MET[k]
    return moved(p, {"z": step, "l": y})


def img_place(p, m):
    step, y = MET[m // 2]
    return {**moved(p, {"x": step, "h": y, "l": y}), "c": m % 2}


def iota(shape, dim):
    return lax.broadcasted_iota(jnp.int32, shape, dim).astype(F32)


def dot(a, b):
    return jnp.dot(a, b, preferred_element_type=F32)


def earlier():
    return jnp.where(iota((B, B), 0) < iota((B, B), 1), 1.0, 0.0).astype(BF16)


def grains(n):
    return lax.shift_left(lax.shift_right_logical(n + (GRAIN - 1), 4), 4)


def pair_kernel(
    cap, img, word, cap_other, img_other, word_other, carried, kept, words, ranks
):
    first = lax.axis_index("c") == 0
    ok = lax.shift_right_logical(
        jnp.concatenate([word[...], word_other[...]], axis=0), OK_BIT
    )
    order = dot(jnp.broadcast_to(ok[:, None], (2, 8, B)).reshape(16, B).astype(F32).astype(BF16), earlier())
    found = jnp.where(ok > 0, jnp.concatenate([order[0:1], order[8:9]], axis=0), ABSENT)
    ranks[...] = found[0:1, :]
    both = jnp.where(
        first == (lax.broadcasted_iota(jnp.int32, (2, B), 0) == 0), word[...], word_other[...]
    )
    words[...] = jnp.broadcast_to(both[None], (8, 2, B))
    packed = []
    for i, block in enumerate((img, img_other)):
        pick = jnp.where(iota((B, B), 0) == found[i:i + 1, :], 1.0, 0.0).astype(BF16)
        packed.append(dot(pick, block[...]).astype(BF16))
    carried[0:B, :] = jnp.where(first, cap[...], packed[1])
    carried[B:2 * B, :] = jnp.where(first, cap_other[...], packed[0])
    kept[0:B, :] = jnp.where(first, packed[0], cap_other[...])
    kept[B:2 * B, :] = jnp.where(first, packed[1], cap[...])


def table_row(p):
    return ((p["z"] * 2 + p["l"]) * 8 + p["x"] * 2 + p["h"]) * 2 + p["c"]


def lookup_kernel(table, ranks, columns, counts, real, pos, words_v):
    p = place()
    words = table[...].reshape(128, B)
    words_v[...] = words
    ok = (lax.shift_right_logical(words, OK_BIT) & 1).astype(F32)
    rank = dot(ok.astype(BF16), earlier())
    real[...] = jnp.full((8, 128), jnp.sum(ok), F32)
    known = jnp.transpose(jnp.where(ok > 0, rank + 1.0, 0.0)).astype(BF16)
    for k in range(CAPS):
        row = words_v[pl.ds(table_row(cap_place(p, k)), 1), :]
        pos[k:k + 1, :] = (row & ((1 << OK_BIT) - 1)).astype(F32)
    at = pos[...]
    hi = jnp.floor((at + 0.5) * (1.0 / B))
    lo = at - hi * B
    line = lax.broadcasted_iota(jnp.int32, (128, B), 0)
    bits = lambda low, mask: lax.shift_right_logical(line, low) & mask
    block = (bits(1, 7) * 16 + bits(5, 3) * 4 + bits(0, 1) * 2 + bits(4, 1)).astype(F32)
    inner = iota((B, B), 0)
    for k in range(CAPS):
        pick = jnp.where(block == hi[k:k + 1, :], 1.0, 0.0).astype(BF16)
        column = dot(known, pick)
        pos[k:k + 1, :] = jnp.sum(
            jnp.where(inner == lo[k:k + 1, :], column, 0.0), axis=0, keepdims=True
        )
    value = pos[...]
    live = value > 0.0
    marks = jnp.where(live, 1.0, 0.0)
    order = dot(marks.astype(BF16), earlier())
    ranks[...] = jnp.where(live, order, ABSENT)
    start = jnp.zeros((1, 1), F32)
    base = jnp.full((CAPS, B), -ABSENT, F32)
    counts[0:CAPS, :] = jnp.broadcast_to(
        jnp.sum(marks, axis=1, keepdims=True).astype(jnp.int32), (CAPS, 128)
    )
    for m in range(IMGS):
        number = flat(img_place(p, m))
        row = words_v[pl.ds(table_row(img_place(p, m)), 1), :]
        row = lax.shift_right_logical(row, OK_BIT) & 1
        count = jnp.sum(row.astype(F32), axis=1, keepdims=True)
        base = jnp.where(hi == number.astype(F32), start, base)
        start = start + jnp.floor((count + (GRAIN - 1.0)) * (1.0 / GRAIN)) * GRAIN
        counts[CAPS + m:CAPS + m + 1, :] = jnp.broadcast_to(count.astype(jnp.int32), (1, 128))
    targets = jnp.where(live, base + value - 1.0, -ABSENT)
    order = ranks[...]
    lane = iota((B, 128), 1)
    result = jnp.zeros((B, 128), F32)
    for k in range(CAPS):
        hit = inner == order[k:k + 1, :]
        target = jnp.sum(jnp.where(hit, targets[k:k + 1, :], 0.0), axis=1, keepdims=True)
        result = jnp.where(lane == float(k), target, result)
    columns[...] = result


def starts_of(counts, first, number):
    found, at = [], jnp.int32(0)
    for k in range(number):
        found.append(pl.multiple_of(at, GRAIN))
        at = at + grains(counts[first + k, 0])
    return found + [pl.multiple_of(at, GRAIN)]


def compact(counts, ranks, carried, kept, cap_out, img_out, first):
    core = lax.axis_index("c")
    slot = iota((B, B), 0)
    at = starts_of(counts, 0, CAPS)
    for k, (a, b) in enumerate(zip(carried, kept), first):
        block = jnp.where(core == 0, a[0:B, :], b[B:2 * B, :])
        pick = jnp.where(slot == ranks[k:k + 1, :], 1.0, 0.0).astype(BF16)
        cap_out[pl.ds(at[k], B), :] = dot(pick, block).astype(BF16)
    at = starts_of(counts, CAPS, IMGS)
    for k, (a, b) in enumerate(zip(carried, kept), first):
        for side in range(2):
            rows = pl.ds(side * B, B)
            img_out[pl.ds(at[2 * k + side], B), :] = jnp.where(core == 0, b[rows, :], a[rows, :])


def compact_kernel(part, counts, ranks, *refs):
    first, last = PARTS[part]
    refs = refs[2 if part else 0:]
    number = last - first
    cap_out, img_out = refs[2 * number:]
    compact(counts, ranks, refs[:number], refs[number:2 * number], cap_out, img_out, first)
    if last == CAPS:
        cap_end = starts_of(counts, 0, CAPS)[-1]
        img_end = starts_of(counts, CAPS, IMGS)[-1]
        cap_out[pl.ds(cap_end, RC), :] = jnp.zeros((RC, E), BF16)
        img_out[pl.ds(img_end, TAIL), :] = jnp.zeros((TAIL, E), BF16)


def score_kernel(
    counts, columns, cap_v, img_v, out, own_row,
    t_v, pos_b, bias_b, rmax, rmatch, rsum, col_bias, cmax, cmatch, csum, lines_v,
):
    img_at = starts_of(counts, CAPS, IMGS)
    col_bias[...] = jnp.full((8, C + 384), LOW, F32)
    column = iota((8, 384), 1)
    for m in range(IMGS):
        whole = lax.shift_left(lax.shift_right_logical(img_at[m], 7), 7)
        span = pl.ds(pl.multiple_of(whole, 128), 384)
        begin = (img_at[m] - whole).astype(F32)
        end = begin + counts[CAPS + m, 0].astype(F32)
        inside = (column >= begin) & (column < end)
        col_bias[:, span] = jnp.where(inside, 0.0, col_bias[:, span])
    cap_at = starts_of(counts, 0, CAPS)
    slot = iota((B, 128), 0)
    for k in range(CAPS):
        rows = pl.ds(cap_at[k], B)
        pos_b[rows, :] = jnp.broadcast_to(columns[:, k:k + 1], (B, 128))
        bias_b[rows, :] = jnp.where(slot < counts[k, 0].astype(F32), 0.0, LOW)
    rows_used = cap_at[CAPS]
    tail = pl.ds(rows_used, RC)
    bias_b[tail, :] = jnp.full((RC, 128), LOW, F32)
    pos_b[tail, :] = jnp.full((RC, 128), -ABSENT, F32)
    cmax[...] = jnp.full(cmax.shape, 4.0 * LOW, F32)
    cmatch[...] = jnp.zeros(cmatch.shape, F32)
    csum[...] = jnp.zeros(csum.shape, F32)

    def tiles(count):
        @pl.loop(0, lax.div(rows_used + (RC - 1), RC))
        def _(i):
            rows = pl.ds(pl.multiple_of(i * RC, RC), RC)
            a = cap_v[rows, :]
            for n in range(count):
                s = lax.dot_general(
                    a, img_v[n * NC:(n + 1) * NC, :], (((1,), (1,)), ((), ())),
                    preferred_element_type=F32,
                )
                q = s * LOG2E
                highest, found = None, None
                for half in range(2):
                    span = pl.ds(n * NC + half * 128, 128)
                    qh = q[:, half * 128:(half + 1) * 128]
                    t = (qh + bias_b[rows, :]) + col_bias[0:1, span]
                    t_v[rows, span] = t
                    number = iota((1, 128), 1) + float(n * NC + half * 128)
                    w = jnp.where(pos_b[rows, :] == number, qh, 0.0)
                    highest = t if half == 0 else jnp.maximum(highest, t)
                    found = w if half == 0 else found + w
                    cmax[:, span] = jnp.maximum(
                        cmax[:, span], jnp.max(t.reshape(-1, 8, 128), axis=0)
                    )
                    cmatch[:, span] += jnp.sum(w.reshape(-1, 8, 128), axis=0)
                if n == 0:
                    rmax[rows, :] = highest
                    rmatch[rows, :] = found
                else:
                    rmax[rows, :] = jnp.maximum(rmax[rows, :], highest)
                    rmatch[rows, :] += found
            rmax[rows, :] = jnp.broadcast_to(
                jnp.max(rmax[rows, :], axis=1, keepdims=True), (RC, 128)
            )

        top = jnp.max(cmax[...], axis=0, keepdims=True)
        cmax[...] = jnp.broadcast_to(top, cmax.shape)

        def piece(r, totals):
            rows = pl.ds(pl.multiple_of(r * PIECE, PIECE), PIECE)
            peak = rmax[rows, :]
            acc = jnp.zeros((PIECE, 128), F32)
            out = []
            for n in range(2 * count):
                t = t_v[rows, n * 128:(n + 1) * 128]
                acc = acc + jnp.exp2(t - peak)
                f = jnp.exp2(t.reshape(-1, 8, 128) - cmax[:, n * 128:(n + 1) * 128][None])
                out.append(totals[n] + jnp.sum(f, axis=0))
            rsum[rows, :] = acc
            return tuple(out)

        totals = lax.fori_loop(
            0, lax.div(rows_used + (PIECE - 1), PIECE), piece,
            tuple(jnp.zeros((8, 128), F32) for _ in range(2 * count)),
        )
        for n in range(2 * count):
            csum[:, n * 128:(n + 1) * 128] = totals[n]

    used = jnp.maximum(lax.div(img_at[IMGS] + (NC - 1), NC), 1)
    for below, count in zip((0, *COUNTS), COUNTS):
        pl.when((used > below) & (used <= count))(lambda count=count: tiles(count))

    p = place()
    lanes = lax.broadcasted_iota(jnp.int32, (B, 128), 1)
    for k in range(CAPS):
        rows = pl.ds(cap_at[k], B)
        total = jnp.sum(rsum[rows, :], axis=1, keepdims=True)
        match = jnp.sum(rmatch[rows, :], axis=1, keepdims=True)
        packed = jnp.where(lanes == 0, rmax[rows, :] + jnp.log2(total), match)
        lines = jnp.transpose(packed)
        if k:
            put(out, flat(cap_place(p, k)), lines)
        else:
            put(own_row, 0, lines)
    line = lax.broadcasted_iota(jnp.int32, (8, C), 0)
    total = jnp.sum(csum[...], axis=0, keepdims=True)
    match = jnp.sum(cmatch[...], axis=0, keepdims=True)
    lines_v[:, :C] = jnp.where(line == 0, cmax[0:1, :] + jnp.log2(total), match)
    lines_v[:, C:] = jnp.zeros((8, 384), F32)
    for m in range(IMGS):
        whole = lax.shift_left(lax.shift_right_logical(img_at[m], 7), 7)
        slab = lines_v[:, pl.ds(pl.multiple_of(whole, 128), 384)]
        slab = pltpu.roll(slab, lax.rem(384 - (img_at[m] - whole), 384), 1)
        put(out, flat(img_place(p, m)), slab)


def put(out, at, lines):
    for i in range(2):
        out[at, 0:1, i * B:(i + 1) * B] = lines[i:i + 1, :B]


def joined(parts, ranks):
    sums, matches = parts[:, :B], parts[:, B:]
    peak = jnp.max(sums, axis=0, keepdims=True)
    total = jnp.sum(jnp.exp2(sums - peak), axis=0, keepdims=True)
    match = jnp.sum(matches, axis=0, keepdims=True)
    packed = jnp.broadcast_to(LN2 * (peak - match + jnp.log2(total)), (8, B))
    packed = jnp.concatenate([packed, jnp.zeros((8, 256 - B), F32)], axis=1)
    column = jnp.transpose(packed)[:B, 0:1]
    return jnp.sum(jnp.where(iota((B, B), 0) == ranks, column, 0.0), axis=0, keepdims=True)


def loss_kernel(
    parts, own_row, row_ranks, col_ranks, real, caption_loss, image_loss, total, rows, cols
):
    p = place()
    rows[0:1, :] = own_row[0, :, :]
    for k in range(1, CAPS):
        rows[k:k + 1, :] = parts[flat(cap_place(p, k)), :, :]
    for m in range(IMGS):
        cols[m:m + 1, :] = parts[flat(img_place(p, m)), :, :]
    caption = joined(rows[...], row_ranks[0:1, :])
    image = joined(cols[...], col_ranks[...])
    caption_loss[...] = caption
    image_loss[...] = image
    both = jnp.sum(caption, axis=1, keepdims=True) + jnp.sum(image, axis=1, keepdims=True)
    share = both / (2.0 * real[0:1, 0:1])
    total[...] = jnp.broadcast_to(share, (128, 8)).reshape(128, 1, 8)


def small(mib, flops):
    return dict(
        compiler_params=pltpu.CompilerParams(vmem_limit_bytes=mib * 1024 * 1024),
        cost_estimate=pl.CostEstimate(flops=flops, bytes_accessed=10**6, transcendentals=0),
    )


def step(captions, images, positives, valid):
    shape = jax.ShapeDtypeStruct
    pair = shape((2 * B, E), BF16)
    word = (positives + valid * (1 << OK_BIT))[None]
    others = [send(value, other_core) for value in (captions, images, word)]
    carried, kept, words, image_ranks = pl.pallas_call(
        pair_kernel,
        out_shape=[pair, pair, shape((8, 2, B), jnp.int32), shape((1, B), F32)],
        in_specs=[VMEM] * 6,
        out_specs=[VMEM] * 4,
        **small(8, 10**8),
    )(captions, images, word, *others)
    near = send(carried, partner)
    a1, a3 = (send(carried, along(s)) for s in (1, 3))
    b1, b3 = (send(near, along(s)) for s in (1, 3))
    c1, c3 = send(a1, along(1)), send(b3, along(3))
    met = dict(y=near, a1=a1, a3=a3, b1=b1, b3=b3, c1=c1, c3=c3)
    swapped = [kept] + [send(v, other_core) for v in met.values()]
    carried = [carried, *met.values()]
    part = lax.all_to_all(words, ("x", "h"), 0, 0, tiled=True)
    part = jnp.broadcast_to(part.reshape(1, 16, B), (8, 16, B))
    table = lax.all_to_all(part, ("z", "l"), 0, 0, tiled=True)
    ranks, columns, counts, real = pl.pallas_call(
        lookup_kernel,
        out_shape=[
            shape((CAPS, B), F32), shape((B, 128), F32),
            shape((CAPS + IMGS, 128), jnp.int32), shape((8, 128), F32),
        ],
        in_specs=[VMEM],
        out_specs=[VMEM] * 4,
        scratch_shapes=[pltpu.VMEM((CAPS, B), F32), pltpu.VMEM((128, B), jnp.int32)],
        **small(4, 3 * 10**9),
    )(table)
    buffers = []
    for part, (first, last) in enumerate(PARTS):
        buffers = pl.pallas_call(
            functools.partial(compact_kernel, part),
            out_shape=[shape((CAP_ROWS, E), BF16), shape((IMG_ROWS, E), BF16)],
            in_specs=[SMEM] + [VMEM] * (1 + len(buffers) + 2 * (last - first)),
            out_specs=[VMEM] * 2,
            input_output_aliases={2: 0, 3: 1} if part else {},
            **small(10, 10**9),
        )(counts, ranks, *buffers, *carried[first:last], *swapped[first:last])
    cap_v, img_v = buffers
    out, own_row = pl.pallas_call(
        score_kernel,
        out_shape=[shape((n, 1, 2 * B), F32) for n in (128, 1)],
        in_specs=[SMEM] + [VMEM] * 3,
        out_specs=[VMEM] * 2,
        scratch_shapes=[
            pltpu.VMEM((R, C), F32),
            *[pltpu.VMEM((R + RC, 128), F32)] * 5,
            pltpu.VMEM((8, C + 384), F32),
            *[pltpu.VMEM((8, C), F32)] * 3,
            pltpu.VMEM((8, C + 384), F32),
        ],
        compiler_params=pltpu.CompilerParams(vmem_limit_bytes=31 * 1024 * 1024),
        cost_estimate=pl.CostEstimate(
            flops=R * C * E, bytes_accessed=2 * (R + C) * E, transcendentals=R * C
        ),
    )(counts, columns, cap_v, img_v)
    parts = lax.all_to_all(out, AXES, 0, 0, tiled=True)
    caption_loss, image_loss, total = pl.pallas_call(
        loss_kernel,
        out_shape=[shape((1, B), F32), shape((1, B), F32), shape((128, 1, 8), F32)],
        in_specs=[VMEM] * 5,
        out_specs=[VMEM] * 3,
        scratch_shapes=[pltpu.VMEM((CAPS, 2 * B), F32), pltpu.VMEM((IMGS, 2 * B), F32)],
        **small(4, 10**8),
    )(parts, own_row, ranks, image_ranks, real)
    totals = lax.all_to_all(total, AXES, 0, 0, tiled=True)
    return caption_loss.reshape(B), image_loss.reshape(B), jnp.sum(totals[:, 0, 0])


def solution(mesh):
    torus = Mesh(mesh.devices.reshape(*SIZES.values()), AXES)
    return jax.shard_map(
        step,
        mesh=torus,
        in_specs=(P(AXES, None), P(AXES, None), P(AXES), P(AXES)),
        out_specs=(P(AXES), P(AXES), P()),
        check_vma=False,
    )
```

```python
import functools
import itertools

import jax
import jax.numpy as jnp
from jax import lax
from jax.experimental import pallas as pl
from jax.experimental.pallas import tpu as pltpu
from jax.sharding import Mesh
from jax.sharding import PartitionSpec as P


SIZES = {"x": 4, "h": 2, "z": 4, "c": 2, "l": 2}
AXES = tuple(SIZES)
LOG2E = 1.4426950408889634
LN2 = 0.6931471805599453
LOW = -1.0e30

B = 192
E = 768
MET = ((0, 0), (0, 1), (3, 0), (1, 0), (3, 1), (1, 1), (2, 0), (2, 1))
PARTS = ((0, 6), (6, 8))
CAPS = len(MET)
IMGS = 2 * len(MET)
C = IMGS * B
RC = 448
R = -(-CAPS * B // RC) * RC
CAP_ROWS = CAPS * B + RC
NC = 256
COUNTS = (2, 4, 5, 6, 7, 8, 10, 12)
TAIL = 2 * NC
IMG_ROWS = C + TAIL
PIECE = 32
GRAIN = 16
OK_BIT = 15
ABSENT = 9999.0

F32 = jnp.float32
BF16 = jnp.bfloat16
VMEM = pl.BlockSpec(memory_space=pltpu.VMEM)
SMEM = pl.BlockSpec(memory_space=pltpu.SMEM)


def send(value, to):
    pairs = []
    for at in itertools.product(*map(range, SIZES.values())):
        p = dict(zip(AXES, at))
        pairs.append((flat(p), flat({**p, **to(p)})))
    return lax.ppermute(value, AXES, pairs)


def other_core(p):
    return {"c": 1 - p["c"]}


def partner(p):
    return {"l": 1 - p["l"], "h": p["h"] ^ p["c"]}


def along(step):
    def to(p):
        axis = "x" if p["c"] else "z"
        return {axis: (p[axis] + step) % 4}

    return to


def place():
    return {a: lax.axis_index(a) for a in AXES}


def flat(p):
    at = 0
    for a in AXES:
        at = at * SIZES[a] + p[a]
    return at


def moved(p, off):
    q = dict(p)
    for a, d in off.items():
        q[a] = lax.rem(p[a] + d, SIZES[a])
    return q


def cap_place(p, k):
    step, y = MET[k]
    return moved(p, {"z": step, "l": y})


def img_place(p, m):
    step, y = MET[m // 2]
    return {**moved(p, {"x": step, "h": y, "l": y}), "c": m % 2}


def iota(shape, dim):
    return lax.broadcasted_iota(jnp.int32, shape, dim).astype(F32)


def dot(a, b):
    return jnp.dot(a, b, preferred_element_type=F32)


def earlier():
    return jnp.where(iota((B, B), 0) < iota((B, B), 1), 1.0, 0.0).astype(BF16)


def grains(n):
    return lax.shift_left(lax.shift_right_logical(n + (GRAIN - 1), 4), 4)


def pair_kernel(own, cap_other, img_other, word, word_other, carried, words, ranks):
    first = lax.axis_index("c") == 0
    ok = lax.shift_right_logical(
        jnp.concatenate([word[...], word_other[...]], axis=0), OK_BIT
    )
    marks = jnp.broadcast_to(ok[:, None], (2, 8, B)).reshape(16, B).astype(F32).astype(BF16)
    order = dot(marks, earlier())
    found = jnp.where(ok > 0, jnp.concatenate([order[0:1], order[8:9]], axis=0), ABSENT)
    ranks[...] = found[0:1, :]
    both = jnp.where(
        first == (lax.broadcasted_iota(jnp.int32, (2, B), 0) == 0), word[...], word_other[...]
    )
    words[...] = jnp.broadcast_to(both[None], (8, 2, B))
    packed = []
    for i, block in enumerate((own, img_other)):
        pick = jnp.where(iota((B, B), 0) == found[i:i + 1, :], 1.0, 0.0).astype(BF16)
        packed.append(dot(pick, block[...]).astype(BF16))
    carried[0:B, :] = jnp.where(first, own[...], packed[1])
    carried[B:2 * B, :] = jnp.where(first, cap_other[...], packed[0])


def table_row(p):
    return ((p["z"] * 2 + p["l"]) * 8 + p["x"] * 2 + p["h"]) * 2 + p["c"]


def lookup_kernel(table, ranks, columns, counts, real, pos, words_v):
    p = place()
    words = table[...].reshape(128, B)
    words_v[...] = words
    ok = (lax.shift_right_logical(words, OK_BIT) & 1).astype(F32)
    rank = dot(ok.astype(BF16), earlier())
    real[...] = jnp.full((8, 128), jnp.sum(ok), F32)
    known = jnp.transpose(jnp.where(ok > 0, rank + 1.0, 0.0)).astype(BF16)
    for k in range(CAPS):
        row = words_v[pl.ds(table_row(cap_place(p, k)), 1), :]
        pos[k:k + 1, :] = (row & ((1 << OK_BIT) - 1)).astype(F32)
    at = pos[...]
    hi = jnp.floor((at + 0.5) * (1.0 / B))
    lo = at - hi * B
    line = lax.broadcasted_iota(jnp.int32, (128, B), 0)
    bits = lambda low, mask: lax.shift_right_logical(line, low) & mask
    block = (bits(1, 7) * 16 + bits(5, 3) * 4 + bits(0, 1) * 2 + bits(4, 1)).astype(F32)
    inner = iota((B, B), 0)
    for k in range(CAPS):
        pick = jnp.where(block == hi[k:k + 1, :], 1.0, 0.0).astype(BF16)
        column = dot(known, pick)
        pos[k:k + 1, :] = jnp.sum(
            jnp.where(inner == lo[k:k + 1, :], column, 0.0), axis=0, keepdims=True
        )
    value = pos[...]
    live = value > 0.0
    marks = jnp.where(live, 1.0, 0.0)
    order = dot(marks.astype(BF16), earlier())
    ranks[...] = jnp.where(live, order, ABSENT)
    start = jnp.zeros((1, 1), F32)
    base = jnp.full((CAPS, B), -ABSENT, F32)
    counts[0:CAPS, :] = jnp.broadcast_to(
        jnp.sum(marks, axis=1, keepdims=True).astype(jnp.int32), (CAPS, 128)
    )
    for m in range(IMGS):
        number = flat(img_place(p, m))
        row = words_v[pl.ds(table_row(img_place(p, m)), 1), :]
        row = lax.shift_right_logical(row, OK_BIT) & 1
        count = jnp.sum(row.astype(F32), axis=1, keepdims=True)
        base = jnp.where(hi == number.astype(F32), start, base)
        start = start + jnp.floor((count + (GRAIN - 1.0)) * (1.0 / GRAIN)) * GRAIN
        counts[CAPS + m:CAPS + m + 1, :] = jnp.broadcast_to(count.astype(jnp.int32), (1, 128))
    targets = jnp.where(live, base + value - 1.0, -ABSENT)
    order = ranks[...]
    lane = iota((B, 128), 1)
    result = jnp.zeros((B, 128), F32)
    for k in range(CAPS):
        hit = inner == order[k:k + 1, :]
        target = jnp.sum(jnp.where(hit, targets[k:k + 1, :], 0.0), axis=1, keepdims=True)
        result = jnp.where(lane == float(k), target, result)
    columns[...] = result


def starts_of(counts, first, number):
    found, at = [], jnp.int32(0)
    for k in range(number):
        found.append(pl.multiple_of(at, GRAIN))
        at = at + grains(counts[first + k, 0])
    return found + [pl.multiple_of(at, GRAIN)]


def compact(counts, ranks, carried, kept, cap_out, img_out, first):
    core = lax.axis_index("c")
    slot = iota((B, B), 0)
    at = starts_of(counts, 0, CAPS)
    for k, (a, b) in enumerate(zip(carried, kept), first):
        block = jnp.where(core == 0, a[0:B, :], b[B:2 * B, :])
        pick = jnp.where(slot == ranks[k:k + 1, :], 1.0, 0.0).astype(BF16)
        cap_out[pl.ds(at[k], B), :] = dot(pick, block).astype(BF16)
    at = starts_of(counts, CAPS, IMGS)
    for k, (a, b) in enumerate(zip(carried, kept), first):
        for side in range(2):
            rows = pl.ds(side * B, B)
            img_out[pl.ds(at[2 * k + side], B), :] = jnp.where(core == 0, b[rows, :], a[rows, :])


def compact_kernel(part, counts, ranks, *refs):
    first, last = PARTS[part]
    refs = refs[2 if part else 0:]
    number = last - first
    cap_out, img_out = refs[2 * number:]
    compact(counts, ranks, refs[:number], refs[number:2 * number], cap_out, img_out, first)
    if last == CAPS:
        cap_end = starts_of(counts, 0, CAPS)[-1]
        img_end = starts_of(counts, CAPS, IMGS)[-1]
        cap_out[pl.ds(cap_end, RC), :] = jnp.zeros((RC, E), BF16)
        img_out[pl.ds(img_end, TAIL), :] = jnp.zeros((TAIL, E), BF16)


def score_kernel(
    counts, columns, cap_v, img_v, out, own_row,
    t_v, pos_b, bias_b, rmax, rmatch, rsum, col_bias, cmax, cmatch, csum, lines_v,
):
    img_at = starts_of(counts, CAPS, IMGS)
    col_bias[...] = jnp.full((8, C + 384), LOW, F32)
    column = iota((8, 384), 1)
    for m in range(IMGS):
        whole = lax.shift_left(lax.shift_right_logical(img_at[m], 7), 7)
        span = pl.ds(pl.multiple_of(whole, 128), 384)
        begin = (img_at[m] - whole).astype(F32)
        end = begin + counts[CAPS + m, 0].astype(F32)
        inside = (column >= begin) & (column < end)
        col_bias[:, span] = jnp.where(inside, 0.0, col_bias[:, span])
    cap_at = starts_of(counts, 0, CAPS)
    slot = iota((B, 128), 0)
    for k in range(CAPS):
        rows = pl.ds(cap_at[k], B)
        pos_b[rows, :] = jnp.broadcast_to(columns[:, k:k + 1], (B, 128))
        bias_b[rows, :] = jnp.where(slot < counts[k, 0].astype(F32), 0.0, LOW)
    rows_used = cap_at[CAPS]
    tail = pl.ds(rows_used, RC)
    bias_b[tail, :] = jnp.full((RC, 128), LOW, F32)
    pos_b[tail, :] = jnp.full((RC, 128), -ABSENT, F32)
    cmax[...] = jnp.full(cmax.shape, 4.0 * LOW, F32)
    cmatch[...] = jnp.zeros(cmatch.shape, F32)
    csum[...] = jnp.zeros(csum.shape, F32)

    def tiles(count):
        @pl.loop(0, lax.div(rows_used + (RC - 1), RC))
        def _(i):
            rows = pl.ds(pl.multiple_of(i * RC, RC), RC)
            a = cap_v[rows, :]
            for n in range(count):
                s = lax.dot_general(
                    a, img_v[n * NC:(n + 1) * NC, :], (((1,), (1,)), ((), ())),
                    preferred_element_type=F32,
                )
                q = s * LOG2E
                highest, found = None, None
                for half in range(2):
                    span = pl.ds(n * NC + half * 128, 128)
                    qh = q[:, half * 128:(half + 1) * 128]
                    t = (qh + bias_b[rows, :]) + col_bias[0:1, span]
                    t_v[rows, span] = t
                    number = iota((1, 128), 1) + float(n * NC + half * 128)
                    w = jnp.where(pos_b[rows, :] == number, qh, 0.0)
                    highest = t if half == 0 else jnp.maximum(highest, t)
                    found = w if half == 0 else found + w
                    cmax[:, span] = jnp.maximum(
                        cmax[:, span], jnp.max(t.reshape(-1, 8, 128), axis=0)
                    )
                    cmatch[:, span] += jnp.sum(w.reshape(-1, 8, 128), axis=0)
                if n == 0:
                    rmax[rows, :] = highest
                    rmatch[rows, :] = found
                else:
                    rmax[rows, :] = jnp.maximum(rmax[rows, :], highest)
                    rmatch[rows, :] += found
            rmax[rows, :] = jnp.broadcast_to(
                jnp.max(rmax[rows, :], axis=1, keepdims=True), (RC, 128)
            )

        top = jnp.max(cmax[...], axis=0, keepdims=True)
        cmax[...] = jnp.broadcast_to(top, cmax.shape)

        def piece(r, totals):
            rows = pl.ds(pl.multiple_of(r * PIECE, PIECE), PIECE)
            peak = rmax[rows, :]
            acc = jnp.zeros((PIECE, 128), F32)
            out = []
            for n in range(2 * count):
                t = t_v[rows, n * 128:(n + 1) * 128]
                acc = acc + jnp.exp2(t - peak)
                f = jnp.exp2(t.reshape(-1, 8, 128) - cmax[:, n * 128:(n + 1) * 128][None])
                out.append(totals[n] + jnp.sum(f, axis=0))
            rsum[rows, :] = acc
            return tuple(out)

        totals = lax.fori_loop(
            0, lax.div(rows_used + (PIECE - 1), PIECE), piece,
            tuple(jnp.zeros((8, 128), F32) for _ in range(2 * count)),
        )
        for n in range(2 * count):
            csum[:, n * 128:(n + 1) * 128] = totals[n]

    used = jnp.maximum(lax.div(img_at[IMGS] + (NC - 1), NC), 1)
    for below, count in zip((0, *COUNTS), COUNTS):
        pl.when((used > below) & (used <= count))(lambda count=count: tiles(count))

    p = place()
    lanes = lax.broadcasted_iota(jnp.int32, (B, 128), 1)
    for k in range(CAPS):
        rows = pl.ds(cap_at[k], B)
        total = jnp.sum(rsum[rows, :], axis=1, keepdims=True)
        match = jnp.sum(rmatch[rows, :], axis=1, keepdims=True)
        packed = jnp.where(lanes == 0, rmax[rows, :] + jnp.log2(total), match)
        lines = jnp.transpose(packed)
        if k:
            put(out, flat(cap_place(p, k)), lines)
        else:
            put(own_row, 0, lines)
    line = lax.broadcasted_iota(jnp.int32, (8, C), 0)
    total = jnp.sum(csum[...], axis=0, keepdims=True)
    match = jnp.sum(cmatch[...], axis=0, keepdims=True)
    lines_v[:, :C] = jnp.where(line == 0, cmax[0:1, :] + jnp.log2(total), match)
    lines_v[:, C:] = jnp.zeros((8, 384), F32)
    for m in range(IMGS):
        whole = lax.shift_left(lax.shift_right_logical(img_at[m], 7), 7)
        slab = lines_v[:, pl.ds(pl.multiple_of(whole, 128), 384)]
        slab = pltpu.roll(slab, lax.rem(384 - (img_at[m] - whole), 384), 1)
        put(out, flat(img_place(p, m)), slab)


def put(out, at, lines):
    for i in range(2):
        out[at, 0:1, i * B:(i + 1) * B] = lines[i:i + 1, :B]


def joined(parts, ranks):
    sums, matches = parts[:, :B], parts[:, B:]
    peak = jnp.max(sums, axis=0, keepdims=True)
    total = jnp.sum(jnp.exp2(sums - peak), axis=0, keepdims=True)
    match = jnp.sum(matches, axis=0, keepdims=True)
    packed = jnp.broadcast_to(LN2 * (peak - match + jnp.log2(total)), (8, B))
    packed = jnp.concatenate([packed, jnp.zeros((8, 256 - B), F32)], axis=1)
    column = jnp.transpose(packed)[:B, 0:1]
    return jnp.sum(jnp.where(iota((B, B), 0) == ranks, column, 0.0), axis=0, keepdims=True)


def loss_kernel(
    parts, own_row, row_ranks, col_ranks, real, caption_loss, image_loss, total, rows, cols
):
    p = place()
    rows[0:1, :] = own_row[0, :, :]
    for k in range(1, CAPS):
        rows[k:k + 1, :] = parts[flat(cap_place(p, k)), :, :]
    for m in range(IMGS):
        cols[m:m + 1, :] = parts[flat(img_place(p, m)), :, :]
    caption = joined(rows[...], row_ranks[0:1, :])
    image = joined(cols[...], col_ranks[...])
    caption_loss[...] = caption
    image_loss[...] = image
    both = jnp.sum(caption, axis=1, keepdims=True) + jnp.sum(image, axis=1, keepdims=True)
    share = both / (2.0 * real[0:1, 0:1])
    total[...] = jnp.broadcast_to(share, (128, 8)).reshape(128, 1, 8)


def small(mib, flops):
    return dict(
        compiler_params=pltpu.CompilerParams(vmem_limit_bytes=mib * 1024 * 1024),
        cost_estimate=pl.CostEstimate(flops=flops, bytes_accessed=10**6, transcendentals=0),
    )


def step(captions, images, positives, valid):
    shape = jax.ShapeDtypeStruct
    pair = shape((2 * B, E), BF16)
    word = (positives + valid * (1 << OK_BIT))[None]
    others = [send(value, other_core) for value in (captions, images, word)]
    own = jnp.where(lax.axis_index("c") == 0, captions, images)
    carried, words, image_ranks = pl.pallas_call(
        pair_kernel,
        out_shape=[pair, shape((8, 2, B), jnp.int32), shape((1, B), F32)],
        in_specs=[VMEM] * 5,
        out_specs=[VMEM] * 3,
        **small(8, 10**8),
    )(own, others[0], others[1], word, others[2])
    near = send(carried, partner)
    a1, a3 = (send(carried, along(s)) for s in (1, 3))
    b1, b3 = (send(near, along(s)) for s in (1, 3))
    c1, c3 = send(a1, along(1)), send(b3, along(3))
    met = dict(own=carried, y=near, a1=a1, a3=a3, b1=b1, b3=b3, c1=c1, c3=c3)
    swapped = [send(v, other_core) for v in met.values()]
    carried = list(met.values())
    part = lax.all_to_all(words, ("x", "h"), 0, 0, tiled=True)
    part = jnp.broadcast_to(part.reshape(1, 16, B), (8, 16, B))
    table = lax.all_to_all(part, ("z", "l"), 0, 0, tiled=True)
    ranks, columns, counts, real = pl.pallas_call(
        lookup_kernel,
        out_shape=[
            shape((CAPS, B), F32), shape((B, 128), F32),
            shape((CAPS + IMGS, 128), jnp.int32), shape((8, 128), F32),
        ],
        in_specs=[VMEM],
        out_specs=[VMEM] * 4,
        scratch_shapes=[pltpu.VMEM((CAPS, B), F32), pltpu.VMEM((128, B), jnp.int32)],
        **small(4, 3 * 10**9),
    )(table)
    buffers = []
    for part, (first, last) in enumerate(PARTS):
        buffers = pl.pallas_call(
            functools.partial(compact_kernel, part),
            out_shape=[shape((CAP_ROWS, E), BF16), shape((IMG_ROWS, E), BF16)],
            in_specs=[SMEM] + [VMEM] * (1 + len(buffers) + 2 * (last - first)),
            out_specs=[VMEM] * 2,
            input_output_aliases={2: 0, 3: 1} if part else {},
            **small(10, 10**9),
        )(counts, ranks, *buffers, *carried[first:last], *swapped[first:last])
    cap_v, img_v = buffers
    out, own_row = pl.pallas_call(
        score_kernel,
        out_shape=[shape((n, 1, 2 * B), F32) for n in (128, 1)],
        in_specs=[SMEM] + [VMEM] * 3,
        out_specs=[VMEM] * 2,
        scratch_shapes=[
            pltpu.VMEM((R, C), F32),
            *[pltpu.VMEM((R + RC, 128), F32)] * 5,
            pltpu.VMEM((8, C + 384), F32),
            *[pltpu.VMEM((8, C), F32)] * 3,
            pltpu.VMEM((8, C + 384), F32),
        ],
        compiler_params=pltpu.CompilerParams(vmem_limit_bytes=31 * 1024 * 1024),
        cost_estimate=pl.CostEstimate(
            flops=R * C * E, bytes_accessed=2 * (R + C) * E, transcendentals=R * C
        ),
    )(counts, columns, cap_v, img_v)
    parts = lax.all_to_all(out, AXES, 0, 0, tiled=True)
    caption_loss, image_loss, total = pl.pallas_call(
        loss_kernel,
        out_shape=[shape((1, B), F32), shape((1, B), F32), shape((128, 1, 8), F32)],
        in_specs=[VMEM] * 5,
        out_specs=[VMEM] * 3,
        scratch_shapes=[pltpu.VMEM((CAPS, 2 * B), F32), pltpu.VMEM((IMGS, 2 * B), F32)],
        **small(4, 10**8),
    )(parts, own_row, ranks, image_ranks, real)
    totals = lax.all_to_all(total, AXES, 0, 0, tiled=True)
    return caption_loss.reshape(B), image_loss.reshape(B), jnp.sum(totals[:, 0, 0])


def solution(mesh):
    torus = Mesh(mesh.devices.reshape(*SIZES.values()), AXES)
    return jax.shard_map(
        step,
        mesh=torus,
        in_specs=(P(AXES, None), P(AXES, None), P(AXES), P(AXES)),
        out_specs=(P(AXES), P(AXES), P()),
        check_vma=False,
    )
```

```python
import functools
import itertools

import jax
import jax.numpy as jnp
from jax import lax
from jax.experimental import pallas as pl
from jax.experimental.pallas import tpu as pltpu
from jax.sharding import Mesh
from jax.sharding import PartitionSpec as P


SIZES = {"x": 4, "h": 2, "z": 4, "c": 2, "l": 2}
AXES = tuple(SIZES)
LOG2E = 1.4426950408889634
LN2 = 0.6931471805599453
LOW = -1.0e30

B = 192
E = 768
MET = ((0, 0), (0, 1), (3, 0), (1, 0), (3, 1), (1, 1), (2, 0), (2, 1))
PARTS = ((0, 6), (6, 8))
CAPS = len(MET)
IMGS = 2 * len(MET)
C = IMGS * B
RC = 448
R = -(-CAPS * B // RC) * RC
CAP_ROWS = CAPS * B + RC
NC = 256
COUNTS = (2, 4, 5, 6, 7, 8, 10, 12)
TAIL = 2 * NC
IMG_ROWS = C + TAIL
PIECE = 32
GRAIN = 16
OK_BIT = 15
ABSENT = 9999.0

F32 = jnp.float32
BF16 = jnp.bfloat16
VMEM = pl.BlockSpec(memory_space=pltpu.VMEM)
SMEM = pl.BlockSpec(memory_space=pltpu.SMEM)


def send(value, to):
    pairs = []
    for at in itertools.product(*map(range, SIZES.values())):
        p = dict(zip(AXES, at))
        pairs.append((flat(p), flat({**p, **to(p)})))
    return lax.ppermute(value, AXES, pairs)


def other_core(p):
    return {"c": 1 - p["c"]}


def partner(p):
    return {"l": 1 - p["l"], "h": p["h"] ^ p["c"]}


def along(step):
    def to(p):
        axis = "x" if p["c"] else "z"
        return {axis: (p[axis] + step) % 4}

    return to


def place():
    return {a: lax.axis_index(a) for a in AXES}


def flat(p):
    at = 0
    for a in AXES:
        at = at * SIZES[a] + p[a]
    return at


def moved(p, off):
    q = dict(p)
    for a, d in off.items():
        q[a] = lax.rem(p[a] + d, SIZES[a])
    return q


def cap_place(p, k):
    step, y = MET[k]
    return moved(p, {"z": step, "l": y})


def img_place(p, m):
    step, y = MET[m // 2]
    return {**moved(p, {"x": step, "h": y, "l": y}), "c": m % 2}


def iota(shape, dim):
    return lax.broadcasted_iota(jnp.int32, shape, dim).astype(F32)


def dot(a, b):
    return jnp.dot(a, b, preferred_element_type=F32)


def earlier():
    return jnp.where(iota((B, B), 0) < iota((B, B), 1), 1.0, 0.0).astype(BF16)


def grains(n):
    return lax.shift_left(lax.shift_right_logical(n + (GRAIN - 1), 4), 4)


def pair_kernel(own, cap_other, img_other, word, word_other, carried, words, ranks):
    first = lax.axis_index("c") == 0
    ok = lax.shift_right_logical(
        jnp.concatenate([word[...], word_other[...]], axis=0), OK_BIT
    )
    marks = jnp.broadcast_to(ok[:, None], (2, 8, B)).reshape(16, B).astype(F32).astype(BF16)
    order = dot(marks, earlier())
    found = jnp.where(ok > 0, jnp.concatenate([order[0:1], order[8:9]], axis=0), ABSENT)
    ranks[...] = found[0:1, :]
    both = jnp.where(
        first == (lax.broadcasted_iota(jnp.int32, (2, B), 0) == 0), word[...], word_other[...]
    )
    words[...] = jnp.broadcast_to(both[None], (8, 2, B))
    packed = []
    for i, block in enumerate((own, img_other)):
        pick = jnp.where(iota((B, B), 0) == found[i:i + 1, :], 1.0, 0.0).astype(BF16)
        packed.append(dot(pick, block[...]).astype(BF16))
    carried[0:B, :] = jnp.where(first, own[...], packed[1])
    carried[B:2 * B, :] = jnp.where(first, cap_other[...], packed[0])


def spread_kernel(part, words):
    words[...] = jnp.broadcast_to(part[...].reshape(1, 16, B), (8, 16, B))


def table_row(p):
    return ((p["z"] * 2 + p["l"]) * 8 + p["x"] * 2 + p["h"]) * 2 + p["c"]


def lookup_kernel(table, ranks, columns, counts, real, pos, words_v):
    p = place()
    words = table[...].reshape(128, B)
    words_v[...] = words
    ok = (lax.shift_right_logical(words, OK_BIT) & 1).astype(F32)
    rank = dot(ok.astype(BF16), earlier())
    real[...] = jnp.full((8, 128), jnp.sum(ok), F32)
    known = jnp.transpose(jnp.where(ok > 0, rank + 1.0, 0.0)).astype(BF16)
    for k in range(CAPS):
        row = words_v[pl.ds(table_row(cap_place(p, k)), 1), :]
        pos[k:k + 1, :] = (row & ((1 << OK_BIT) - 1)).astype(F32)
    at = pos[...]
    hi = jnp.floor((at + 0.5) * (1.0 / B))
    lo = at - hi * B
    line = lax.broadcasted_iota(jnp.int32, (128, B), 0)
    bits = lambda low, mask: lax.shift_right_logical(line, low) & mask
    block = (bits(1, 7) * 16 + bits(5, 3) * 4 + bits(0, 1) * 2 + bits(4, 1)).astype(F32)
    inner = iota((B, B), 0)
    for k in range(CAPS):
        pick = jnp.where(block == hi[k:k + 1, :], 1.0, 0.0).astype(BF16)
        column = dot(known, pick)
        pos[k:k + 1, :] = jnp.sum(
            jnp.where(inner == lo[k:k + 1, :], column, 0.0), axis=0, keepdims=True
        )
    value = pos[...]
    live = value > 0.0
    marks = jnp.where(live, 1.0, 0.0)
    order = dot(marks.astype(BF16), earlier())
    ranks[...] = jnp.where(live, order, ABSENT)
    start = jnp.zeros((1, 1), F32)
    base = jnp.full((CAPS, B), -ABSENT, F32)
    counts[0:CAPS, :] = jnp.broadcast_to(
        jnp.sum(marks, axis=1, keepdims=True).astype(jnp.int32), (CAPS, 128)
    )
    for m in range(IMGS):
        number = flat(img_place(p, m))
        row = words_v[pl.ds(table_row(img_place(p, m)), 1), :]
        row = lax.shift_right_logical(row, OK_BIT) & 1
        count = jnp.sum(row.astype(F32), axis=1, keepdims=True)
        base = jnp.where(hi == number.astype(F32), start, base)
        start = start + jnp.floor((count + (GRAIN - 1.0)) * (1.0 / GRAIN)) * GRAIN
        counts[CAPS + m:CAPS + m + 1, :] = jnp.broadcast_to(count.astype(jnp.int32), (1, 128))
    targets = jnp.where(live, base + value - 1.0, -ABSENT)
    order = ranks[...]
    lane = iota((B, 128), 1)
    result = jnp.zeros((B, 128), F32)
    for k in range(CAPS):
        hit = inner == order[k:k + 1, :]
        target = jnp.sum(jnp.where(hit, targets[k:k + 1, :], 0.0), axis=1, keepdims=True)
        result = jnp.where(lane == float(k), target, result)
    columns[...] = result


def starts_of(counts, first, number):
    found, at = [], jnp.int32(0)
    for k in range(number):
        found.append(pl.multiple_of(at, GRAIN))
        at = at + grains(counts[first + k, 0])
    return found + [pl.multiple_of(at, GRAIN)]


def compact(counts, ranks, carried, kept, cap_out, img_out, first):
    core = lax.axis_index("c")
    slot = iota((B, B), 0)
    at = starts_of(counts, 0, CAPS)
    for k, (a, b) in enumerate(zip(carried, kept), first):
        block = jnp.where(core == 0, a[0:B, :], b[B:2 * B, :])
        pick = jnp.where(slot == ranks[k:k + 1, :], 1.0, 0.0).astype(BF16)
        cap_out[pl.ds(at[k], B), :] = dot(pick, block).astype(BF16)
    at = starts_of(counts, CAPS, IMGS)
    for k, (a, b) in enumerate(zip(carried, kept), first):
        for side in range(2):
            rows = pl.ds(side * B, B)
            img_out[pl.ds(at[2 * k + side], B), :] = jnp.where(core == 0, b[rows, :], a[rows, :])


def compact_kernel(part, counts, ranks, *refs):
    first, last = PARTS[part]
    refs = refs[2 if part else 0:]
    number = last - first
    cap_out, img_out = refs[2 * number:]
    if part == 0:
        cap_end = starts_of(counts, 0, CAPS)[-1]
        img_end = starts_of(counts, CAPS, IMGS)[-1]
        cap_out[pl.ds(cap_end, RC), :] = jnp.zeros((RC, E), BF16)
        img_out[pl.ds(img_end, TAIL), :] = jnp.zeros((TAIL, E), BF16)
    compact(counts, ranks, refs[:number], refs[number:2 * number], cap_out, img_out, first)


def score_kernel(
    counts, columns, cap_v, img_v, out, own_row,
    t_v, pos_b, bias_b, rmax, rmatch, rsum, col_bias, cmax, cmatch, csum, lines_v,
):
    img_at = starts_of(counts, CAPS, IMGS)
    col_bias[...] = jnp.full((8, C + 384), LOW, F32)
    column = iota((8, 384), 1)
    for m in range(IMGS):
        whole = lax.shift_left(lax.shift_right_logical(img_at[m], 7), 7)
        span = pl.ds(pl.multiple_of(whole, 128), 384)
        begin = (img_at[m] - whole).astype(F32)
        end = begin + counts[CAPS + m, 0].astype(F32)
        inside = (column >= begin) & (column < end)
        col_bias[:, span] = jnp.where(inside, 0.0, col_bias[:, span])
    cap_at = starts_of(counts, 0, CAPS)
    slot = iota((B, 128), 0)
    for k in range(CAPS):
        rows = pl.ds(cap_at[k], B)
        pos_b[rows, :] = jnp.broadcast_to(columns[:, k:k + 1], (B, 128))
        bias_b[rows, :] = jnp.where(slot < counts[k, 0].astype(F32), 0.0, LOW)
    rows_used = cap_at[CAPS]
    tail = pl.ds(rows_used, RC)
    bias_b[tail, :] = jnp.full((RC, 128), LOW, F32)
    pos_b[tail, :] = jnp.full((RC, 128), -ABSENT, F32)
    cmax[...] = jnp.full(cmax.shape, 4.0 * LOW, F32)
    cmatch[...] = jnp.zeros(cmatch.shape, F32)
    csum[...] = jnp.zeros(csum.shape, F32)

    def tiles(count):
        @pl.loop(0, lax.div(rows_used + (RC - 1), RC))
        def _(i):
            rows = pl.ds(pl.multiple_of(i * RC, RC), RC)
            a = cap_v[rows, :]
            for n in range(count):
                s = lax.dot_general(
                    a, img_v[n * NC:(n + 1) * NC, :], (((1,), (1,)), ((), ())),
                    preferred_element_type=F32,
                )
                q = s * LOG2E
                highest, found = None, None
                for half in range(2):
                    span = pl.ds(n * NC + half * 128, 128)
                    qh = q[:, half * 128:(half + 1) * 128]
                    t = (qh + bias_b[rows, :]) + col_bias[0:1, span]
                    t_v[rows, span] = t
                    number = iota((1, 128), 1) + float(n * NC + half * 128)
                    w = jnp.where(pos_b[rows, :] == number, qh, 0.0)
                    highest = t if half == 0 else jnp.maximum(highest, t)
                    found = w if half == 0 else found + w
                    cmax[:, span] = jnp.maximum(
                        cmax[:, span], jnp.max(t.reshape(-1, 8, 128), axis=0)
                    )
                    cmatch[:, span] += jnp.sum(w.reshape(-1, 8, 128), axis=0)
                if n == 0:
                    rmax[rows, :] = highest
                    rmatch[rows, :] = found
                else:
                    rmax[rows, :] = jnp.maximum(rmax[rows, :], highest)
                    rmatch[rows, :] += found
            rmax[rows, :] = jnp.broadcast_to(
                jnp.max(rmax[rows, :], axis=1, keepdims=True), (RC, 128)
            )

        top = jnp.max(cmax[...], axis=0, keepdims=True)
        cmax[...] = jnp.broadcast_to(top, cmax.shape)

        def piece(r, totals):
            rows = pl.ds(pl.multiple_of(r * PIECE, PIECE), PIECE)
            peak = rmax[rows, :]
            acc = jnp.zeros((PIECE, 128), F32)
            out = []
            for n in range(2 * count):
                t = t_v[rows, n * 128:(n + 1) * 128]
                acc = acc + jnp.exp2(t - peak)
                f = jnp.exp2(t.reshape(-1, 8, 128) - cmax[:, n * 128:(n + 1) * 128][None])
                out.append(totals[n] + jnp.sum(f, axis=0))
            rsum[rows, :] = acc
            return tuple(out)

        totals = lax.fori_loop(
            0, lax.div(rows_used + (PIECE - 1), PIECE), piece,
            tuple(jnp.zeros((8, 128), F32) for _ in range(2 * count)),
        )
        for n in range(2 * count):
            csum[:, n * 128:(n + 1) * 128] = totals[n]

    used = jnp.maximum(lax.div(img_at[IMGS] + (NC - 1), NC), 1)
    for below, count in zip((0, *COUNTS), COUNTS):
        pl.when((used > below) & (used <= count))(lambda count=count: tiles(count))

    p = place()
    lanes = lax.broadcasted_iota(jnp.int32, (B, 128), 1)
    for k in range(CAPS):
        rows = pl.ds(cap_at[k], B)
        total = jnp.sum(rsum[rows, :], axis=1, keepdims=True)
        match = jnp.sum(rmatch[rows, :], axis=1, keepdims=True)
        packed = jnp.where(lanes == 0, rmax[rows, :] + jnp.log2(total), match)
        lines = jnp.transpose(packed)
        if k:
            put(out, flat(cap_place(p, k)), lines)
        else:
            put(own_row, 0, lines)
    line = lax.broadcasted_iota(jnp.int32, (8, C), 0)
    total = jnp.sum(csum[...], axis=0, keepdims=True)
    match = jnp.sum(cmatch[...], axis=0, keepdims=True)
    lines_v[:, :C] = jnp.where(line == 0, cmax[0:1, :] + jnp.log2(total), match)
    lines_v[:, C:] = jnp.zeros((8, 384), F32)
    for m in range(IMGS):
        whole = lax.shift_left(lax.shift_right_logical(img_at[m], 7), 7)
        slab = lines_v[:, pl.ds(pl.multiple_of(whole, 128), 384)]
        slab = pltpu.roll(slab, lax.rem(384 - (img_at[m] - whole), 384), 1)
        put(out, flat(img_place(p, m)), slab)


def put(out, at, lines):
    for i in range(2):
        out[at, 0:1, i * B:(i + 1) * B] = lines[i:i + 1, :B]


def joined(parts, ranks):
    sums, matches = parts[:, :B], parts[:, B:]
    peak = jnp.max(sums, axis=0, keepdims=True)
    total = jnp.sum(jnp.exp2(sums - peak), axis=0, keepdims=True)
    match = jnp.sum(matches, axis=0, keepdims=True)
    packed = jnp.broadcast_to(LN2 * (peak - match + jnp.log2(total)), (8, B))
    packed = jnp.concatenate([packed, jnp.zeros((8, 256 - B), F32)], axis=1)
    column = jnp.transpose(packed)[:B, 0:1]
    return jnp.sum(jnp.where(iota((B, B), 0) == ranks, column, 0.0), axis=0, keepdims=True)


def loss_kernel(
    parts, own_row, row_ranks, col_ranks, real, caption_loss, image_loss, total, rows, cols
):
    p = place()
    rows[0:1, :] = own_row[0, :, :]
    for k in range(1, CAPS):
        rows[k:k + 1, :] = parts[flat(cap_place(p, k)), :, :]
    for m in range(IMGS):
        cols[m:m + 1, :] = parts[flat(img_place(p, m)), :, :]
    caption = joined(rows[...], row_ranks[0:1, :])
    image = joined(cols[...], col_ranks[...])
    caption_loss[...] = caption
    image_loss[...] = image
    both = jnp.sum(caption, axis=1, keepdims=True) + jnp.sum(image, axis=1, keepdims=True)
    share = both / (2.0 * real[0:1, 0:1])
    total[...] = jnp.broadcast_to(share, (128, 8)).reshape(128, 1, 8)


def small(mib, flops):
    return dict(
        compiler_params=pltpu.CompilerParams(vmem_limit_bytes=mib * 1024 * 1024),
        cost_estimate=pl.CostEstimate(flops=flops, bytes_accessed=10**6, transcendentals=0),
    )


def step(captions, images, positives, valid):
    shape = jax.ShapeDtypeStruct
    pair = shape((2 * B, E), BF16)
    word = (positives + valid * (1 << OK_BIT))[None]
    others = [send(value, other_core) for value in (captions, images, word)]
    own = jnp.where(lax.axis_index("c") == 0, captions, images)
    carried, words, image_ranks = pl.pallas_call(
        pair_kernel,
        out_shape=[pair, shape((8, 2, B), jnp.int32), shape((1, B), F32)],
        in_specs=[VMEM] * 5,
        out_specs=[VMEM] * 3,
        **small(8, 10**8),
    )(own, others[0], others[1], word, others[2])
    near = send(carried, partner)
    a1, a3 = (send(carried, along(s)) for s in (1, 3))
    b1, b3 = (send(near, along(s)) for s in (1, 3))
    c1, c3 = send(a1, along(1)), send(b3, along(3))
    met = dict(own=carried, y=near, a1=a1, a3=a3, b1=b1, b3=b3, c1=c1, c3=c3)
    swapped = [send(v, other_core) for v in met.values()]
    carried = list(met.values())
    part = lax.all_to_all(words, ("x", "h"), 0, 0, tiled=True)
    part = pl.pallas_call(
        spread_kernel, out_shape=shape((8, 16, B), jnp.int32), in_specs=[VMEM],
        out_specs=VMEM, **small(62, 10**8),
    )(part)
    table = lax.all_to_all(part, ("z", "l"), 0, 0, tiled=True)
    ranks, columns, counts, real = pl.pallas_call(
        lookup_kernel,
        out_shape=[
            shape((CAPS, B), F32), shape((B, 128), F32),
            shape((CAPS + IMGS, 128), jnp.int32), shape((8, 128), F32),
        ],
        in_specs=[VMEM],
        out_specs=[VMEM] * 4,
        scratch_shapes=[pltpu.VMEM((CAPS, B), F32), pltpu.VMEM((128, B), jnp.int32)],
        **small(4, 3 * 10**9),
    )(table)
    buffers = []
    for part, (first, last) in enumerate(PARTS):
        buffers = pl.pallas_call(
            functools.partial(compact_kernel, part),
            out_shape=[shape((CAP_ROWS, E), BF16), shape((IMG_ROWS, E), BF16)],
            in_specs=[SMEM] + [VMEM] * (1 + len(buffers) + 2 * (last - first)),
            out_specs=[VMEM] * 2,
            input_output_aliases={2: 0, 3: 1} if part else {},
            **small(10, 10**9),
        )(counts, ranks, *buffers, *carried[first:last], *swapped[first:last])
    cap_v, img_v = buffers
    out, own_row = pl.pallas_call(
        score_kernel,
        out_shape=[shape((n, 1, 2 * B), F32) for n in (128, 1)],
        in_specs=[SMEM] + [VMEM] * 3,
        out_specs=[VMEM] * 2,
        scratch_shapes=[
            pltpu.VMEM((R, C), F32),
            *[pltpu.VMEM((R + RC, 128), F32)] * 5,
            pltpu.VMEM((8, C + 384), F32),
            *[pltpu.VMEM((8, C), F32)] * 3,
            pltpu.VMEM((8, C + 384), F32),
        ],
        compiler_params=pltpu.CompilerParams(vmem_limit_bytes=31 * 1024 * 1024),
        cost_estimate=pl.CostEstimate(
            flops=R * C * E, bytes_accessed=2 * (R + C) * E, transcendentals=R * C
        ),
    )(counts, columns, cap_v, img_v)
    parts = lax.all_to_all(out, AXES, 0, 0, tiled=True)
    caption_loss, image_loss, total = pl.pallas_call(
        loss_kernel,
        out_shape=[shape((1, B), F32), shape((1, B), F32), shape((128, 1, 8), F32)],
        in_specs=[VMEM] * 5,
        out_specs=[VMEM] * 3,
        scratch_shapes=[pltpu.VMEM((CAPS, 2 * B), F32), pltpu.VMEM((IMGS, 2 * B), F32)],
        **small(4, 10**8),
    )(parts, own_row, ranks, image_ranks, real)
    totals = lax.all_to_all(total, AXES, 0, 0, tiled=True)
    return caption_loss.reshape(B), image_loss.reshape(B), jnp.sum(totals[:, 0, 0])


def solution(mesh):
    torus = Mesh(mesh.devices.reshape(*SIZES.values()), AXES)
    return jax.shard_map(
        step,
        mesh=torus,
        in_specs=(P(AXES, None), P(AXES, None), P(AXES), P(AXES)),
        out_specs=(P(AXES), P(AXES), P()),
        check_vma=False,
    )
```

```python
import functools
import itertools

import jax
import jax.numpy as jnp
from jax import lax
from jax.experimental import pallas as pl
from jax.experimental.pallas import tpu as pltpu
from jax.sharding import Mesh
from jax.sharding import PartitionSpec as P


SIZES = {"x": 4, "h": 2, "z": 4, "c": 2, "l": 2}
AXES = tuple(SIZES)
LOG2E = 1.4426950408889634
LN2 = 0.6931471805599453
LOW = -1.0e30

B = 192
E = 768
MET = ((0, 0), (0, 1), (3, 0), (1, 0), (3, 1), (1, 1), (2, 0), (2, 1))
PARTS = ((0, 6), (6, 8))
CAPS = len(MET)
IMGS = 2 * len(MET)
C = IMGS * B
RC = 448
R = -(-CAPS * B // RC) * RC
CAP_ROWS = CAPS * B + RC
NC = 256
COUNTS = (2, 4, 5, 6, 7, 8, 10, 12)
TAIL = 2 * NC
IMG_ROWS = C + TAIL
PIECE = 32
SPAN = 7 * 128
GRAIN = 16
OK_BIT = 15
ABSENT = 9999.0

F32 = jnp.float32
BF16 = jnp.bfloat16
VMEM = pl.BlockSpec(memory_space=pltpu.VMEM)
SMEM = pl.BlockSpec(memory_space=pltpu.SMEM)


def send(value, to):
    pairs = []
    for at in itertools.product(*map(range, SIZES.values())):
        p = dict(zip(AXES, at))
        pairs.append((flat(p), flat({**p, **to(p)})))
    return lax.ppermute(value, AXES, pairs)


def other_core(p):
    return {"c": 1 - p["c"]}


def partner(p):
    return {"l": 1 - p["l"], "h": p["h"] ^ p["c"]}


def along(step):
    def to(p):
        axis = "x" if p["c"] else "z"
        return {axis: (p[axis] + step) % 4}

    return to


def place():
    return {a: lax.axis_index(a) for a in AXES}


def flat(p):
    at = 0
    for a in AXES:
        at = at * SIZES[a] + p[a]
    return at


def moved(p, off):
    q = dict(p)
    for a, d in off.items():
        q[a] = lax.rem(p[a] + d, SIZES[a])
    return q


def cap_place(p, k):
    step, y = MET[k]
    return moved(p, {"z": step, "l": y})


def img_place(p, m):
    step, y = MET[m // 2]
    return {**moved(p, {"x": step, "h": y, "l": y}), "c": m % 2}


def iota(shape, dim):
    return lax.broadcasted_iota(jnp.int32, shape, dim).astype(F32)


def dot(a, b):
    return jnp.dot(a, b, preferred_element_type=F32)


def earlier():
    return jnp.where(iota((B, B), 0) < iota((B, B), 1), 1.0, 0.0).astype(BF16)


def grains(n):
    return lax.shift_left(lax.shift_right_logical(n + (GRAIN - 1), 4), 4)


def pair_kernel(own, cap_other, img_other, word, word_other, carried, words, ranks):
    first = lax.axis_index("c") == 0
    ok = lax.shift_right_logical(
        jnp.concatenate([word[...], word_other[...]], axis=0), OK_BIT
    )
    marks = jnp.broadcast_to(ok[:, None], (2, 8, B)).reshape(16, B).astype(F32).astype(BF16)
    order = dot(marks, earlier())
    found = jnp.where(ok > 0, jnp.concatenate([order[0:1], order[8:9]], axis=0), ABSENT)
    ranks[...] = found[0:1, :]
    both = jnp.where(
        first == (lax.broadcasted_iota(jnp.int32, (2, B), 0) == 0), word[...], word_other[...]
    )
    words[...] = jnp.broadcast_to(both[None], (8, 2, B))
    packed = []
    for i, block in enumerate((own, img_other)):
        pick = jnp.where(iota((B, B), 0) == found[i:i + 1, :], 1.0, 0.0).astype(BF16)
        packed.append(dot(pick, block[...]).astype(BF16))
    carried[0:B, :] = jnp.where(first, own[...], packed[1])
    carried[B:2 * B, :] = jnp.where(first, cap_other[...], packed[0])


def spread_kernel(part, words):
    words[...] = jnp.broadcast_to(part[...].reshape(1, 16, B), (8, 16, B))


def table_row(p):
    return ((p["z"] * 2 + p["l"]) * 8 + p["x"] * 2 + p["h"]) * 2 + p["c"]


def lookup_kernel(table, ranks, columns, counts, real, pos, words_v):
    p = place()
    words = table[...].reshape(128, B)
    words_v[...] = words
    ok = (lax.shift_right_logical(words, OK_BIT) & 1).astype(F32)
    rank = dot(ok.astype(BF16), earlier())
    real[...] = jnp.full((8, 128), jnp.sum(ok), F32)
    known = jnp.transpose(jnp.where(ok > 0, rank + 1.0, 0.0)).astype(BF16)
    for k in range(CAPS):
        row = words_v[pl.ds(table_row(cap_place(p, k)), 1), :]
        pos[k:k + 1, :] = (row & ((1 << OK_BIT) - 1)).astype(F32)
    at = pos[...]
    hi = jnp.floor((at + 0.5) * (1.0 / B))
    lo = at - hi * B
    line = lax.broadcasted_iota(jnp.int32, (128, B), 0)
    bits = lambda low, mask: lax.shift_right_logical(line, low) & mask
    block = (bits(1, 7) * 16 + bits(5, 3) * 4 + bits(0, 1) * 2 + bits(4, 1)).astype(F32)
    inner = iota((B, B), 0)
    for k in range(CAPS):
        pick = jnp.where(block == hi[k:k + 1, :], 1.0, 0.0).astype(BF16)
        column = dot(known, pick)
        pos[k:k + 1, :] = jnp.sum(
            jnp.where(inner == lo[k:k + 1, :], column, 0.0), axis=0, keepdims=True
        )
    value = pos[...]
    live = value > 0.0
    marks = jnp.where(live, 1.0, 0.0)
    order = dot(marks.astype(BF16), earlier())
    ranks[...] = jnp.where(live, order, ABSENT)
    start = jnp.zeros((1, 1), F32)
    base = jnp.full((CAPS, B), -ABSENT, F32)
    counts[0:CAPS, :] = jnp.broadcast_to(
        jnp.sum(marks, axis=1, keepdims=True).astype(jnp.int32), (CAPS, 128)
    )
    for m in range(IMGS):
        number = flat(img_place(p, m))
        row = words_v[pl.ds(table_row(img_place(p, m)), 1), :]
        row = lax.shift_right_logical(row, OK_BIT) & 1
        count = jnp.sum(row.astype(F32), axis=1, keepdims=True)
        base = jnp.where(hi == number.astype(F32), start, base)
        start = start + jnp.floor((count + (GRAIN - 1.0)) * (1.0 / GRAIN)) * GRAIN
        counts[CAPS + m:CAPS + m + 1, :] = jnp.broadcast_to(count.astype(jnp.int32), (1, 128))
    targets = jnp.where(live, base + value - 1.0, -ABSENT)
    order = ranks[...]
    lane = iota((B, 128), 1)
    result = jnp.zeros((B, 128), F32)
    for k in range(CAPS):
        hit = inner == order[k:k + 1, :]
        target = jnp.sum(jnp.where(hit, targets[k:k + 1, :], 0.0), axis=1, keepdims=True)
        result = jnp.where(lane == float(k), target, result)
    columns[...] = result


def starts_of(counts, first, number):
    found, at = [], jnp.int32(0)
    for k in range(number):
        found.append(pl.multiple_of(at, GRAIN))
        at = at + grains(counts[first + k, 0])
    return found + [pl.multiple_of(at, GRAIN)]


def compact(counts, ranks, carried, kept, cap_out, img_out, first):
    core = lax.axis_index("c")
    slot = iota((B, B), 0)
    at = starts_of(counts, 0, CAPS)
    for k, (a, b) in enumerate(zip(carried, kept), first):
        block = jnp.where(core == 0, a[0:B, :], b[B:2 * B, :])
        pick = jnp.where(slot == ranks[k:k + 1, :], 1.0, 0.0).astype(BF16)
        cap_out[pl.ds(at[k], B), :] = dot(pick, block).astype(BF16)
    at = starts_of(counts, CAPS, IMGS)
    for k, (a, b) in enumerate(zip(carried, kept), first):
        for side in range(2):
            rows = pl.ds(side * B, B)
            img_out[pl.ds(at[2 * k + side], B), :] = jnp.where(core == 0, b[rows, :], a[rows, :])


def compact_kernel(part, counts, ranks, *refs):
    first, last = PARTS[part]
    refs = refs[2 if part else 0:]
    number = last - first
    cap_out, img_out = refs[2 * number:]
    if part == 0:
        cap_end = starts_of(counts, 0, CAPS)[-1]
        img_end = starts_of(counts, CAPS, IMGS)[-1]
        cap_out[pl.ds(cap_end, RC), :] = jnp.zeros((RC, E), BF16)
        img_out[pl.ds(img_end, TAIL), :] = jnp.zeros((TAIL, E), BF16)
    compact(counts, ranks, refs[:number], refs[number:2 * number], cap_out, img_out, first)


def score_kernel(
    counts, columns, cap_v, img_v, out, own_row,
    t_v, pos_b, bias_b, rmax, rmatch, rsum, col_bias, cmax, cmatch, csum, lines_v, row_lines,
):
    img_at = starts_of(counts, CAPS, IMGS)
    col_bias[...] = jnp.full((8, C + 384), LOW, F32)
    column = iota((8, 384), 1)
    for m in range(IMGS):
        whole = lax.shift_left(lax.shift_right_logical(img_at[m], 7), 7)
        span = pl.ds(pl.multiple_of(whole, 128), 384)
        begin = (img_at[m] - whole).astype(F32)
        end = begin + counts[CAPS + m, 0].astype(F32)
        inside = (column >= begin) & (column < end)
        col_bias[:, span] = jnp.where(inside, 0.0, col_bias[:, span])
    cap_at = starts_of(counts, 0, CAPS)
    slot = iota((B, 128), 0)
    for k in range(CAPS):
        rows = pl.ds(cap_at[k], B)
        pos_b[rows, :] = jnp.broadcast_to(columns[:, k:k + 1], (B, 128))
        bias_b[rows, :] = jnp.where(slot < counts[k, 0].astype(F32), 0.0, LOW)
    rows_used = cap_at[CAPS]
    tail = pl.ds(rows_used, RC)
    bias_b[tail, :] = jnp.full((RC, 128), LOW, F32)
    pos_b[tail, :] = jnp.full((RC, 128), -ABSENT, F32)
    cmax[...] = jnp.full(cmax.shape, 4.0 * LOW, F32)
    cmatch[...] = jnp.zeros(cmatch.shape, F32)
    csum[...] = jnp.zeros(csum.shape, F32)

    def tiles(count):
        @pl.loop(0, lax.div(rows_used + (RC - 1), RC))
        def _(i):
            rows = pl.ds(pl.multiple_of(i * RC, RC), RC)
            a = cap_v[rows, :]
            for n in range(count):
                s = lax.dot_general(
                    a, img_v[n * NC:(n + 1) * NC, :], (((1,), (1,)), ((), ())),
                    preferred_element_type=F32,
                )
                q = s * LOG2E
                highest, found = None, None
                for half in range(2):
                    span = pl.ds(n * NC + half * 128, 128)
                    qh = q[:, half * 128:(half + 1) * 128]
                    t = (qh + bias_b[rows, :]) + col_bias[0:1, span]
                    t_v[rows, span] = t
                    number = iota((1, 128), 1) + float(n * NC + half * 128)
                    w = jnp.where(pos_b[rows, :] == number, qh, 0.0)
                    highest = t if half == 0 else jnp.maximum(highest, t)
                    found = w if half == 0 else found + w
                    cmax[:, span] = jnp.maximum(
                        cmax[:, span], jnp.max(t.reshape(-1, 8, 128), axis=0)
                    )
                    cmatch[:, span] += jnp.sum(w.reshape(-1, 8, 128), axis=0)
                if n == 0:
                    rmax[rows, :] = highest
                    rmatch[rows, :] = found
                else:
                    rmax[rows, :] = jnp.maximum(rmax[rows, :], highest)
                    rmatch[rows, :] += found
            rmax[rows, :] = jnp.broadcast_to(
                jnp.max(rmax[rows, :], axis=1, keepdims=True), (RC, 128)
            )

        top = jnp.max(cmax[...], axis=0, keepdims=True)
        cmax[...] = jnp.broadcast_to(top, cmax.shape)

        def piece(r, totals):
            rows = pl.ds(pl.multiple_of(r * PIECE, PIECE), PIECE)
            peak = rmax[rows, :]
            acc = jnp.zeros((PIECE, 128), F32)
            out = []
            for n in range(2 * count):
                t = t_v[rows, n * 128:(n + 1) * 128]
                acc = acc + jnp.exp2(t - peak)
                f = jnp.exp2(t.reshape(-1, 8, 128) - cmax[:, n * 128:(n + 1) * 128][None])
                out.append(totals[n] + jnp.sum(f, axis=0))
            rsum[rows, :] = acc
            return tuple(out)

        totals = lax.fori_loop(
            0, lax.div(rows_used + (PIECE - 1), PIECE), piece,
            tuple(jnp.zeros((8, 128), F32) for _ in range(2 * count)),
        )
        for n in range(2 * count):
            csum[:, n * 128:(n + 1) * 128] = totals[n]

    used = jnp.maximum(lax.div(img_at[IMGS] + (NC - 1), NC), 1)
    for below, count in zip((0, *COUNTS), COUNTS):
        pl.when((used > below) & (used <= count))(lambda count=count: tiles(count))

    lanes = lax.broadcasted_iota(jnp.int32, (128, 128), 1)

    @pl.loop(0, lax.div(rows_used + (SPAN - 1), SPAN))
    def _(i):
        for j in range(SPAN // 128):
            rows = pl.ds(pl.multiple_of(i * SPAN + j * 128, 128), 128)
            total = jnp.sum(rsum[rows, :], axis=1, keepdims=True)
            match = jnp.sum(rmatch[rows, :], axis=1, keepdims=True)
            packed = jnp.where(lanes == 0, rmax[rows, :] + jnp.log2(total), match)
            row_lines[:, rows] = jnp.transpose(packed)[0:8, :]

    line = lax.broadcasted_iota(jnp.int32, (8, C), 0)
    total = jnp.sum(csum[...], axis=0, keepdims=True)
    match = jnp.sum(cmatch[...], axis=0, keepdims=True)
    lines_v[:, :C] = jnp.where(line == 0, cmax[0:1, :] + jnp.log2(total), match)
    p = place()
    for k in range(CAPS):
        cut = cut_at(row_lines, cap_at[k])
        if k:
            put(out, flat(cap_place(p, k)), cut)
        else:
            put(own_row, 0, cut)
    for m in range(IMGS):
        put(out, flat(img_place(p, m)), cut_at(lines_v, img_at[m]))


def cut_at(lines, start):
    whole = lax.shift_left(lax.shift_right_logical(start, 7), 7)
    slab = lines[:, pl.ds(pl.multiple_of(whole, 128), 384)]
    return pltpu.roll(slab, lax.rem(384 - (start - whole), 384), 1)


def put(out, at, lines):
    for i in range(2):
        out[at, 0:1, i * B:(i + 1) * B] = lines[i:i + 1, :B]


def joined(parts, ranks):
    sums, matches = parts[:, :B], parts[:, B:]
    peak = jnp.max(sums, axis=0, keepdims=True)
    total = jnp.sum(jnp.exp2(sums - peak), axis=0, keepdims=True)
    match = jnp.sum(matches, axis=0, keepdims=True)
    packed = jnp.broadcast_to(LN2 * (peak - match + jnp.log2(total)), (8, B))
    packed = jnp.concatenate([packed, jnp.zeros((8, 256 - B), F32)], axis=1)
    column = jnp.transpose(packed)[:B, 0:1]
    return jnp.sum(jnp.where(iota((B, B), 0) == ranks, column, 0.0), axis=0, keepdims=True)


def loss_kernel(
    parts, own_row, row_ranks, col_ranks, real, caption_loss, image_loss, total, rows, cols
):
    p = place()
    rows[0:1, :] = own_row[0, :, :]
    for k in range(1, CAPS):
        rows[k:k + 1, :] = parts[flat(cap_place(p, k)), :, :]
    for m in range(IMGS):
        cols[m:m + 1, :] = parts[flat(img_place(p, m)), :, :]
    caption = joined(rows[...], row_ranks[0:1, :])
    image = joined(cols[...], col_ranks[...])
    caption_loss[...] = caption
    image_loss[...] = image
    both = jnp.sum(caption, axis=1, keepdims=True) + jnp.sum(image, axis=1, keepdims=True)
    share = both / (2.0 * real[0:1, 0:1])
    total[...] = jnp.broadcast_to(share, (128, 8)).reshape(128, 1, 8)


def small(mib, flops):
    return dict(
        compiler_params=pltpu.CompilerParams(vmem_limit_bytes=mib * 1024 * 1024),
        cost_estimate=pl.CostEstimate(flops=flops, bytes_accessed=10**6, transcendentals=0),
    )


def step(captions, images, positives, valid):
    shape = jax.ShapeDtypeStruct
    pair = shape((2 * B, E), BF16)
    word = (positives + valid * (1 << OK_BIT))[None]
    others = [send(value, other_core) for value in (captions, images, word)]
    own = jnp.where(lax.axis_index("c") == 0, captions, images)
    carried, words, image_ranks = pl.pallas_call(
        pair_kernel,
        out_shape=[pair, shape((8, 2, B), jnp.int32), shape((1, B), F32)],
        in_specs=[VMEM] * 5,
        out_specs=[VMEM] * 3,
        **small(8, 10**8),
    )(own, others[0], others[1], word, others[2])
    near = send(carried, partner)
    a1, a3 = (send(carried, along(s)) for s in (1, 3))
    b1, b3 = (send(near, along(s)) for s in (1, 3))
    c1, c3 = send(a1, along(1)), send(b3, along(3))
    met = dict(own=carried, y=near, a1=a1, a3=a3, b1=b1, b3=b3, c1=c1, c3=c3)
    swapped = [send(v, other_core) for v in met.values()]
    carried = list(met.values())
    part = lax.all_to_all(words, ("x", "h"), 0, 0, tiled=True)
    part = pl.pallas_call(
        spread_kernel, out_shape=shape((8, 16, B), jnp.int32), in_specs=[VMEM],
        out_specs=VMEM, **small(2, 10**8),
    )(part)
    table = lax.all_to_all(part, ("z", "l"), 0, 0, tiled=True)
    ranks, columns, counts, real = pl.pallas_call(
        lookup_kernel,
        out_shape=[
            shape((CAPS, B), F32), shape((B, 128), F32),
            shape((CAPS + IMGS, 128), jnp.int32), shape((8, 128), F32),
        ],
        in_specs=[VMEM],
        out_specs=[VMEM] * 4,
        scratch_shapes=[pltpu.VMEM((CAPS, B), F32), pltpu.VMEM((128, B), jnp.int32)],
        **small(4, 3 * 10**9),
    )(table)
    buffers = []
    for part, (first, last) in enumerate(PARTS):
        buffers = pl.pallas_call(
            functools.partial(compact_kernel, part),
            out_shape=[shape((CAP_ROWS, E), BF16), shape((IMG_ROWS, E), BF16)],
            in_specs=[SMEM] + [VMEM] * (1 + len(buffers) + 2 * (last - first)),
            out_specs=[VMEM] * 2,
            input_output_aliases={2: 0, 3: 1} if part else {},
            **small(10, 10**9),
        )(counts, ranks, *buffers, *carried[first:last], *swapped[first:last])
    cap_v, img_v = buffers
    out, own_row = pl.pallas_call(
        score_kernel,
        out_shape=[shape((n, 1, 2 * B), F32) for n in (128, 1)],
        in_specs=[SMEM] + [VMEM] * 3,
        out_specs=[VMEM] * 2,
        scratch_shapes=[
            pltpu.VMEM((R, C), F32),
            *[pltpu.VMEM((R + RC, 128), F32)] * 5,
            pltpu.VMEM((8, C + 384), F32),
            *[pltpu.VMEM((8, C), F32)] * 3,
            pltpu.VMEM((8, C + 384), F32),
            pltpu.VMEM((8, R + 384), F32),
        ],
        compiler_params=pltpu.CompilerParams(vmem_limit_bytes=31 * 1024 * 1024),
        cost_estimate=pl.CostEstimate(
            flops=R * C * E, bytes_accessed=2 * (R + C) * E, transcendentals=R * C
        ),
    )(counts, columns, cap_v, img_v)
    parts = lax.all_to_all(out, AXES, 0, 0, tiled=True)
    caption_loss, image_loss, total = pl.pallas_call(
        loss_kernel,
        out_shape=[shape((1, B), F32), shape((1, B), F32), shape((128, 1, 8), F32)],
        in_specs=[VMEM] * 5,
        out_specs=[VMEM] * 3,
        scratch_shapes=[pltpu.VMEM((CAPS, 2 * B), F32), pltpu.VMEM((IMGS, 2 * B), F32)],
        **small(4, 10**8),
    )(parts, own_row, ranks, image_ranks, real)
    totals = lax.all_to_all(total, AXES, 0, 0, tiled=True)
    return caption_loss.reshape(B), image_loss.reshape(B), jnp.sum(totals[:, 0, 0])


def solution(mesh):
    torus = Mesh(mesh.devices.reshape(*SIZES.values()), AXES)
    return jax.shard_map(
        step,
        mesh=torus,
        in_specs=(P(AXES, None), P(AXES, None), P(AXES), P(AXES)),
        out_specs=(P(AXES), P(AXES), P()),
        check_vma=False,
    )
```

```python
import functools
import itertools

import jax
import jax.numpy as jnp
from jax import lax
from jax.experimental import pallas as pl
from jax.experimental.pallas import tpu as pltpu
from jax.sharding import Mesh
from jax.sharding import PartitionSpec as P


SIZES = {"x": 4, "h": 2, "z": 4, "c": 2, "l": 2}
AXES = tuple(SIZES)
LOG2E = 1.4426950408889634
LN2 = 0.6931471805599453
LOW = -1.0e30

B = 192
E = 768
MET = ((0, 0), (0, 1), (3, 0), (1, 0), (3, 1), (1, 1), (2, 0), (2, 1))
PARTS = ((0, 4), (4, 7))
LATE = PARTS[-1][1]
CAPS = len(MET)
IMGS = 2 * len(MET)
C = IMGS * B
RC = 448
R = -(-CAPS * B // RC) * RC
CAP_ROWS = CAPS * B + RC
NC = 256
COUNTS = (2, 4, 5, 6, 7, 8, 10, 12)
TAIL = 2 * NC
IMG_ROWS = C + TAIL
PIECE = 32
SPAN = 7 * 128
GRAIN = 16
OK_BIT = 15
ABSENT = 9999.0

F32 = jnp.float32
BF16 = jnp.bfloat16
VMEM = pl.BlockSpec(memory_space=pltpu.VMEM)
SMEM = pl.BlockSpec(memory_space=pltpu.SMEM)


def send(value, to):
    pairs = []
    for at in itertools.product(*map(range, SIZES.values())):
        p = dict(zip(AXES, at))
        pairs.append((flat(p), flat({**p, **to(p)})))
    return lax.ppermute(value, AXES, pairs)


def other_core(p):
    return {"c": 1 - p["c"]}


def partner(p):
    return {"l": 1 - p["l"], "h": p["h"] ^ p["c"]}


def along(step):
    def to(p):
        axis = "x" if p["c"] else "z"
        return {axis: (p[axis] + step) % 4}

    return to


def place():
    return {a: lax.axis_index(a) for a in AXES}


def flat(p):
    at = 0
    for a in AXES:
        at = at * SIZES[a] + p[a]
    return at


def moved(p, off):
    q = dict(p)
    for a, d in off.items():
        q[a] = lax.rem(p[a] + d, SIZES[a])
    return q


def cap_place(p, k):
    step, y = MET[k]
    return moved(p, {"z": step, "l": y})


def img_place(p, m):
    step, y = MET[m // 2]
    return {**moved(p, {"x": step, "h": y, "l": y}), "c": m % 2}


def iota(shape, dim):
    return lax.broadcasted_iota(jnp.int32, shape, dim).astype(F32)


def dot(a, b):
    return jnp.dot(a, b, preferred_element_type=F32)


def earlier():
    return jnp.where(iota((B, B), 0) < iota((B, B), 1), 1.0, 0.0).astype(BF16)


def grains(n):
    return lax.shift_left(lax.shift_right_logical(n + (GRAIN - 1), 4), 4)


def pair_kernel(own, cap_other, img_other, word, word_other, carried, words, ranks):
    first = lax.axis_index("c") == 0
    ok = lax.shift_right_logical(
        jnp.concatenate([word[...], word_other[...]], axis=0), OK_BIT
    )
    marks = jnp.broadcast_to(ok[:, None], (2, 8, B)).reshape(16, B).astype(F32).astype(BF16)
    order = dot(marks, earlier())
    found = jnp.where(ok > 0, jnp.concatenate([order[0:1], order[8:9]], axis=0), ABSENT)
    ranks[...] = found[0:1, :]
    both = jnp.where(
        first == (lax.broadcasted_iota(jnp.int32, (2, B), 0) == 0), word[...], word_other[...]
    )
    words[...] = jnp.broadcast_to(both[None], (8, 2, B))
    packed = []
    for i, block in enumerate((own, img_other)):
        pick = jnp.where(iota((B, B), 0) == found[i:i + 1, :], 1.0, 0.0).astype(BF16)
        packed.append(dot(pick, block[...]).astype(BF16))
    carried[0:B, :] = jnp.where(first, own[...], packed[1])
    carried[B:2 * B, :] = jnp.where(first, cap_other[...], packed[0])


def spread_kernel(part, words):
    words[...] = jnp.broadcast_to(part[...].reshape(1, 16, B), (8, 16, B))


def table_row(p):
    return ((p["z"] * 2 + p["l"]) * 8 + p["x"] * 2 + p["h"]) * 2 + p["c"]


def lookup_kernel(table, ranks, columns, counts, real, pos, words_v):
    p = place()
    words = table[...].reshape(128, B)
    words_v[...] = words
    ok = (lax.shift_right_logical(words, OK_BIT) & 1).astype(F32)
    rank = dot(ok.astype(BF16), earlier())
    real[...] = jnp.full((8, 128), jnp.sum(ok), F32)
    known = jnp.transpose(jnp.where(ok > 0, rank + 1.0, 0.0)).astype(BF16)
    for k in range(CAPS):
        row = words_v[pl.ds(table_row(cap_place(p, k)), 1), :]
        pos[k:k + 1, :] = (row & ((1 << OK_BIT) - 1)).astype(F32)
    at = pos[...]
    hi = jnp.floor((at + 0.5) * (1.0 / B))
    lo = at - hi * B
    line = lax.broadcasted_iota(jnp.int32, (128, B), 0)
    bits = lambda low, mask: lax.shift_right_logical(line, low) & mask
    block = (bits(1, 7) * 16 + bits(5, 3) * 4 + bits(0, 1) * 2 + bits(4, 1)).astype(F32)
    inner = iota((B, B), 0)
    for k in range(CAPS):
        pick = jnp.where(block == hi[k:k + 1, :], 1.0, 0.0).astype(BF16)
        column = dot(known, pick)
        pos[k:k + 1, :] = jnp.sum(
            jnp.where(inner == lo[k:k + 1, :], column, 0.0), axis=0, keepdims=True
        )
    value = pos[...]
    live = value > 0.0
    marks = jnp.where(live, 1.0, 0.0)
    order = dot(marks.astype(BF16), earlier())
    ranks[...] = jnp.where(live, order, ABSENT)
    start = jnp.zeros((1, 1), F32)
    base = jnp.full((CAPS, B), -ABSENT, F32)
    counts[0:CAPS, :] = jnp.broadcast_to(
        jnp.sum(marks, axis=1, keepdims=True).astype(jnp.int32), (CAPS, 128)
    )
    for m in range(IMGS):
        number = flat(img_place(p, m))
        row = words_v[pl.ds(table_row(img_place(p, m)), 1), :]
        row = lax.shift_right_logical(row, OK_BIT) & 1
        count = jnp.sum(row.astype(F32), axis=1, keepdims=True)
        base = jnp.where(hi == number.astype(F32), start, base)
        start = start + jnp.floor((count + (GRAIN - 1.0)) * (1.0 / GRAIN)) * GRAIN
        counts[CAPS + m:CAPS + m + 1, :] = jnp.broadcast_to(count.astype(jnp.int32), (1, 128))
    targets = jnp.where(live, base + value - 1.0, -ABSENT)
    order = ranks[...]
    lane = iota((B, 128), 1)
    result = jnp.zeros((B, 128), F32)
    for k in range(CAPS):
        hit = inner == order[k:k + 1, :]
        target = jnp.sum(jnp.where(hit, targets[k:k + 1, :], 0.0), axis=1, keepdims=True)
        result = jnp.where(lane == float(k), target, result)
    columns[...] = result


def starts_of(counts, first, number):
    found, at = [], jnp.int32(0)
    for k in range(number):
        found.append(pl.multiple_of(at, GRAIN))
        at = at + grains(counts[first + k, 0])
    return found + [pl.multiple_of(at, GRAIN)]


def compact(counts, ranks, carried, kept, cap_out, img_out, first):
    core = lax.axis_index("c")
    slot = iota((B, B), 0)
    at = starts_of(counts, 0, CAPS)
    for k, (a, b) in enumerate(zip(carried, kept), first):
        block = jnp.where(core == 0, a[0:B, :], b[B:2 * B, :])
        pick = jnp.where(slot == ranks[k:k + 1, :], 1.0, 0.0).astype(BF16)
        cap_out[pl.ds(at[k], B), :] = dot(pick, block).astype(BF16)
    at = starts_of(counts, CAPS, IMGS)
    for k, (a, b) in enumerate(zip(carried, kept), first):
        for side in range(2):
            rows = pl.ds(side * B, B)
            img_out[pl.ds(at[2 * k + side], B), :] = jnp.where(core == 0, b[rows, :], a[rows, :])


def compact_kernel(part, counts, ranks, *refs):
    first, last = PARTS[part]
    refs = refs[2 if part else 0:]
    number = last - first
    cap_out, img_out = refs[2 * number:]
    if part == 0:
        cap_end = starts_of(counts, 0, CAPS)[-1]
        img_end = starts_of(counts, CAPS, IMGS)[-1]
        cap_out[pl.ds(cap_end, RC), :] = jnp.zeros((RC, E), BF16)
        img_out[pl.ds(img_end, TAIL), :] = jnp.zeros((TAIL, E), BF16)
    compact(counts, ranks, refs[:number], refs[number:2 * number], cap_out, img_out, first)


def score_kernel(
    counts, columns, ranks, cap_in, img_in, carried, swapped, out, own_row, cap_v, img_v,
    t_v, pos_b, bias_b, rmax, rmatch, rsum, col_bias, cmax, cmatch, csum, lines_v, row_lines,
):
    del cap_in, img_in
    compact(counts, ranks, [carried], [swapped], cap_v, img_v, LATE)
    img_at = starts_of(counts, CAPS, IMGS)
    col_bias[...] = jnp.full((8, C + 384), LOW, F32)
    column = iota((8, 384), 1)
    for m in range(IMGS):
        whole = lax.shift_left(lax.shift_right_logical(img_at[m], 7), 7)
        span = pl.ds(pl.multiple_of(whole, 128), 384)
        begin = (img_at[m] - whole).astype(F32)
        end = begin + counts[CAPS + m, 0].astype(F32)
        inside = (column >= begin) & (column < end)
        col_bias[:, span] = jnp.where(inside, 0.0, col_bias[:, span])
    cap_at = starts_of(counts, 0, CAPS)
    slot = iota((B, 128), 0)
    for k in range(CAPS):
        rows = pl.ds(cap_at[k], B)
        pos_b[rows, :] = jnp.broadcast_to(columns[:, k:k + 1], (B, 128))
        bias_b[rows, :] = jnp.where(slot < counts[k, 0].astype(F32), 0.0, LOW)
    rows_used = cap_at[CAPS]
    tail = pl.ds(rows_used, RC)
    bias_b[tail, :] = jnp.full((RC, 128), LOW, F32)
    pos_b[tail, :] = jnp.full((RC, 128), -ABSENT, F32)
    cmax[...] = jnp.full(cmax.shape, 4.0 * LOW, F32)
    cmatch[...] = jnp.zeros(cmatch.shape, F32)
    csum[...] = jnp.zeros(csum.shape, F32)

    def tiles(count):
        @pl.loop(0, lax.div(rows_used + (RC - 1), RC))
        def _(i):
            rows = pl.ds(pl.multiple_of(i * RC, RC), RC)
            a = cap_v[rows, :]
            for n in range(count):
                s = lax.dot_general(
                    a, img_v[n * NC:(n + 1) * NC, :], (((1,), (1,)), ((), ())),
                    preferred_element_type=F32,
                )
                q = s * LOG2E
                highest, found = None, None
                for half in range(2):
                    span = pl.ds(n * NC + half * 128, 128)
                    qh = q[:, half * 128:(half + 1) * 128]
                    t = (qh + bias_b[rows, :]) + col_bias[0:1, span]
                    t_v[rows, span] = t
                    number = iota((1, 128), 1) + float(n * NC + half * 128)
                    w = jnp.where(pos_b[rows, :] == number, qh, 0.0)
                    highest = t if half == 0 else jnp.maximum(highest, t)
                    found = w if half == 0 else found + w
                    cmax[:, span] = jnp.maximum(
                        cmax[:, span], jnp.max(t.reshape(-1, 8, 128), axis=0)
                    )
                    cmatch[:, span] += jnp.sum(w.reshape(-1, 8, 128), axis=0)
                if n == 0:
                    rmax[rows, :] = highest
                    rmatch[rows, :] = found
                else:
                    rmax[rows, :] = jnp.maximum(rmax[rows, :], highest)
                    rmatch[rows, :] += found
            rmax[rows, :] = jnp.broadcast_to(
                jnp.max(rmax[rows, :], axis=1, keepdims=True), (RC, 128)
            )

        top = jnp.max(cmax[...], axis=0, keepdims=True)
        cmax[...] = jnp.broadcast_to(top, cmax.shape)

        def piece(r, totals):
            rows = pl.ds(pl.multiple_of(r * PIECE, PIECE), PIECE)
            peak = rmax[rows, :]
            acc = jnp.zeros((PIECE, 128), F32)
            out = []
            for n in range(2 * count):
                t = t_v[rows, n * 128:(n + 1) * 128]
                acc = acc + jnp.exp2(t - peak)
                f = jnp.exp2(t.reshape(-1, 8, 128) - cmax[:, n * 128:(n + 1) * 128][None])
                out.append(totals[n] + jnp.sum(f, axis=0))
            rsum[rows, :] = acc
            return tuple(out)

        totals = lax.fori_loop(
            0, lax.div(rows_used + (PIECE - 1), PIECE), piece,
            tuple(jnp.zeros((8, 128), F32) for _ in range(2 * count)),
        )
        for n in range(2 * count):
            csum[:, n * 128:(n + 1) * 128] = totals[n]

    used = jnp.maximum(lax.div(img_at[IMGS] + (NC - 1), NC), 1)
    for below, count in zip((0, *COUNTS), COUNTS):
        pl.when((used > below) & (used <= count))(lambda count=count: tiles(count))

    lanes = lax.broadcasted_iota(jnp.int32, (128, 128), 1)

    @pl.loop(0, lax.div(rows_used + (SPAN - 1), SPAN))
    def _(i):
        for j in range(SPAN // 128):
            rows = pl.ds(pl.multiple_of(i * SPAN + j * 128, 128), 128)
            total = jnp.sum(rsum[rows, :], axis=1, keepdims=True)
            match = jnp.sum(rmatch[rows, :], axis=1, keepdims=True)
            packed = jnp.where(lanes == 0, rmax[rows, :] + jnp.log2(total), match)
            row_lines[:, rows] = jnp.transpose(packed)[0:8, :]

    line = lax.broadcasted_iota(jnp.int32, (8, C), 0)
    total = jnp.sum(csum[...], axis=0, keepdims=True)
    match = jnp.sum(cmatch[...], axis=0, keepdims=True)
    lines_v[:, :C] = jnp.where(line == 0, cmax[0:1, :] + jnp.log2(total), match)
    p = place()
    for k in range(CAPS):
        cut = cut_at(row_lines, cap_at[k])
        if k:
            put(out, flat(cap_place(p, k)), cut)
        else:
            put(own_row, 0, cut)
    for m in range(IMGS):
        put(out, flat(img_place(p, m)), cut_at(lines_v, img_at[m]))


def cut_at(lines, start):
    whole = lax.shift_left(lax.shift_right_logical(start, 7), 7)
    slab = lines[:, pl.ds(pl.multiple_of(whole, 128), 384)]
    return pltpu.roll(slab, lax.rem(384 - (start - whole), 384), 1)


def put(out, at, lines):
    for i in range(2):
        out[at, 0:1, i * B:(i + 1) * B] = lines[i:i + 1, :B]


def joined(parts, ranks):
    sums, matches = parts[:, :B], parts[:, B:]
    peak = jnp.max(sums, axis=0, keepdims=True)
    total = jnp.sum(jnp.exp2(sums - peak), axis=0, keepdims=True)
    match = jnp.sum(matches, axis=0, keepdims=True)
    packed = jnp.broadcast_to(LN2 * (peak - match + jnp.log2(total)), (8, B))
    packed = jnp.concatenate([packed, jnp.zeros((8, 256 - B), F32)], axis=1)
    column = jnp.transpose(packed)[:B, 0:1]
    return jnp.sum(jnp.where(iota((B, B), 0) == ranks, column, 0.0), axis=0, keepdims=True)


def loss_kernel(
    parts, own_row, row_ranks, col_ranks, real, caption_loss, image_loss, total, rows, cols
):
    p = place()
    rows[0:1, :] = own_row[0, :, :]
    for k in range(1, CAPS):
        rows[k:k + 1, :] = parts[flat(cap_place(p, k)), :, :]
    for m in range(IMGS):
        cols[m:m + 1, :] = parts[flat(img_place(p, m)), :, :]
    caption = joined(rows[...], row_ranks[0:1, :])
    image = joined(cols[...], col_ranks[...])
    caption_loss[...] = caption
    image_loss[...] = image
    both = jnp.sum(caption, axis=1, keepdims=True) + jnp.sum(image, axis=1, keepdims=True)
    share = both / (2.0 * real[0:1, 0:1])
    total[...] = jnp.broadcast_to(share, (128, 8)).reshape(128, 1, 8)


def small(mib, flops):
    return dict(
        compiler_params=pltpu.CompilerParams(vmem_limit_bytes=mib * 1024 * 1024),
        cost_estimate=pl.CostEstimate(flops=flops, bytes_accessed=10**6, transcendentals=0),
    )


def step(captions, images, positives, valid):
    shape = jax.ShapeDtypeStruct
    pair = shape((2 * B, E), BF16)
    word = (positives + valid * (1 << OK_BIT))[None]
    others = [send(value, other_core) for value in (captions, images, word)]
    own = jnp.where(lax.axis_index("c") == 0, captions, images)
    carried, words, image_ranks = pl.pallas_call(
        pair_kernel,
        out_shape=[pair, shape((8, 2, B), jnp.int32), shape((1, B), F32)],
        in_specs=[VMEM] * 5,
        out_specs=[VMEM] * 3,
        **small(8, 10**8),
    )(own, others[0], others[1], word, others[2])
    near = send(carried, partner)
    a1, a3 = (send(carried, along(s)) for s in (1, 3))
    b1, b3 = (send(near, along(s)) for s in (1, 3))
    c1, c3 = send(a1, along(1)), send(b3, along(3))
    met = dict(own=carried, y=near, a1=a1, a3=a3, b1=b1, b3=b3, c1=c1, c3=c3)
    swapped = [send(v, other_core) for v in met.values()]
    carried = list(met.values())
    part = lax.all_to_all(words, ("x", "h"), 0, 0, tiled=True)
    part = pl.pallas_call(
        spread_kernel, out_shape=shape((8, 16, B), jnp.int32), in_specs=[VMEM],
        out_specs=VMEM, **small(2, 10**8),
    )(part)
    table = lax.all_to_all(part, ("z", "l"), 0, 0, tiled=True)
    ranks, columns, counts, real = pl.pallas_call(
        lookup_kernel,
        out_shape=[
            shape((CAPS, B), F32), shape((B, 128), F32),
            shape((CAPS + IMGS, 128), jnp.int32), shape((8, 128), F32),
        ],
        in_specs=[VMEM],
        out_specs=[VMEM] * 4,
        scratch_shapes=[pltpu.VMEM((CAPS, B), F32), pltpu.VMEM((128, B), jnp.int32)],
        **small(4, 3 * 10**9),
    )(table)
    buffers = []
    for part, (first, last) in enumerate(PARTS):
        buffers = pl.pallas_call(
            functools.partial(compact_kernel, part),
            out_shape=[shape((CAP_ROWS, E), BF16), shape((IMG_ROWS, E), BF16)],
            in_specs=[SMEM] + [VMEM] * (1 + len(buffers) + 2 * (last - first)),
            out_specs=[VMEM] * 2,
            input_output_aliases={2: 0, 3: 1} if part else {},
            **small(10, 10**9),
        )(counts, ranks, *buffers, *carried[first:last], *swapped[first:last])
    out, own_row, _, _ = pl.pallas_call(
        score_kernel,
        out_shape=[
            *(shape((n, 1, 2 * B), F32) for n in (128, 1)),
            shape((CAP_ROWS, E), BF16), shape((IMG_ROWS, E), BF16),
        ],
        in_specs=[SMEM] + [VMEM] * 6,
        out_specs=[VMEM] * 4,
        input_output_aliases={3: 2, 4: 3},
        scratch_shapes=[
            pltpu.VMEM((R, C), F32),
            *[pltpu.VMEM((R + RC, 128), F32)] * 5,
            pltpu.VMEM((8, C + 384), F32),
            *[pltpu.VMEM((8, C), F32)] * 3,
            pltpu.VMEM((8, C + 384), F32),
            pltpu.VMEM((8, R + 384), F32),
        ],
        compiler_params=pltpu.CompilerParams(vmem_limit_bytes=31 * 1024 * 1024),
        cost_estimate=pl.CostEstimate(
            flops=R * C * E, bytes_accessed=2 * (R + C) * E, transcendentals=R * C
        ),
    )(counts, columns, ranks, *buffers, carried[LATE], swapped[LATE])
    parts = lax.all_to_all(out, AXES, 0, 0, tiled=True)
    caption_loss, image_loss, total = pl.pallas_call(
        loss_kernel,
        out_shape=[shape((1, B), F32), shape((1, B), F32), shape((128, 1, 8), F32)],
        in_specs=[VMEM] * 5,
        out_specs=[VMEM] * 3,
        scratch_shapes=[pltpu.VMEM((CAPS, 2 * B), F32), pltpu.VMEM((IMGS, 2 * B), F32)],
        **small(4, 10**8),
    )(parts, own_row, ranks, image_ranks, real)
    totals = lax.all_to_all(total, AXES, 0, 0, tiled=True)
    return caption_loss.reshape(B), image_loss.reshape(B), jnp.sum(totals[:, 0, 0])


def solution(mesh):
    torus = Mesh(mesh.devices.reshape(*SIZES.values()), AXES)
    return jax.shard_map(
        step,
        mesh=torus,
        in_specs=(P(AXES, None), P(AXES, None), P(AXES), P(AXES)),
        out_specs=(P(AXES), P(AXES), P()),
        check_vma=False,
    )
```

```python
import functools
import itertools

import jax
import jax.numpy as jnp
from jax import lax
from jax.experimental import pallas as pl
from jax.experimental.pallas import tpu as pltpu
from jax.sharding import Mesh
from jax.sharding import PartitionSpec as P


SIZES = {"x": 4, "h": 2, "z": 4, "c": 2, "l": 2}
AXES = tuple(SIZES)
LOG2E = 1.4426950408889634
LN2 = 0.6931471805599453
LOW = -1.0e30

B = 192
E = 768
MET = ((0, 0), (0, 1), (3, 0), (1, 0), (3, 1), (1, 1), (2, 0), (2, 1))
PARTS = ((0, 4), (4, 6))
LATE = PARTS[-1][1]
CAPS = len(MET)
IMGS = 2 * len(MET)
C = IMGS * B
RC = 448
R = -(-CAPS * B // RC) * RC
CAP_ROWS = CAPS * B + RC
NC = 256
COUNTS = (2, 4, 5, 6, 7, 8, 10, 12)
TAIL = 2 * NC
IMG_ROWS = C + TAIL
PIECE = 64
SPAN = 7 * 128
GRAIN = 16
OK_BIT = 15
ABSENT = 9999.0

F32 = jnp.float32
BF16 = jnp.bfloat16
VMEM = pl.BlockSpec(memory_space=pltpu.VMEM)
SMEM = pl.BlockSpec(memory_space=pltpu.SMEM)


def send(value, to):
    pairs = []
    for at in itertools.product(*map(range, SIZES.values())):
        p = dict(zip(AXES, at))
        pairs.append((flat(p), flat({**p, **to(p)})))
    return lax.ppermute(value, AXES, pairs)


def other_core(p):
    return {"c": 1 - p["c"]}


def partner(p):
    return {"l": 1 - p["l"], "h": p["h"] ^ p["c"]}


def along(step):
    def to(p):
        axis = "x" if p["c"] else "z"
        return {axis: (p[axis] + step) % 4}

    return to


def place():
    return {a: lax.axis_index(a) for a in AXES}


def flat(p):
    at = 0
    for a in AXES:
        at = at * SIZES[a] + p[a]
    return at


def moved(p, off):
    q = dict(p)
    for a, d in off.items():
        q[a] = lax.rem(p[a] + d, SIZES[a])
    return q


def cap_place(p, k):
    step, y = MET[k]
    return moved(p, {"z": step, "l": y})


def img_place(p, m):
    step, y = MET[m // 2]
    return {**moved(p, {"x": step, "h": y, "l": y}), "c": m % 2}


def iota(shape, dim):
    return lax.broadcasted_iota(jnp.int32, shape, dim).astype(F32)


def dot(a, b):
    return jnp.dot(a, b, preferred_element_type=F32)


def earlier():
    return jnp.where(iota((B, B), 0) < iota((B, B), 1), 1.0, 0.0).astype(BF16)


def grains(n):
    return lax.shift_left(lax.shift_right_logical(n + (GRAIN - 1), 4), 4)


def pair_kernel(own, cap_other, img_other, word, word_other, carried, words, ranks):
    first = lax.axis_index("c") == 0
    ok = lax.shift_right_logical(
        jnp.concatenate([word[...], word_other[...]], axis=0), OK_BIT
    )
    marks = jnp.broadcast_to(ok[:, None], (2, 8, B)).reshape(16, B).astype(F32).astype(BF16)
    order = dot(marks, earlier())
    found = jnp.where(ok > 0, jnp.concatenate([order[0:1], order[8:9]], axis=0), ABSENT)
    ranks[...] = found[0:1, :]
    both = jnp.where(
        first == (lax.broadcasted_iota(jnp.int32, (2, B), 0) == 0), word[...], word_other[...]
    )
    words[...] = jnp.broadcast_to(both[None], (8, 2, B))
    packed = []
    for i, block in enumerate((own, img_other)):
        pick = jnp.where(iota((B, B), 0) == found[i:i + 1, :], 1.0, 0.0).astype(BF16)
        packed.append(dot(pick, block[...]).astype(BF16))
    carried[0:B, :] = jnp.where(first, own[...], packed[1])
    carried[B:2 * B, :] = jnp.where(first, cap_other[...], packed[0])


def spread_kernel(part, words):
    words[...] = jnp.broadcast_to(part[...].reshape(1, 16, B), (8, 16, B))


def table_row(p):
    return ((p["z"] * 2 + p["l"]) * 8 + p["x"] * 2 + p["h"]) * 2 + p["c"]


def lookup_kernel(table, ranks, columns, counts, real, pos, words_v):
    p = place()
    words = table[...].reshape(128, B)
    words_v[...] = words
    ok = (lax.shift_right_logical(words, OK_BIT) & 1).astype(F32)
    rank = dot(ok.astype(BF16), earlier())
    real[...] = jnp.full((8, 128), jnp.sum(ok), F32)
    known = jnp.transpose(jnp.where(ok > 0, rank + 1.0, 0.0)).astype(BF16)
    for k in range(CAPS):
        row = words_v[pl.ds(table_row(cap_place(p, k)), 1), :]
        pos[k:k + 1, :] = (row & ((1 << OK_BIT) - 1)).astype(F32)
    at = pos[...]
    hi = jnp.floor((at + 0.5) * (1.0 / B))
    lo = at - hi * B
    line = lax.broadcasted_iota(jnp.int32, (128, B), 0)
    bits = lambda low, mask: lax.shift_right_logical(line, low) & mask
    block = (bits(1, 7) * 16 + bits(5, 3) * 4 + bits(0, 1) * 2 + bits(4, 1)).astype(F32)
    inner = iota((B, B), 0)
    for k in range(CAPS):
        pick = jnp.where(block == hi[k:k + 1, :], 1.0, 0.0).astype(BF16)
        column = dot(known, pick)
        pos[k:k + 1, :] = jnp.sum(
            jnp.where(inner == lo[k:k + 1, :], column, 0.0), axis=0, keepdims=True
        )
    value = pos[...]
    live = value > 0.0
    marks = jnp.where(live, 1.0, 0.0)
    order = dot(marks.astype(BF16), earlier())
    ranks[...] = jnp.where(live, order, ABSENT)
    start = jnp.zeros((1, 1), F32)
    base = jnp.full((CAPS, B), -ABSENT, F32)
    counts[0:CAPS, :] = jnp.broadcast_to(
        jnp.sum(marks, axis=1, keepdims=True).astype(jnp.int32), (CAPS, 128)
    )
    for m in range(IMGS):
        number = flat(img_place(p, m))
        row = words_v[pl.ds(table_row(img_place(p, m)), 1), :]
        row = lax.shift_right_logical(row, OK_BIT) & 1
        count = jnp.sum(row.astype(F32), axis=1, keepdims=True)
        base = jnp.where(hi == number.astype(F32), start, base)
        start = start + jnp.floor((count + (GRAIN - 1.0)) * (1.0 / GRAIN)) * GRAIN
        counts[CAPS + m:CAPS + m + 1, :] = jnp.broadcast_to(count.astype(jnp.int32), (1, 128))
    targets = jnp.where(live, base + value - 1.0, -ABSENT)
    order = ranks[...]
    lane = iota((B, 128), 1)
    result = jnp.zeros((B, 128), F32)
    for k in range(CAPS):
        hit = inner == order[k:k + 1, :]
        target = jnp.sum(jnp.where(hit, targets[k:k + 1, :], 0.0), axis=1, keepdims=True)
        result = jnp.where(lane == float(k), target, result)
    columns[...] = result


def starts_of(counts, first, number):
    found, at = [], jnp.int32(0)
    for k in range(number):
        found.append(pl.multiple_of(at, GRAIN))
        at = at + grains(counts[first + k, 0])
    return found + [pl.multiple_of(at, GRAIN)]


def compact(counts, ranks, carried, kept, cap_out, img_out, first):
    core = lax.axis_index("c")
    slot = iota((B, B), 0)
    at = starts_of(counts, 0, CAPS)
    for k, (a, b) in enumerate(zip(carried, kept), first):
        block = jnp.where(core == 0, a[0:B, :], b[B:2 * B, :])
        pick = jnp.where(slot == ranks[k:k + 1, :], 1.0, 0.0).astype(BF16)
        cap_out[pl.ds(at[k], B), :] = dot(pick, block).astype(BF16)
    at = starts_of(counts, CAPS, IMGS)
    for k, (a, b) in enumerate(zip(carried, kept), first):
        for side in range(2):
            rows = pl.ds(side * B, B)
            img_out[pl.ds(at[2 * k + side], B), :] = jnp.where(core == 0, b[rows, :], a[rows, :])


def compact_kernel(part, counts, ranks, *refs):
    first, last = PARTS[part]
    refs = refs[2 if part else 0:]
    number = last - first
    cap_out, img_out = refs[2 * number:]
    if part == 0:
        cap_end = starts_of(counts, 0, CAPS)[-1]
        img_end = starts_of(counts, CAPS, IMGS)[-1]
        cap_out[pl.ds(cap_end, RC), :] = jnp.zeros((RC, E), BF16)
        img_out[pl.ds(img_end, TAIL), :] = jnp.zeros((TAIL, E), BF16)
    compact(counts, ranks, refs[:number], refs[number:2 * number], cap_out, img_out, first)


def score_kernel(
    counts, columns, ranks, cap_in, img_in, c1, c3, c1_other, c3_other,
    out, own_row, cap_v, img_v,
    t_v, pos_b, bias_b, rmax, rmatch, rsum, col_bias, cmax, cmatch, csum, lines_v, row_lines,
):
    del cap_in, img_in
    compact(counts, ranks, [c1, c3], [c1_other, c3_other], cap_v, img_v, LATE)
    img_at = starts_of(counts, CAPS, IMGS)
    col_bias[...] = jnp.full((8, C + 384), LOW, F32)
    column = iota((8, 384), 1)
    for m in range(IMGS):
        whole = lax.shift_left(lax.shift_right_logical(img_at[m], 7), 7)
        span = pl.ds(pl.multiple_of(whole, 128), 384)
        begin = (img_at[m] - whole).astype(F32)
        end = begin + counts[CAPS + m, 0].astype(F32)
        inside = (column >= begin) & (column < end)
        col_bias[:, span] = jnp.where(inside, 0.0, col_bias[:, span])
    cap_at = starts_of(counts, 0, CAPS)
    slot = iota((B, 128), 0)
    for k in range(CAPS):
        rows = pl.ds(cap_at[k], B)
        pos_b[rows, :] = jnp.broadcast_to(columns[:, k:k + 1], (B, 128))
        bias_b[rows, :] = jnp.where(slot < counts[k, 0].astype(F32), 0.0, LOW)
    rows_used = cap_at[CAPS]
    tail = pl.ds(rows_used, RC)
    bias_b[tail, :] = jnp.full((RC, 128), LOW, F32)
    pos_b[tail, :] = jnp.full((RC, 128), -ABSENT, F32)
    cmax[...] = jnp.full(cmax.shape, 4.0 * LOW, F32)
    cmatch[...] = jnp.zeros(cmatch.shape, F32)
    csum[...] = jnp.zeros(csum.shape, F32)

    def tiles(count):
        @pl.loop(0, lax.div(rows_used + (RC - 1), RC))
        def _(i):
            rows = pl.ds(pl.multiple_of(i * RC, RC), RC)
            a = cap_v[rows, :]
            for n in range(count):
                s = lax.dot_general(
                    a, img_v[n * NC:(n + 1) * NC, :], (((1,), (1,)), ((), ())),
                    preferred_element_type=F32,
                )
                q = s * LOG2E
                highest, found = None, None
                for half in range(2):
                    span = pl.ds(n * NC + half * 128, 128)
                    qh = q[:, half * 128:(half + 1) * 128]
                    t = (qh + bias_b[rows, :]) + col_bias[0:1, span]
                    t_v[rows, span] = t
                    number = iota((1, 128), 1) + float(n * NC + half * 128)
                    w = jnp.where(pos_b[rows, :] == number, qh, 0.0)
                    highest = t if half == 0 else jnp.maximum(highest, t)
                    found = w if half == 0 else found + w
                    cmax[:, span] = jnp.maximum(
                        cmax[:, span], jnp.max(t.reshape(-1, 8, 128), axis=0)
                    )
                    cmatch[:, span] += jnp.sum(w.reshape(-1, 8, 128), axis=0)
                if n == 0:
                    rmax[rows, :] = highest
                    rmatch[rows, :] = found
                else:
                    rmax[rows, :] = jnp.maximum(rmax[rows, :], highest)
                    rmatch[rows, :] += found
            rmax[rows, :] = jnp.broadcast_to(
                jnp.max(rmax[rows, :], axis=1, keepdims=True), (RC, 128)
            )

        top = jnp.max(cmax[...], axis=0, keepdims=True)
        cmax[...] = jnp.broadcast_to(top, cmax.shape)

        def piece(r, totals):
            rows = pl.ds(pl.multiple_of(r * PIECE, PIECE), PIECE)
            peak = rmax[rows, :]
            acc = jnp.zeros((PIECE, 128), F32)
            out = []
            for n in range(2 * count):
                t = t_v[rows, n * 128:(n + 1) * 128]
                acc = acc + jnp.exp2(t - peak)
                f = jnp.exp2(t.reshape(-1, 8, 128) - cmax[:, n * 128:(n + 1) * 128][None])
                out.append(totals[n] + jnp.sum(f, axis=0))
            rsum[rows, :] = acc
            return tuple(out)

        totals = lax.fori_loop(
            0, lax.div(rows_used + (PIECE - 1), PIECE), piece,
            tuple(jnp.zeros((8, 128), F32) for _ in range(2 * count)),
        )
        for n in range(2 * count):
            csum[:, n * 128:(n + 1) * 128] = totals[n]

    used = jnp.maximum(lax.div(img_at[IMGS] + (NC - 1), NC), 1)
    for below, count in zip((0, *COUNTS), COUNTS):
        pl.when((used > below) & (used <= count))(lambda count=count: tiles(count))

    lanes = lax.broadcasted_iota(jnp.int32, (128, 128), 1)

    @pl.loop(0, lax.div(rows_used + (SPAN - 1), SPAN))
    def _(i):
        for j in range(SPAN // 128):
            rows = pl.ds(pl.multiple_of(i * SPAN + j * 128, 128), 128)
            total = jnp.sum(rsum[rows, :], axis=1, keepdims=True)
            match = jnp.sum(rmatch[rows, :], axis=1, keepdims=True)
            packed = jnp.where(lanes == 0, rmax[rows, :] + jnp.log2(total), match)
            row_lines[:, rows] = jnp.transpose(packed)[0:8, :]

    line = lax.broadcasted_iota(jnp.int32, (8, C), 0)
    total = jnp.sum(csum[...], axis=0, keepdims=True)
    match = jnp.sum(cmatch[...], axis=0, keepdims=True)
    lines_v[:, :C] = jnp.where(line == 0, cmax[0:1, :] + jnp.log2(total), match)
    p = place()
    for k in range(CAPS):
        cut = cut_at(row_lines, cap_at[k])
        if k:
            put(out, flat(cap_place(p, k)), cut)
        else:
            put(own_row, 0, cut)
    for m in range(IMGS):
        put(out, flat(img_place(p, m)), cut_at(lines_v, img_at[m]))


def cut_at(lines, start):
    whole = lax.shift_left(lax.shift_right_logical(start, 7), 7)
    slab = lines[:, pl.ds(pl.multiple_of(whole, 128), 384)]
    return pltpu.roll(slab, lax.rem(384 - (start - whole), 384), 1)


def put(out, at, lines):
    for i in range(2):
        out[at, 0:1, i * B:(i + 1) * B] = lines[i:i + 1, :B]


def joined(parts, ranks):
    sums, matches = parts[:, :B], parts[:, B:]
    peak = jnp.max(sums, axis=0, keepdims=True)
    total = jnp.sum(jnp.exp2(sums - peak), axis=0, keepdims=True)
    match = jnp.sum(matches, axis=0, keepdims=True)
    packed = jnp.broadcast_to(LN2 * (peak - match + jnp.log2(total)), (8, B))
    packed = jnp.concatenate([packed, jnp.zeros((8, 256 - B), F32)], axis=1)
    column = jnp.transpose(packed)[:B, 0:1]
    return jnp.sum(jnp.where(iota((B, B), 0) == ranks, column, 0.0), axis=0, keepdims=True)


def loss_kernel(
    parts, own_row, row_ranks, col_ranks, real, caption_loss, image_loss, total, rows, cols
):
    p = place()
    rows[0:1, :] = own_row[0, :, :]
    for k in range(1, CAPS):
        rows[k:k + 1, :] = parts[flat(cap_place(p, k)), :, :]
    for m in range(IMGS):
        cols[m:m + 1, :] = parts[flat(img_place(p, m)), :, :]
    caption = joined(rows[...], row_ranks[0:1, :])
    image = joined(cols[...], col_ranks[...])
    caption_loss[...] = caption
    image_loss[...] = image
    both = jnp.sum(caption, axis=1, keepdims=True) + jnp.sum(image, axis=1, keepdims=True)
    share = both / (2.0 * real[0:1, 0:1])
    total[...] = jnp.broadcast_to(share, (128, 8)).reshape(128, 1, 8)


def sum_kernel(totals, loss):
    loss[...] = jnp.sum(totals[...].reshape(128, 8)[:, 0:1], axis=0, keepdims=True)


def small(mib, flops):
    return dict(
        compiler_params=pltpu.CompilerParams(vmem_limit_bytes=mib * 1024 * 1024),
        cost_estimate=pl.CostEstimate(flops=flops, bytes_accessed=10**6, transcendentals=0),
    )


def step(captions, images, positives, valid):
    shape = jax.ShapeDtypeStruct
    pair = shape((2 * B, E), BF16)
    word = (positives + valid * (1 << OK_BIT))[None]
    others = [send(value, other_core) for value in (captions, images, word)]
    own = jnp.where(lax.axis_index("c") == 0, captions, images)
    carried, words, image_ranks = pl.pallas_call(
        pair_kernel,
        out_shape=[pair, shape((8, 2, B), jnp.int32), shape((1, B), F32)],
        in_specs=[VMEM] * 5,
        out_specs=[VMEM] * 3,
        **small(8, 10**8),
    )(own, others[0], others[1], word, others[2])
    near = send(carried, partner)
    a1, a3 = (send(carried, along(s)) for s in (1, 3))
    b1, b3 = (send(near, along(s)) for s in (1, 3))
    c1, c3 = send(a1, along(1)), send(b3, along(3))
    met = dict(own=carried, y=near, a1=a1, a3=a3, b1=b1, b3=b3, c1=c1, c3=c3)
    swapped = [send(v, other_core) for v in met.values()]
    carried = list(met.values())
    part = lax.all_to_all(words, ("x", "h"), 0, 0, tiled=True)
    part = pl.pallas_call(
        spread_kernel, out_shape=shape((8, 16, B), jnp.int32), in_specs=[VMEM],
        out_specs=VMEM, **small(2, 10**8),
    )(part)
    table = lax.all_to_all(part, ("z", "l"), 0, 0, tiled=True)
    ranks, columns, counts, real = pl.pallas_call(
        lookup_kernel,
        out_shape=[
            shape((CAPS, B), F32), shape((B, 128), F32),
            shape((CAPS + IMGS, 128), jnp.int32), shape((8, 128), F32),
        ],
        in_specs=[VMEM],
        out_specs=[VMEM] * 4,
        scratch_shapes=[pltpu.VMEM((CAPS, B), F32), pltpu.VMEM((128, B), jnp.int32)],
        **small(4, 3 * 10**9),
    )(table)
    buffers = []
    for part, (first, last) in enumerate(PARTS):
        buffers = pl.pallas_call(
            functools.partial(compact_kernel, part),
            out_shape=[shape((CAP_ROWS, E), BF16), shape((IMG_ROWS, E), BF16)],
            in_specs=[SMEM] + [VMEM] * (1 + len(buffers) + 2 * (last - first)),
            out_specs=[VMEM] * 2,
            input_output_aliases={2: 0, 3: 1} if part else {},
            **small(10, 10**9),
        )(counts, ranks, *buffers, *carried[first:last], *swapped[first:last])
    out, own_row, _, _ = pl.pallas_call(
        score_kernel,
        out_shape=[
            *(shape((n, 1, 2 * B), F32) for n in (128, 1)),
            shape((CAP_ROWS, E), BF16), shape((IMG_ROWS, E), BF16),
        ],
        in_specs=[SMEM] + [VMEM] * 8,
        out_specs=[VMEM] * 4,
        input_output_aliases={3: 2, 4: 3},
        scratch_shapes=[
            pltpu.VMEM((R, C), F32),
            *[pltpu.VMEM((R + RC, 128), F32)] * 5,
            pltpu.VMEM((8, C + 384), F32),
            *[pltpu.VMEM((8, C), F32)] * 3,
            pltpu.VMEM((8, C + 384), F32),
            pltpu.VMEM((8, R + 384), F32),
        ],
        compiler_params=pltpu.CompilerParams(vmem_limit_bytes=31 * 1024 * 1024),
        cost_estimate=pl.CostEstimate(
            flops=R * C * E, bytes_accessed=2 * (R + C) * E, transcendentals=R * C
        ),
    )(counts, columns, ranks, *buffers, *carried[LATE:], *swapped[LATE:])
    parts = lax.all_to_all(out, AXES, 0, 0, tiled=True)
    caption_loss, image_loss, total = pl.pallas_call(
        loss_kernel,
        out_shape=[shape((1, B), F32), shape((1, B), F32), shape((128, 1, 8), F32)],
        in_specs=[VMEM] * 5,
        out_specs=[VMEM] * 3,
        scratch_shapes=[pltpu.VMEM((CAPS, 2 * B), F32), pltpu.VMEM((IMGS, 2 * B), F32)],
        **small(4, 10**8),
    )(parts, own_row, ranks, image_ranks, real)
    totals = lax.all_to_all(total, AXES, 0, 0, tiled=True)
    loss = pl.pallas_call(
        sum_kernel, out_shape=shape((1, 1), F32), in_specs=[VMEM], out_specs=VMEM,
        **small(4, 10**6),
    )(totals)
    return caption_loss.reshape(B), image_loss.reshape(B), loss.reshape(())


def solution(mesh):
    torus = Mesh(mesh.devices.reshape(*SIZES.values()), AXES)
    return jax.shard_map(
        step,
        mesh=torus,
        in_specs=(P(AXES, None), P(AXES, None), P(AXES), P(AXES)),
        out_specs=(P(AXES), P(AXES), P()),
        check_vma=False,
    )
```
